32 devices in a mesh: tm: 8 (over z, y), space: 4 (over x, core).
Axes of the slice: x: 2, y: 2, z: 4, core: 2. Of those that a mesh axis runs over, the one named last changes fastest.
Arguments:
- right_side: float32 [512, 32, 256], P('tm', 'space'), may hold values from -24 to 24
- diffusion: float32 [32, 256], P('space'), may hold values from 0.5 to 4
- velocity: float32 [2, 32, 256], P(None, 'space'), may hold values from -0.5 to 0.5
Outputs:
- solution: float32 [512, 32, 256], P('tm', 'space')
- residual: float32 [512, 32, 256], P('tm', 'space')
The draws below stay inside these ranges and needn't reach their ends.
All inputs are finite; a program needn't handle non-finite values.
Results may differ from the reference program's by a relative error of at most 0.0003.
Values sent between devices are 32-bit elements; how exact they have to be, the bound alone decides.
No kernel may reach another device: no remote copies, remote signals or barrier semaphores. Data moves between devices by JAX's collectives and lax.ppermute only.
A program may use at most 64 MiB of HBM per device.

```python
import math
import jax
import jax.numpy as jnp
from jax import lax

L = 512
NC = 256
KRYLOV = 3
SWEEPS = 3
NR = 32


def draw_right_side(key, part):
    base_key = jax.random.fold_in(key, 7)
    first = jax.random.fold_in(base_key, 0)
    noise = jax.random.normal(first, (L, NR, NC), jnp.float32)
    ramp = jnp.exp(jnp.arange(L, dtype=jnp.float32) * (math.log(3.0) / (L - 1)))[:, None, None]
    field = noise
    return jnp.clip(field * ramp, -24.0, 24.0)


def block_scale(key, dims, pieces, low, largest):
    loudness = 1.0
    for axis_at, shards_of in pieces:
        heights = jax.random.uniform(jax.random.fold_in(jax.random.fold_in(key, 6), axis_at), (shards_of,), jnp.float32, low / len(pieces), largest / len(pieces))
        loudness = loudness * jnp.repeat(jnp.exp(heights), dims[axis_at] // shards_of).reshape((-1,) + (1,) * (len(dims) - 1 - axis_at))
    return loudness


def setup_inputs(seed: int = 0) -> dict:
    splits = jax.random.split(jax.random.key(seed), 4)
    right_side = draw_right_side(jax.random.fold_in(splits[3], 71), 0)
    diffusion = jnp.clip(jnp.exp(math.log(4.0) - 2.0794415 * jax.random.uniform(splits[1], (NR, NC), jnp.float32) ** block_scale(splits[1], (NR, NC), ((0, 4),), -0.2, 0.2)), 0.5, 4.0)
    velocity = jnp.clip(jax.random.uniform(splits[2], (2, NR, NC), jnp.float32, -0.5, 0.5) * block_scale(splits[2], (2, NR, NC), ((1, 4),), -0.4, 0.0), -0.5, 0.5)
    return {"right_side": right_side, "diffusion": diffusion, "velocity": velocity}


alpha_corner = 0.05
damping = 0.8
epsilon = 1e-06

def stencil(field, padded, diffusion, velocity):
    north = padded[..., :-2, 1:-1]
    south = padded[..., 2:, 1:-1]
    west = padded[..., 1:-1, :-2]
    east = padded[..., 1:-1, 2:]
    return (1.0 + 4.0 * diffusion) * field - diffusion * (north + south + west + east) + velocity[0] * (east - west) + velocity[1] * (south - north)

def apply_step(field, diffusion, velocity):
    padded = jnp.pad(field, ((0, 0), (1, 1), (1, 1)))
    return stencil(field, padded, diffusion, velocity)

def system(field, diffusion, velocity):
    image = apply_step(field, diffusion, velocity)
    earlier = jnp.concatenate([jnp.zeros_like(field[:1]), field[:-1]], axis=0)
    return image - earlier

def divided(real_part, imag_part, diag_real, diag_imag, modulus):
    return (damping * (real_part * diag_real + imag_part * diag_imag) / modulus, damping * (imag_part * diag_real - real_part * diag_imag) / modulus)

def remainder(source_real, source_imag, image_real, image_imag, guess_real, guess_imag, shift_real, shift_imag):
    return (source_real - (image_real - (shift_real * guess_real + shift_imag * guess_imag)), source_imag - (image_imag - (shift_real * guess_imag - shift_imag * guess_real)))

def precondition(vector, diffusion, velocity):
    times = jnp.arange(L, dtype=jnp.float32)
    log_decay = math.log(alpha_corner) / L
    decay = math.exp(log_decay)
    scaled = vector * jnp.exp(times * log_decay)[:, None, None]
    spectrum = jnp.fft.fft(scaled, axis=0)
    source_real = jnp.real(spectrum)
    source_imag = jnp.imag(spectrum)
    angles = times * (2.0 * math.pi / L)
    shift_real = (decay * jnp.cos(angles))[:, None, None]
    shift_imag = (decay * jnp.sin(angles))[:, None, None]
    diag_real = 1.0 + 4.0 * diffusion - shift_real
    diag_imag = shift_imag
    modulus = diag_real * diag_real + diag_imag * diag_imag
    guess_real, guess_imag = divided(source_real, source_imag, diag_real, diag_imag, modulus)
    for sweep in range(SWEEPS - 1):
        image_real = apply_step(guess_real, diffusion, velocity)
        image_imag = apply_step(guess_imag, diffusion, velocity)
        left_real, left_imag = remainder(source_real, source_imag, image_real, image_imag, guess_real, guess_imag, shift_real, shift_imag)
        step_real, step_imag = divided(left_real, left_imag, diag_real, diag_imag, modulus)
        guess_real = guess_real + step_real
        guess_imag = guess_imag + step_imag
    back = jnp.real(jnp.fft.ifft(guess_real + 1j * guess_imag, axis=0))
    return back * jnp.exp(-times * log_decay)[:, None, None]

def least_squares(hessen, beta):
    ortho = []
    upper = [[None] * KRYLOV for row in range(KRYLOV)]
    for column in range(KRYLOV):
        current = hessen[:, column]
        for row in range(column):
            factor = jnp.sum(ortho[row] * current)
            upper[row][column] = factor
            current = current - factor * ortho[row]
        length = jnp.sqrt(jnp.sum(current * current))
        upper[column][column] = length
        ortho.append(current / length)
    target = [ortho[row][0] * beta for row in range(KRYLOV)]
    values = [None] * KRYLOV
    for row in reversed(range(KRYLOV)):
        accum = target[row]
        for later in range(row + 1, KRYLOV):
            accum = accum - upper[row][later] * values[later]
        values[row] = accum / upper[row][row]
    return jnp.stack(values)

def reference(right_side, diffusion, velocity):
    beta = jnp.sqrt(jnp.sum(right_side * right_side) + epsilon)
    basis = [right_side / beta]
    prepared = []
    hessen = jnp.zeros((KRYLOV + 1, KRYLOV), right_side.dtype)
    for column in range(KRYLOV):
        direction = precondition(basis[column], diffusion, velocity)
        prepared.append(direction)
        image = system(direction, diffusion, velocity)
        projections = jnp.stack([jnp.sum(vector * image) for vector in basis])
        for row in range(column + 1):
            image = image - projections[row] * basis[row]
        length = jnp.sqrt(jnp.sum(image * image) + epsilon)
        hessen = hessen.at[:column + 1, column].set(projections)
        hessen = hessen.at[column + 1, column].set(length)
        basis.append(image / length)
    coeffs = least_squares(hessen, beta)
    solution = prepared[0] * coeffs[0]
    for column in range(1, KRYLOV):
        solution = solution + prepared[column] * coeffs[column]
    first = (jnp.arange(KRYLOV + 1) == 0).astype(right_side.dtype)
    target = beta * first - lax.optimization_barrier(jnp.sum(hessen * coeffs[None, :], axis=1))
    residual = basis[0] * target[0]
    for row in range(1, KRYLOV + 1):
        residual = residual + basis[row] * target[row]
    return (solution, residual)
```

```python
import math

import jax
import jax.numpy as jnp
from jax import lax
from jax.experimental import pallas as pl
from jax.experimental.pallas import tpu as pltpu
from jax.sharding import PartitionSpec as P

L = 512
KRYLOV = 3
SWEEPS = 3


alpha_corner = 0.05
damping = 0.8
epsilon = 1e-06
highest = lax.Precision.HIGHEST


def extended(block, sides, width):
    for axis, dim in sides:
        count = lax.axis_size(axis)
        forward = [(i, i + 1) for i in range(count - 1)]
        backward = [(target, source) for source, target in forward]
        low = lax.ppermute(
            lax.slice_in_dim(block, block.shape[dim] - width, None, axis=dim), axis, forward
        )
        high = lax.ppermute(lax.slice_in_dim(block, 0, width, axis=dim), axis, backward)
        block = jnp.concatenate([low, block, high], axis=dim)
    return block


def from_behind(block, axis, distance):
    devices = range(lax.axis_size(axis))
    route = [(i - distance, i) for i in devices if i - distance in devices]
    return lax.ppermute(block, axis, route)


def shifted(padded, row_dim, col_dim, rows, cols, row_start, col_start):
    piece = lax.slice_in_dim(padded, row_start, row_start + rows, axis=row_dim)
    return lax.slice_in_dim(piece, col_start, col_start + cols, axis=col_dim)


def stencil(field, padded, row_dim, col_dim, diffusion, velocity_col, velocity_row):
    rows = field.shape[row_dim]
    cols = field.shape[col_dim]
    north = shifted(padded, row_dim, col_dim, rows, cols, 0, 1)
    south = shifted(padded, row_dim, col_dim, rows, cols, 2, 1)
    west = shifted(padded, row_dim, col_dim, rows, cols, 1, 0)
    east = shifted(padded, row_dim, col_dim, rows, cols, 1, 2)
    return (
        (1.0 + 4.0 * diffusion) * field
        - diffusion * (north + south + west + east)
        + velocity_col * (east - west)
        + velocity_row * (south - north)
    )


def divided(real_part, imag_part, diag_real, diag_imag, modulus):
    return (
        damping * (real_part * diag_real + imag_part * diag_imag) / modulus,
        damping * (imag_part * diag_real - real_part * diag_imag) / modulus,
    )


def remainder(
    source_real, source_imag, image_real, image_imag, guess_real, guess_imag, shift_real, shift_imag
):
    return (
        source_real - (image_real - (shift_real * guess_real + shift_imag * guess_imag)),
        source_imag - (image_imag - (shift_real * guess_imag - shift_imag * guess_real)),
    )


def dft_tables(length):
    index = jnp.arange(length, dtype=jnp.int32)
    product = index[:, None] * index[None, :] % length
    angle = product.astype(jnp.float32) * (2.0 * math.pi / length)
    return (jnp.cos(angle), jnp.sin(angle))


def least_squares(hessen, beta):
    ortho = []
    upper = [[None] * KRYLOV for row in range(KRYLOV)]
    for column in range(KRYLOV):
        current = hessen[:, column]
        for row in range(column):
            factor = jnp.sum(ortho[row] * current)
            upper[row][column] = factor
            current = current - factor * ortho[row]
        length = jnp.sqrt(jnp.sum(current * current))
        upper[column][column] = length
        ortho.append(current / length)
    target = [ortho[row][0] * beta for row in range(KRYLOV)]
    values = [None] * KRYLOV
    for row in reversed(range(KRYLOV)):
        accum = target[row]
        for later in range(row + 1, KRYLOV):
            accum = accum - upper[row][later] * values[later]
        values[row] = accum / upper[row][row]
    return jnp.stack(values)


def generic_device(right_side, diffusion, velocity):
    steps_here = right_side.shape[0]
    devices_tm = lax.axis_size("tm")
    position = lax.axis_index("tm")
    log_decay = math.log(alpha_corner) / L
    decay = math.exp(log_decay)
    local_steps = position * steps_here + jnp.arange(steps_here, dtype=jnp.int32)
    times = local_steps.astype(jnp.float32)
    weights = jnp.exp(times * log_decay)[:, None, None]
    unweights = jnp.exp(-times * log_decay)[:, None, None]
    cosine, sine = dft_tables(L)
    velocity_col = velocity[0]
    velocity_row = velocity[1]
    width = right_side.shape[2] // devices_tm
    start = position * width
    diff_strip = lax.dynamic_slice_in_dim(diffusion, start, width, 1)[:, :, None]
    col_strip = lax.dynamic_slice_in_dim(velocity_col, start, width, 1)[:, :, None]
    row_strip = lax.dynamic_slice_in_dim(velocity_row, start, width, 1)[:, :, None]
    angles = jnp.arange(L, dtype=jnp.int32).astype(jnp.float32) * (2.0 * math.pi / L)
    shift_real = decay * jnp.cos(angles)
    shift_imag = decay * jnp.sin(angles)
    diag_real = 1.0 + 4.0 * diff_strip - shift_real
    modulus = diag_real * diag_real + shift_imag * shift_imag

    def forward(block):
        real_part = jnp.dot(block, cosine, precision=highest)
        imag_part = -jnp.dot(block, sine, precision=highest)
        return jnp.concatenate([real_part, imag_part], axis=2)

    total = lax.psum(jnp.sum(right_side * right_side), ("tm", "space"))
    beta = jnp.sqrt(total + epsilon)
    basis = [right_side / beta]
    prepared = []
    hessen = jnp.zeros((KRYLOV + 1, KRYLOV), jnp.float32)
    for column in range(KRYLOV):
        moved = jnp.transpose(basis[column] * weights, (1, 2, 0))
        spectrum = forward(lax.all_to_all(moved, "tm", split_axis=1, concat_axis=2, tiled=True))
        source_real = spectrum[:, :, :L]
        source_imag = spectrum[:, :, L:]
        guess_real, guess_imag = divided(source_real, source_imag, diag_real, shift_imag, modulus)
        for sweep in range(SWEEPS - 1):
            joined = jnp.concatenate([guess_real, guess_imag], axis=2)
            padded = extended(joined, (("tm", 1), ("space", 0)), 1)
            image = stencil(joined, padded, 0, 1, diff_strip, col_strip, row_strip)
            left_real, left_imag = remainder(
                source_real,
                source_imag,
                image[:, :, :L],
                image[:, :, L:],
                guess_real,
                guess_imag,
                shift_real,
                shift_imag,
            )
            step_real, step_imag = divided(left_real, left_imag, diag_real, shift_imag, modulus)
            guess_real = guess_real + step_real
            guess_imag = guess_imag + step_imag
        back = (
            jnp.dot(guess_real, cosine, precision=highest)
            - jnp.dot(guess_imag, sine, precision=highest)
        ) / L
        back = lax.all_to_all(back, "tm", split_axis=2, concat_axis=1, tiled=True)
        direction = jnp.transpose(back, (2, 0, 1)) * unweights
        prepared.append(direction)
        apply_padded = extended(direction, (("space", 1),), 1)
        apply_padded = jnp.pad(apply_padded, ((0, 0), (0, 0), (1, 1)))
        apply_image = stencil(direction, apply_padded, 1, 2, diffusion, velocity_col, velocity_row)
        earlier = from_behind(direction[-1:], "tm", 1)
        image = apply_image - jnp.concatenate([earlier, direction[:-1]], axis=0)
        local = jnp.stack([jnp.sum(vector * image) for vector in basis])
        projections = lax.psum(local, ("tm", "space"))
        for row in range(column + 1):
            image = image - projections[row] * basis[row]
        squares = lax.psum(jnp.sum(image * image), ("tm", "space"))
        length = jnp.sqrt(squares + epsilon)
        hessen = hessen.at[: column + 1, column].set(projections)
        hessen = hessen.at[column + 1, column].set(length)
        basis.append(image / length)
    coeffs = least_squares(hessen, beta)
    solution = prepared[0] * coeffs[0]
    for column in range(1, KRYLOV):
        solution = solution + prepared[column] * coeffs[column]
    first = (jnp.arange(KRYLOV + 1) == 0).astype(jnp.float32)
    target = beta * first - jnp.sum(hessen * coeffs[None, :], axis=1)
    residual = basis[0] * target[0]
    for row in range(1, KRYLOV + 1):
        residual = residual + basis[row] * target[row]
    return (solution, residual)


SUB = 8
LANE = 128
AXES = ("tm", "space")
UNROLL = 8


def spin(block, amount, axis=1):
    return pltpu.roll(block, amount % block.shape[axis], axis)


def lane_of(shape):
    return lax.broadcasted_iota(jnp.int32, shape, 1)


def exchange_blocks(pieces, width):
    pieces = list(pieces)
    group = lane_of(pieces[0].shape) // width
    step = 1
    while step < len(pieces):
        keep = (group & step) == 0
        for i in range(len(pieces)):
            if i & step:
                continue
            low, high = pieces[i], pieces[i + step]
            pieces[i] = jnp.where(keep, low, spin(high, step * width))
            pieces[i + step] = jnp.where(keep, spin(low, -step * width), high)
        step *= 2
    return pieces


class Plan:
    def __init__(self, mesh, steps, rows, cols):
        self.tm = mesh.shape["tm"]
        self.space = mesh.shape["space"]
        self.devices = self.tm * self.space
        self.steps = steps
        self.rows = rows
        self.cols = cols
        self.here = steps // self.tm
        self.window = LANE // self.tm
        self.own = cols // self.devices
        self.halo = SWEEPS
        self.slot = self.window // self.space
        self.ring = [self.strip_of(d // self.space, d % self.space) for d in range(self.devices)]
        self.holder = [self.ring.index(j) for j in range(self.devices)]

    def fits(self):
        return (
            LANE % self.tm == 0
            and self.tm == SUB
            and self.rows == SUB * self.space
            and self.cols % self.devices == 0
            and self.cols == 2 * LANE
            and self.steps % (self.tm * 2 * SUB) == 0
            and self.window == 2 * self.own
            and self.own + 2 * self.halo + 2 <= self.window
            and self.here >= 2 * self.window
            and self.slot >= self.halo
            and self.space % 2 == 0
        )

    def strip_of(self, t, s):
        turn = t ^ ((t >> 1) & 1)
        half = self.space // 2
        x, core = s // 2, s % 2
        odd = turn % 2
        return (turn * half + x + odd * (half - 1 - 2 * x)) * 2 + core


def pack_kernel(plan, right_ref, diff_ref, vel_ref, out_ref):
    window, halo, own = plan.window, plan.halo, plan.own
    spot = lane_of((SUB, plan.cols)) % window
    last, final = window - 2, window - 1
    diff = diff_ref[...]
    vel_col = vel_ref[0]
    vel_row = vel_ref[1]
    for a in range(plan.here // SUB):
        sides = [[], []]
        for i in range(SUB):
            n = a * SUB + i
            field = right_ref[n]
            for parity in range(2):
                base = parity * own - halo
                piece = spin(field, -base)
                if n < window:
                    piece = jnp.where(spot == last, spin(diff, last - base - n), piece)
                    piece = jnp.where(spot == final, spin(vel_col, final - base - n), piece)
                elif n < 2 * window:
                    piece = jnp.where(spot == last, spin(vel_row, last - base - n + window), piece)
                sides[parity].append(piece)
        for parity in range(2):
            for part in range(plan.cols // LANE):
                cut = [piece[:, part * LANE : (part + 1) * LANE] for piece in sides[parity]]
                for m, piece in enumerate(exchange_blocks(cut, window)):
                    strip = 2 * (part * SUB + m) + parity
                    out_ref[plan.holder[strip], a * SUB : (a + 1) * SUB, :] = piece


def totals_of(ref):
    return jnp.sum(ref[...], axis=0, keepdims=True)


def pick(totals, k):
    lane = lane_of(totals.shape)
    value = jnp.sum(jnp.where(lane == k, totals, 0.0), axis=1, keepdims=True)
    return jnp.broadcast_to(value, (1, LANE))


class Scalars:
    def __init__(self, sums):
        self.norms = []
        self.scale = []
        self.cross = {}
        self.inner = {}
        self.taken = {}
        self.below = []
        for j, totals in enumerate(sums):
            norm = pick(totals, 0)
            self.norms.append(norm)
            if j == 0:
                self.beta = jnp.sqrt(norm + epsilon)
                self.scale.append(1.0 / self.beta)
            else:
                before = self.scale[j - 1]
                length = jnp.sqrt(before * before * norm + epsilon)
                self.below.append(length)
                self.scale.append(before / length)
            for i in range(j):
                self.cross[i, j] = pick(totals, 1 + i)
            for i in range(j + 1):
                self.inner[i, j] = pick(totals, KRYLOV + i)
                self.taken[i, j] = self.scale[i] * self.scale[i] * self.inner[i, j]

    def finish(self, square):
        last = KRYLOV - 1
        for i in range(KRYLOV):
            square = square - 2.0 * self.taken[i, last] * self.inner[i, last]
            for k in range(KRYLOV):
                pair = self.norms[i] if i == k else self.cross[min(i, k), max(i, k)]
                square = square + self.taken[i, last] * self.taken[k, last] * pair
        scale = self.scale[last]
        self.below.append(jnp.sqrt(jnp.maximum(scale * scale * square, 0.0) + epsilon))
        zero = jnp.zeros_like(self.beta)
        hessen = [[zero] * KRYLOV for row in range(KRYLOV + 1)]
        for j in range(KRYLOV):
            for i in range(j + 1):
                hessen[i][j] = self.scale[i] * self.scale[j] * self.inner[i, j]
            hessen[j + 1][j] = self.below[j]
        ortho = []
        upper = [[None] * KRYLOV for row in range(KRYLOV)]
        for column in range(KRYLOV):
            current = [hessen[row][column] for row in range(KRYLOV + 1)]
            for row in range(column):
                factor = sum(a * b for a, b in zip(ortho[row], current))
                upper[row][column] = factor
                current = [b - factor * a for a, b in zip(ortho[row], current)]
            length = jnp.sqrt(sum(b * b for b in current))
            upper[column][column] = length
            ortho.append([b / length for b in current])
        values = [None] * KRYLOV
        for row in reversed(range(KRYLOV)):
            accum = ortho[row][0] * self.beta
            for later in range(row + 1, KRYLOV):
                accum = accum - upper[row][later] * values[later]
            values[row] = accum / upper[row][row]
        target = []
        for row in range(KRYLOV):
            value = self.beta if row == 0 else zero
            target.append(value - sum(hessen[row][j] * values[j] for j in range(KRYLOV)))
        along = [values[j] * self.scale[j] for j in range(KRYLOV)]
        rest = [
            target[i] * self.scale[i] + along[last] * self.taken[i, last] for i in range(KRYLOV)
        ]
        return along, rest, -along[last]


def coefficients(plan, first_ref, strip, table_ref):
    shape = (plan.rows, LANE)
    window = plan.window
    spot = lane_of(shape) % window
    last, final = window - 2, window - 1
    diff = vel_col = vel_row = jnp.zeros(shape, jnp.float32)
    for k in range(window):
        here = spot == k
        early = first_ref[k]
        diff = jnp.where(here, spin(early, k - last), diff)
        vel_col = jnp.where(here, spin(early, k - final), vel_col)
        vel_row = jnp.where(here, spin(first_ref[window + k], k - last), vel_row)
    row = lax.broadcasted_iota(jnp.int32, shape, 0)
    col = strip * plan.own - plan.halo + spot
    center = 1.0 + 4.0 * diff
    table_ref[0] = center
    table_ref[1] = 1.0 / center
    table_ref[2] = jnp.where(row > 0, diff + vel_row, 0.0)
    table_ref[3] = jnp.where(row < plan.rows - 1, diff - vel_row, 0.0)
    table_ref[4] = jnp.where(col > 0, diff + vel_col, 0.0)
    table_ref[5] = jnp.where(col < plan.cols - 1, diff - vel_col, 0.0)


def krylov_kernel(plan, j, *refs):
    refs = list(refs)
    strip_ref = refs.pop(0)
    strip = strip_ref[0]
    here, window, rows, halo = plan.here, plan.window, plan.rows, plan.halo
    shape = (rows, LANE)
    lane = lane_of(shape)
    spot = lane % window
    low_lane = lane_of((SUB, LANE))
    low_spot = low_lane % window
    even = strip % 2 == 0
    if j == 0:
        recv_ref = refs.pop(0)
        table_ref, q_ref, z_ref, w_ref, near_ref, far_ref, sum_ref, y_ref, g_ref = refs
        older = []

        def unpack(a, carry):
            start = pl.multiple_of(a * SUB, SUB)
            for s in range(plan.space):
                cut = [
                    recv_ref[p * plan.space + s, pl.ds(start, SUB), :] for p in range(plan.tm)
                ]
                for i, piece in enumerate(exchange_blocks(cut, window)):
                    q_ref[a * SUB + i, s * SUB : (s + 1) * SUB, :] = piece
            return carry

        lax.fori_loop(0, here // SUB, unpack, 0)
        coefficients(plan, q_ref, strip, table_ref)
    else:
        table_ref, image_ref, near_in, far_in = refs[:4]
        older = refs[4 : 4 + j]
        sums = refs[4 + j : 4 + 2 * j]
        q_ref, z_ref, w_ref, near_ref, far_ref, sum_ref, y_ref, g_ref = refs[4 + 2 * j :]
        scalars = Scalars([totals_of(ref) for ref in sums])
        taken = [scalars.taken[i, j - 1] for i in range(j)]
    if j == KRYLOV - 1:
        near_ref = far_ref = None
    center = table_ref[0]
    inverse = table_ref[1]
    north, south, west, east = (table_ref[2 + k] for k in range(4))
    zero = jnp.zeros(shape, jnp.float32)

    def around(field):
        return (
            north * spin(field, 1, 0)
            + south * spin(field, -1, 0)
            + west * spin(field, 1)
            + east * spin(field, -1)
        )

    power = inverse
    for _ in range(int(math.log2(here))):
        power = power * power
    opening = jnp.where(lane < window, alpha_corner, 1.0)
    gains = [power * opening]
    reach = window
    while reach < LANE:
        gains.append(gains[-1] * spin(gains[-1], reach))
        reach *= 2
    closing = 1.0 / (1.0 - gains[-1])

    def entering(ends):
        total = spin(ends, window) * opening
        distance = window
        for gain in gains[:-1]:
            total = total + gain * spin(total, distance)
            distance *= 2
        return total * closing

    def loop(body, carry):
        def several(i, carry):
            for k in range(UNROLL):
                carry = body(i * UNROLL + k, carry)
            return carry

        return lax.fori_loop(0, here // UNROLL, several, carry)

    slot = plan.slot
    left_spot = (spot < halo,)
    first_side = jnp.where(even, halo + plan.own, 0)
    second_side = jnp.where(even, 0, halo + plan.own)

    def side_mask(start):
        return (low_spot >= start) & (low_spot < start + halo)

    near_mask = side_mask(first_side)
    far_mask = side_mask(second_side)

    def merged(n):
        image = image_ref[n]
        near = near_in[n]
        far = far_in[n]
        parts = []
        for s in range(plan.space):
            part = image[s * SUB : (s + 1) * SUB]
            part = jnp.where(near_mask, pltpu.roll(near, (first_side - slot * s + LANE) % LANE, 1), part)
            part = jnp.where(far_mask, pltpu.roll(far, (second_side - slot * s + LANE) % LANE, 1), part)
            parts.append(part)
        return jnp.concatenate(parts, axis=0)

    def first(n, y):
        if j == 0:
            q = q_ref[n]
        else:
            q = merged(n)
            for i in range(j):
                q = q - taken[i] * older[i][n]
            q_ref[n] = q
        y = (q + y) * inverse
        y_ref[n] = y
        return y

    y = loop(first, zero)

    def sweep(step):
        def body(n, carry):
            y, z = carry
            z = z * inverse
            guess = damping * (y_ref[n] + z)
            if step:
                guess = (1.0 - damping) * g_ref[n] + guess
            g_ref[n] = guess
            y = (q_ref[n] + around(guess) + y) * inverse
            y_ref[n] = y
            return (y, z)

        return body

    for step in range(SWEEPS - 1):
        y, _ = loop(sweep(step), (zero, entering(y)))
    start = entering(y)
    ending = (1.0 - damping) * g_ref[here - 1] + damping * (y + start * power)
    before = jnp.where(lane < window, 0.0, spin(ending, window))

    near_from = jnp.where(even, plan.own, halo)
    far_from = jnp.where(even, halo, plan.own)
    fields = 1 + j + (j + 1) + (1 if j == KRYLOV - 1 else 0)

    def fold(block):
        return sum(block[s * SUB : (s + 1) * SUB] for s in range(plan.space))

    def last(n, carry):
        z, before, accs = carry
        z = z * inverse
        guess = (1.0 - damping) * g_ref[n] + damping * (y_ref[n] + z)
        z_ref[n] = guess
        image = center * guess - around(guess) - before
        w_ref[n] = image
        if near_ref is not None:
            near = far = None
            for s in range(plan.space):
                part = image[s * SUB : (s + 1) * SUB]
                a = pltpu.roll(part, (slot * s - near_from + LANE) % LANE, 1)
                b = pltpu.roll(part, (slot * s - far_from + LANE) % LANE, 1)
                inside = low_spot // slot == s
                near = a if near is None else jnp.where(inside, a, near)
                far = b if far is None else jnp.where(inside, b, far)
            near_ref[n] = near
            far_ref[n] = far
        q = q_ref[n]
        olds = [ref[n] for ref in older]
        products = [q * q] + [old * q for old in olds] + [old * image for old in olds] + [q * image]
        if j == KRYLOV - 1:
            products.append(image * image)
        accs = tuple(acc + fold(product) for acc, product in zip(accs, products))
        return (z, guess, accs)

    low_zero = jnp.zeros((SUB, LANE), jnp.float32)
    _, _, accs = loop(last, (start, before, (low_zero,) * fields))
    places = [0] + [1 + i for i in range(j)] + [KRYLOV + i for i in range(j + 1)] + [2 * KRYLOV]
    owned = (low_spot >= halo) & (low_spot < halo + plan.own)
    record = jnp.zeros((1, LANE), jnp.float32)
    record_lane = lane_of((1, LANE))
    for place, acc in zip(places, accs):
        value = jnp.sum(jnp.where(owned, acc, 0.0), axis=0, keepdims=True)
        value = jnp.sum(value, axis=1, keepdims=True)
        record = jnp.where(record_lane == place, value, record)
    sum_ref[...] = jnp.broadcast_to(record, sum_ref.shape)


def combine_kernel(plan, *refs):
    q_refs = refs[:KRYLOV]
    z_refs = refs[KRYLOV : 2 * KRYLOV]
    image_ref = refs[2 * KRYLOV]
    sums = refs[2 * KRYLOV + 1 : 3 * KRYLOV + 1]
    out_ref = refs[-1]
    totals = [totals_of(ref) for ref in sums]
    scalars = Scalars(totals)
    along, rest, tail = scalars.finish(pick(totals[-1], 2 * KRYLOV))
    own, halo, window = plan.own, plan.halo, plan.window
    front = lane_of((SUB, LANE)) % window < own
    groups = plan.here // (2 * SUB)

    def body(aa, carry):
        for s in range(plan.space):
            here = slice(s * SUB, (s + 1) * SUB)

            def solution_at(n):
                return sum(c * ref[n, here, :] for c, ref in zip(along, z_refs))

            def residual_at(n):
                total = tail * image_ref[n, here, :]
                for c, ref in zip(rest, q_refs):
                    total = total + c * ref[n, here, :]
                return total

            for f, value in enumerate((solution_at, residual_at)):
                pieces = []
                for i in range(SUB):
                    n = aa * 2 * SUB + 2 * i
                    pieces.append(
                        jnp.where(front, spin(value(n), -halo), spin(value(n + 1), own - halo))
                    )
                start = pl.multiple_of((f * groups + aa) * SUB, SUB)
                for p, piece in enumerate(exchange_blocks(pieces, window)):
                    out_ref[p * plan.space + s, pl.ds(start, SUB), :] = piece
        return carry

    lax.fori_loop(0, groups, body, 0)


def unpack_kernel(plan, recv_ref, *out_refs):
    groups = plan.here // (2 * SUB)
    count = LANE // plan.own

    def body(aa, carry):
        for f, out_ref in enumerate(out_refs):
            start = pl.multiple_of((f * groups + aa) * SUB, SUB)
            for part in range(plan.cols // LANE):
                pieces = [
                    recv_ref[plan.holder[part * count + m], pl.ds(start, SUB), :]
                    for m in range(count)
                ]
                for i, piece in enumerate(exchange_blocks(pieces, plan.own)):
                    out_ref[aa * count + i, :, part * LANE : (part + 1) * LANE] = piece
        return carry

    lax.fori_loop(0, groups, body, 0)


def call(kernel, shapes, operands, scalars=0, scratch=()):
    vmem = pl.BlockSpec(memory_space=pltpu.VMEM)
    smem = pl.BlockSpec(memory_space=pltpu.SMEM)
    return pl.pallas_call(
        kernel,
        out_shape=[jax.ShapeDtypeStruct(shape, jnp.float32) for shape in shapes],
        in_specs=[smem] * scalars + [vmem] * (len(operands) - scalars),
        out_specs=[vmem] * len(shapes),
        scratch_shapes=[pltpu.VMEM(shape, jnp.float32) for shape in scratch],
        compiler_params=pltpu.CompilerParams(vmem_limit_bytes=48 * 1024 * 1024),
    )(*operands)


def everyone(block):
    return lax.all_to_all(block, AXES, split_axis=0, concat_axis=0, tiled=True)


def strip_device(plan, right_side, diffusion, velocity):
    t = lax.axis_index("tm")
    s = lax.axis_index("space")
    strip = plan.strip_of(t, s).astype(jnp.int32).reshape(1)
    count = plan.devices
    hold = plan.holder
    near_route = []
    far_route = []
    for k in range(0, count, 2):
        near_route += [(hold[k], hold[k + 1]), (hold[k + 1], hold[k])]
    for k in range(1, count - 1, 2):
        far_route += [(hold[k], hold[k + 1]), (hold[k + 1], hold[k])]
    bind = lambda kernel, *more: (lambda *refs: kernel(plan, *more, *refs))
    full = (plan.here, plan.rows, LANE)
    side = (plan.here, SUB, LANE)
    small = (count, LANE)
    sent = call(bind(pack_kernel), [(count, plan.here, LANE)], [right_side, diffusion, velocity])[0]
    recv = everyone(sent)
    table, q, z, image, near, far, sums = call(
        bind(krylov_kernel, 0),
        [(6, plan.rows, LANE), full, full, full, side, side, small],
        [strip, recv],
        scalars=1,
        scratch=[full, full],
    )
    qs, zs, totals = [q], [z], []
    for j in range(1, KRYLOV):
        near = lax.ppermute(near, AXES, near_route)
        far = lax.ppermute(far, AXES, far_route)
        totals.append(everyone(sums))
        q, z, image, near, far, sums = call(
            bind(krylov_kernel, j),
            [full, full, full, side, side, small],
            [strip, table, image, near, far, *qs, *totals],
            scalars=1,
            scratch=[full, full],
        )
        qs.append(q)
        zs.append(z)
    totals.append(everyone(sums))
    packed = call(
        bind(combine_kernel), [(count, plan.here, LANE)], [*qs, *zs, image, *totals]
    )[0]
    shape = right_side.shape
    return tuple(call(bind(unpack_kernel), [shape, shape], [everyone(packed)]))


def per_device(mesh):
    def run(right_side, diffusion, velocity):
        rows = right_side.shape[1] * mesh.shape["space"]
        steps = right_side.shape[0] * mesh.shape["tm"]
        plan = Plan(mesh, steps, rows, right_side.shape[2])
        if plan.fits():
            return strip_device(plan, right_side, diffusion, velocity)
        return generic_device(right_side, diffusion, velocity)

    return run


def solution(mesh):
    placed = (P("tm", "space", None), P("space", None), P(None, "space", None))
    return jax.shard_map(
        per_device(mesh),
        mesh=mesh,
        in_specs=placed,
        out_specs=(P("tm", "space", None), P("tm", "space", None)),
        check_vma=False,
    )
```

```python
import math

import jax
import jax.numpy as jnp
from jax import lax
from jax.experimental import pallas as pl
from jax.experimental.pallas import tpu as pltpu
from jax.sharding import PartitionSpec as P

L = 512
KRYLOV = 3
SWEEPS = 3


alpha_corner = 0.05
damping = 0.8
epsilon = 1e-06
highest = lax.Precision.HIGHEST


def extended(block, sides, width):
    for axis, dim in sides:
        count = lax.axis_size(axis)
        forward = [(i, i + 1) for i in range(count - 1)]
        backward = [(target, source) for source, target in forward]
        low = lax.ppermute(
            lax.slice_in_dim(block, block.shape[dim] - width, None, axis=dim), axis, forward
        )
        high = lax.ppermute(lax.slice_in_dim(block, 0, width, axis=dim), axis, backward)
        block = jnp.concatenate([low, block, high], axis=dim)
    return block


def from_behind(block, axis, distance):
    devices = range(lax.axis_size(axis))
    route = [(i - distance, i) for i in devices if i - distance in devices]
    return lax.ppermute(block, axis, route)


def shifted(padded, row_dim, col_dim, rows, cols, row_start, col_start):
    piece = lax.slice_in_dim(padded, row_start, row_start + rows, axis=row_dim)
    return lax.slice_in_dim(piece, col_start, col_start + cols, axis=col_dim)


def stencil(field, padded, row_dim, col_dim, diffusion, velocity_col, velocity_row):
    rows = field.shape[row_dim]
    cols = field.shape[col_dim]
    north = shifted(padded, row_dim, col_dim, rows, cols, 0, 1)
    south = shifted(padded, row_dim, col_dim, rows, cols, 2, 1)
    west = shifted(padded, row_dim, col_dim, rows, cols, 1, 0)
    east = shifted(padded, row_dim, col_dim, rows, cols, 1, 2)
    return (
        (1.0 + 4.0 * diffusion) * field
        - diffusion * (north + south + west + east)
        + velocity_col * (east - west)
        + velocity_row * (south - north)
    )


def divided(real_part, imag_part, diag_real, diag_imag, modulus):
    return (
        damping * (real_part * diag_real + imag_part * diag_imag) / modulus,
        damping * (imag_part * diag_real - real_part * diag_imag) / modulus,
    )


def remainder(
    source_real, source_imag, image_real, image_imag, guess_real, guess_imag, shift_real, shift_imag
):
    return (
        source_real - (image_real - (shift_real * guess_real + shift_imag * guess_imag)),
        source_imag - (image_imag - (shift_real * guess_imag - shift_imag * guess_real)),
    )


def dft_tables(length):
    index = jnp.arange(length, dtype=jnp.int32)
    product = index[:, None] * index[None, :] % length
    angle = product.astype(jnp.float32) * (2.0 * math.pi / length)
    return (jnp.cos(angle), jnp.sin(angle))


def least_squares(hessen, beta):
    ortho = []
    upper = [[None] * KRYLOV for row in range(KRYLOV)]
    for column in range(KRYLOV):
        current = hessen[:, column]
        for row in range(column):
            factor = jnp.sum(ortho[row] * current)
            upper[row][column] = factor
            current = current - factor * ortho[row]
        length = jnp.sqrt(jnp.sum(current * current))
        upper[column][column] = length
        ortho.append(current / length)
    target = [ortho[row][0] * beta for row in range(KRYLOV)]
    values = [None] * KRYLOV
    for row in reversed(range(KRYLOV)):
        accum = target[row]
        for later in range(row + 1, KRYLOV):
            accum = accum - upper[row][later] * values[later]
        values[row] = accum / upper[row][row]
    return jnp.stack(values)


def generic_device(right_side, diffusion, velocity):
    steps_here = right_side.shape[0]
    devices_tm = lax.axis_size("tm")
    position = lax.axis_index("tm")
    log_decay = math.log(alpha_corner) / L
    decay = math.exp(log_decay)
    local_steps = position * steps_here + jnp.arange(steps_here, dtype=jnp.int32)
    times = local_steps.astype(jnp.float32)
    weights = jnp.exp(times * log_decay)[:, None, None]
    unweights = jnp.exp(-times * log_decay)[:, None, None]
    cosine, sine = dft_tables(L)
    velocity_col = velocity[0]
    velocity_row = velocity[1]
    width = right_side.shape[2] // devices_tm
    start = position * width
    diff_strip = lax.dynamic_slice_in_dim(diffusion, start, width, 1)[:, :, None]
    col_strip = lax.dynamic_slice_in_dim(velocity_col, start, width, 1)[:, :, None]
    row_strip = lax.dynamic_slice_in_dim(velocity_row, start, width, 1)[:, :, None]
    angles = jnp.arange(L, dtype=jnp.int32).astype(jnp.float32) * (2.0 * math.pi / L)
    shift_real = decay * jnp.cos(angles)
    shift_imag = decay * jnp.sin(angles)
    diag_real = 1.0 + 4.0 * diff_strip - shift_real
    modulus = diag_real * diag_real + shift_imag * shift_imag

    def forward(block):
        real_part = jnp.dot(block, cosine, precision=highest)
        imag_part = -jnp.dot(block, sine, precision=highest)
        return jnp.concatenate([real_part, imag_part], axis=2)

    total = lax.psum(jnp.sum(right_side * right_side), ("tm", "space"))
    beta = jnp.sqrt(total + epsilon)
    basis = [right_side / beta]
    prepared = []
    hessen = jnp.zeros((KRYLOV + 1, KRYLOV), jnp.float32)
    for column in range(KRYLOV):
        moved = jnp.transpose(basis[column] * weights, (1, 2, 0))
        spectrum = forward(lax.all_to_all(moved, "tm", split_axis=1, concat_axis=2, tiled=True))
        source_real = spectrum[:, :, :L]
        source_imag = spectrum[:, :, L:]
        guess_real, guess_imag = divided(source_real, source_imag, diag_real, shift_imag, modulus)
        for sweep in range(SWEEPS - 1):
            joined = jnp.concatenate([guess_real, guess_imag], axis=2)
            padded = extended(joined, (("tm", 1), ("space", 0)), 1)
            image = stencil(joined, padded, 0, 1, diff_strip, col_strip, row_strip)
            left_real, left_imag = remainder(
                source_real,
                source_imag,
                image[:, :, :L],
                image[:, :, L:],
                guess_real,
                guess_imag,
                shift_real,
                shift_imag,
            )
            step_real, step_imag = divided(left_real, left_imag, diag_real, shift_imag, modulus)
            guess_real = guess_real + step_real
            guess_imag = guess_imag + step_imag
        back = (
            jnp.dot(guess_real, cosine, precision=highest)
            - jnp.dot(guess_imag, sine, precision=highest)
        ) / L
        back = lax.all_to_all(back, "tm", split_axis=2, concat_axis=1, tiled=True)
        direction = jnp.transpose(back, (2, 0, 1)) * unweights
        prepared.append(direction)
        apply_padded = extended(direction, (("space", 1),), 1)
        apply_padded = jnp.pad(apply_padded, ((0, 0), (0, 0), (1, 1)))
        apply_image = stencil(direction, apply_padded, 1, 2, diffusion, velocity_col, velocity_row)
        earlier = from_behind(direction[-1:], "tm", 1)
        image = apply_image - jnp.concatenate([earlier, direction[:-1]], axis=0)
        local = jnp.stack([jnp.sum(vector * image) for vector in basis])
        projections = lax.psum(local, ("tm", "space"))
        for row in range(column + 1):
            image = image - projections[row] * basis[row]
        squares = lax.psum(jnp.sum(image * image), ("tm", "space"))
        length = jnp.sqrt(squares + epsilon)
        hessen = hessen.at[: column + 1, column].set(projections)
        hessen = hessen.at[column + 1, column].set(length)
        basis.append(image / length)
    coeffs = least_squares(hessen, beta)
    solution = prepared[0] * coeffs[0]
    for column in range(1, KRYLOV):
        solution = solution + prepared[column] * coeffs[column]
    first = (jnp.arange(KRYLOV + 1) == 0).astype(jnp.float32)
    target = beta * first - jnp.sum(hessen * coeffs[None, :], axis=1)
    residual = basis[0] * target[0]
    for row in range(1, KRYLOV + 1):
        residual = residual + basis[row] * target[row]
    return (solution, residual)


SUB = 8
LANE = 128
AXES = ("tm", "space")
UNROLL = 8


def spin(block, amount, axis=1):
    return pltpu.roll(block, amount % block.shape[axis], axis)


def lane_of(shape):
    return lax.broadcasted_iota(jnp.int32, shape, 1)


def exchange_blocks(pieces, width, radix):
    pieces = list(pieces)
    lane = lane_of(pieces[0].shape)
    step = 1
    while step < len(pieces):
        digit = lane // (width * step) % radix
        result = list(pieces)
        for i in range(len(pieces)):
            e = i // step % radix
            total = None
            for d in range(radix):
                moved = pieces[i + (d - e) * step]
                if d != e:
                    moved = spin(moved, (d - e) * step * width)
                total = moved if total is None else jnp.where(digit == d, moved, total)
            result[i] = total
        pieces = result
        step *= radix
    return pieces


class Plan:
    def __init__(self, mesh, steps, rows, cols):
        self.tm = mesh.shape["tm"]
        self.space = mesh.shape["space"]
        self.devices = self.tm * self.space
        self.steps = steps
        self.rows = rows
        self.cols = cols
        self.here = steps // self.tm
        self.window = LANE // self.tm
        self.own = cols // self.devices
        self.halo = SWEEPS
        self.slot = self.window // self.space
        self.used = self.own + 2 * self.halo
        self.spare = self.window - self.used
        self.tiles = self.here // SUB
        self.inward = (self.tiles - 1) * SUB + 1
        self.groups = self.here // (2 * SUB)
        self.outward = self.groups * SUB + 2 * self.groups + 1
        self.ring = [self.strip_of(d // self.space, d % self.space) for d in range(self.devices)]
        self.holder = [self.ring.index(j) for j in range(self.devices)]

    def fits(self):
        return (
            LANE % self.tm == 0
            and self.tm == SUB
            and self.rows == SUB * self.space
            and self.cols % self.devices == 0
            and self.cols == 2 * LANE
            and self.steps % (self.tm * 2 * SUB) == 0
            and self.window == 2 * self.own
            and self.spare * (self.tiles - 1) == self.used
            and self.here % UNROLL == 0
            and self.groups * 2 == SUB
            and self.slot >= self.halo
            and self.space % 2 == 0
        )

    def strip_of(self, t, s):
        turn = t ^ ((t >> 1) & 1)
        half = self.space // 2
        x, core = s // 2, s % 2
        odd = turn % 2
        return (turn * half + x + odd * (half - 1 - 2 * x)) * 2 + core


def pack_kernel(plan, place_ref, right_ref, diff_ref, vel_ref, out_ref, tail_ref):
    window, own, halo = plan.window, plan.own, plan.halo
    parts = plan.cols // LANE
    lane = lane_of((SUB, LANE))
    group, spot = lane // window, lane % window
    edge = LANE - (SUB - 1) * window - own + halo

    def strips():
        for parity in range(2):
            for part in range(parts):
                for m in range(SUB):
                    yield parity, part, m, plan.holder[2 * (part * SUB + m) + parity]

    def body(k, carry):
        a = plan.tiles - 1 - k
        fields = [right_ref[a * SUB + i] for i in range(SUB)]
        cache = {}

        def turned(i, part, amount):
            key = (i, part % parts, amount % LANE)
            if key not in cache:
                block = fields[i][:, key[1] * LANE : (key[1] + 1) * LANE]
                cache[key] = spin(block, amount)
            return cache[key]

        pieces = []
        for parity, part, m, _ in strips():
            base = parity * own - halo
            total = None
            for i in range(SUB):
                amount = window * (i - m) - base
                value = turned(i, part, amount)
                if parity == 0 and m == 0:
                    value = jnp.where(spot < halo, turned(i, part - 1, amount), value)
                if parity == 1 and m == SUB - 1:
                    value = jnp.where(spot >= edge, turned(i, part + 1, amount), value)
                total = value if total is None else jnp.where(group == i, value, total)
            pieces.append(total)

        @pl.when(k == 0)
        def _():
            for index, piece in enumerate(pieces):
                tail_ref[index] = piece

        @pl.when(k > 0)
        def _():
            amount = plan.used - plan.spare * a
            for index, (_, _, _, target) in enumerate(strips()):
                tail = pltpu.roll(tail_ref[index], amount, 1)
                piece = jnp.where(spot >= plan.used, tail, pieces[index])
                out_ref[pl.ds(target * plan.inward + a * SUB, SUB), :] = piece

        return carry

    lax.fori_loop(0, plan.tiles, body, 0)
    row = pl.ds(place_ref[0], 1)
    lines = [diff_ref[row, :], vel_ref[0, row, :], vel_ref[1, row, :]]
    sub = lax.broadcasted_iota(jnp.int32, (SUB, LANE), 0)
    blocks = [
        [jnp.broadcast_to(line[:, h * LANE : (h + 1) * LANE], (SUB, LANE)) for h in range(parts)]
        for line in lines
    ]
    for parity in range(2):
        base = parity * own - halo
        for part in range(parts):
            total = jnp.zeros((SUB, LANE), jnp.float32)
            for f in range(len(lines)):
                amount = (f + 1) * window - base

                def slanted(h):
                    flat = spin(blocks[f][h % parts], amount)
                    return pltpu.roll(flat, 0, 1, stride=window, stride_axis=0)

                value = slanted(part)
                if parity == 0:
                    value = jnp.where((sub == SUB - 1) & (spot < halo), slanted(part - 1), value)
                else:
                    value = jnp.where((sub == 0) & (spot >= edge), slanted(part + 1), value)
                total = jnp.where(group == f, value, total)
            for m in range(SUB):
                target = plan.holder[2 * (part * SUB + m) + parity]
                at = target * plan.inward + plan.inward - 1
                out_ref[at : at + 1, :] = total[SUB - 1 - m : SUB - m]


def totals_of(ref):
    return jnp.sum(ref[...], axis=0, keepdims=True) * (1.0 / (damping * damping))


def pick(totals, k):
    lane = lane_of(totals.shape)
    value = jnp.sum(jnp.where(lane == k, totals, 0.0), axis=1, keepdims=True)
    return jnp.broadcast_to(value, (1, LANE))


class Scalars:
    def __init__(self, sums):
        self.norms = []
        self.scale = []
        self.cross = {}
        self.inner = {}
        self.taken = {}
        self.below = []
        for j, totals in enumerate(sums):
            norm = pick(totals, 0)
            self.norms.append(norm)
            if j == 0:
                self.beta = jnp.sqrt(norm + epsilon)
                self.scale.append(1.0 / self.beta)
            else:
                before = self.scale[j - 1]
                length = jnp.sqrt(before * before * norm + epsilon)
                self.below.append(length)
                self.scale.append(before / length)
            for i in range(j):
                self.cross[i, j] = pick(totals, 1 + i)
            for i in range(j + 1):
                self.inner[i, j] = pick(totals, KRYLOV + i)
                self.taken[i, j] = self.scale[i] * self.scale[i] * self.inner[i, j]

    def finish(self, square):
        last = KRYLOV - 1
        for i in range(KRYLOV):
            square = square - 2.0 * self.taken[i, last] * self.inner[i, last]
            for k in range(KRYLOV):
                pair = self.norms[i] if i == k else self.cross[min(i, k), max(i, k)]
                square = square + self.taken[i, last] * self.taken[k, last] * pair
        scale = self.scale[last]
        self.below.append(jnp.sqrt(jnp.maximum(scale * scale * square, 0.0) + epsilon))
        zero = jnp.zeros_like(self.beta)
        hessen = [[zero] * KRYLOV for row in range(KRYLOV + 1)]
        for j in range(KRYLOV):
            for i in range(j + 1):
                hessen[i][j] = self.scale[i] * self.scale[j] * self.inner[i, j]
            hessen[j + 1][j] = self.below[j]
        ortho = []
        upper = [[None] * KRYLOV for row in range(KRYLOV)]
        for column in range(KRYLOV):
            current = [hessen[row][column] for row in range(KRYLOV + 1)]
            for row in range(column):
                factor = sum(a * b for a, b in zip(ortho[row], current))
                upper[row][column] = factor
                current = [b - factor * a for a, b in zip(ortho[row], current)]
            length = jnp.sqrt(sum(b * b for b in current))
            upper[column][column] = length
            ortho.append([b / length for b in current])
        values = [None] * KRYLOV
        for row in reversed(range(KRYLOV)):
            accum = ortho[row][0] * self.beta
            for later in range(row + 1, KRYLOV):
                accum = accum - upper[row][later] * values[later]
            values[row] = accum / upper[row][row]
        return [values[j] * self.scale[j] for j in range(KRYLOV)]


def coefficients(plan, recv_ref, strip, table_ref):
    window = plan.window
    lane = lane_of((SUB, LANE))
    stride = plan.space * plan.inward
    lines = [
        recv_ref[pl.ds(s * plan.inward + plan.inward - 1, SUB, stride), :]
        for s in range(plan.space)
    ]
    fields = []
    for f in range(3):
        parts = []
        for line in lines:
            part = jnp.where(lane < window, spin(line, -f * window), 0.0)
            reach = window
            while reach < LANE:
                part = part + spin(part, reach)
                reach *= 2
            parts.append(part)
        fields.append(jnp.concatenate(parts, axis=0))
    diff, vel_col, vel_row = fields
    shape = (plan.rows, LANE)
    row = lax.broadcasted_iota(jnp.int32, shape, 0)
    col = strip * plan.own - plan.halo + lane_of(shape) % window
    center = 1.0 + 4.0 * diff
    table_ref[0] = damping * center
    table_ref[1] = 1.0 / center
    table_ref[2] = jnp.where(row > 0, damping * (diff + vel_row), 0.0)
    table_ref[3] = jnp.where(row < plan.rows - 1, damping * (diff - vel_row), 0.0)
    table_ref[4] = jnp.where(col > 0, damping * (diff + vel_col), 0.0)
    table_ref[5] = jnp.where(col < plan.cols - 1, damping * (diff - vel_col), 0.0)


def krylov_kernel(plan, j, *refs):
    refs = list(refs)
    strip = refs.pop(0)[0]
    here, window, rows, halo, own = plan.here, plan.window, plan.rows, plan.halo, plan.own
    slot = plan.slot
    final = j == KRYLOV - 1
    shape = (rows, LANE)
    lane = lane_of(shape)
    low_lane = lane_of((SUB, LANE))
    low_spot = low_lane % window
    even = strip % 2 == 0
    older = []
    if j == 0:
        recv_ref = refs.pop(0)
        table_ref = refs.pop(0)
    else:
        table_ref, image_ref, near_in, far_in = refs[:4]
        older = refs[4 : 4 + j]
        sums = refs[4 + j : 4 + 2 * j]
        refs = refs[4 + 2 * j :]
        scalars = Scalars([totals_of(ref) for ref in sums])
        taken = [scalars.taken[i, j - 1] for i in range(j)]
    q_ref, g_ref, w_ref = refs[:3]
    refs = refs[3:]
    near_ref = far_ref = None
    if not final:
        near_ref, far_ref = refs[:2]
        refs = refs[2:]
    sum_ref, y_ref = refs[:2]
    if j == 0:
        tail_ref = refs[2]
        coefficients(plan, recv_ref, strip, table_ref)
    center = table_ref[0]
    inverse = table_ref[1]
    north, south, west, east = (table_ref[2 + k] for k in range(4))
    zero = jnp.zeros(shape, jnp.float32)
    low_zero = jnp.zeros((SUB, LANE), jnp.float32)
    inner = slice(SUB, SUB + rows)

    def around(n, field):
        return (
            north * g_ref[n, SUB - 1 : SUB - 1 + rows, :]
            + south * g_ref[n, SUB + 1 : SUB + 1 + rows, :]
            + west * spin(field, 1)
            + east * spin(field, -1)
        )

    power = inverse
    for _ in range(int(math.log2(here))):
        power = power * power
    opening = jnp.where(lane < window, alpha_corner, 1.0)
    gains = [power * opening]
    reach = window
    while reach < LANE:
        gains.append(gains[-1] * spin(gains[-1], reach))
        reach *= 2
    closing = 1.0 / (1.0 - gains[-1])

    def entering(ends):
        total = spin(ends, window) * opening
        distance = window
        for gain in gains[:-1]:
            total = total + gain * spin(total, distance)
            distance *= 2
        return total * closing

    def settle(base, y):
        for k in range(UNROLL):
            y = (y_ref[base + k] + y) * inverse
            y_ref[base + k] = y
        return y

    for k in range(UNROLL):
        y_ref[k] = zero

    def blank(n):
        g_ref[n] = jnp.zeros((rows + 2 * SUB, LANE), jnp.float32)

    if j == 0:
        last_tile = plan.tiles - 1

        def tails(k, carry):
            for p in (2 * k, 2 * k + 1):
                for s in range(plan.space):
                    source = p * plan.space + s
                    total = low_zero
                    for a in range(last_tile):
                        tile = recv_ref[pl.ds(source * plan.inward + a * SUB, SUB), :]
                        moved = spin(tile, plan.spare * a - plan.used)
                        total = jnp.where(low_spot // plan.spare == a, moved, total)
                    tail_ref[source] = total
            return carry

        lax.fori_loop(0, plan.tm // 2, tails, 0)

        def first(a, y):
            whole = a < last_tile
            at = jnp.minimum(a, last_tile - 1) * SUB
            parts = []
            for s in range(plan.space):
                cut = []
                for p in range(plan.tm):
                    source = p * plan.space + s
                    tile = recv_ref[pl.ds(source * plan.inward + at, SUB), :]
                    cut.append(damping * jnp.where(whole, tile, tail_ref[source]))
                parts.append(exchange_blocks(cut, window, SUB))
            for i in range(SUB):
                n = a * SUB + i
                q = jnp.concatenate([part[i] for part in parts], axis=0)
                q_ref[n] = q
                y = (q + y) * inverse
                y_ref[UNROLL + n] = y
                blank(n)
            return y

        y = lax.fori_loop(0, plan.tiles, first, zero)
    else:
        near_side = jnp.where(even, halo + own, 0)
        far_side = jnp.where(even, 0, halo + own)
        near_mask = (low_spot >= near_side) & (low_spot < near_side + halo)
        far_mask = (low_spot >= far_side) & (low_spot < far_side + halo)

        def first(i, y):
            base = i * UNROLL
            y = settle(base, y)
            for k in range(UNROLL):
                n = base + k
                near, far = near_in[n], far_in[n]
                image = image_ref[n]
                parts = []
                for s in range(plan.space):
                    part = image[s * SUB : (s + 1) * SUB]
                    shift = LANE - slot * s
                    part = jnp.where(near_mask, pltpu.roll(near, (near_side + shift) % LANE, 1), part)
                    part = jnp.where(far_mask, pltpu.roll(far, (far_side + shift) % LANE, 1), part)
                    parts.append(part)
                q = jnp.concatenate(parts, axis=0)
                for t, ref in zip(taken, older):
                    q = q - t * ref[n]
                q_ref[n] = q
                y_ref[UNROLL + n] = q
                blank(n)
            return y

        y = settle(here, lax.fori_loop(0, here // UNROLL, first, zero))

    def sweep(_, ends):
        def body(i, carry):
            y, z = carry
            base = i * UNROLL
            olds = [y_ref[UNROLL + base + k] for k in range(UNROLL)]
            y = settle(base, y)
            for k in range(UNROLL):
                n = base + k
                z = z * inverse
                guess = (1.0 - damping) * g_ref[n, inner, :] + (olds[k] + z)
                g_ref[n, inner, :] = guess
                y_ref[UNROLL + n] = q_ref[n] + around(n, guess)
            return (y, z)

        y, _ = lax.fori_loop(0, here // UNROLL, body, (zero, entering(ends)))
        return settle(here, y)

    y = lax.fori_loop(0, SWEEPS - 1, sweep, y)
    start = entering(y)
    ending = (1.0 - damping) * g_ref[here - 1, inner, :] + (y + start * power)
    before = jnp.where(lane < window, 0.0, damping * spin(ending, window))

    near_from = jnp.where(even, own, halo)
    far_from = jnp.where(even, halo, own)

    def fold(block):
        return sum(block[s * SUB : (s + 1) * SUB] for s in range(plan.space))

    def gather(base, accs):
        for k in range(UNROLL):
            n = base + k
            image = w_ref[n]
            if not final:
                near = far = None
                for s in range(plan.space):
                    part = image[s * SUB : (s + 1) * SUB]
                    a = pltpu.roll(part, (slot * s - near_from + LANE) % LANE, 1)
                    b = pltpu.roll(part, (slot * s - far_from + LANE) % LANE, 1)
                    inside = low_spot // slot == s
                    near = a if near is None else jnp.where(inside, a, near)
                    far = b if far is None else jnp.where(inside, b, far)
                near_ref[n] = near
                far_ref[n] = far
            q = q_ref[n]
            olds = [ref[n] for ref in older]
            products = [q * q] + [old * q for old in olds] + [old * image for old in olds]
            products.append(q * image)
            if final:
                products.append(image * image)
            accs = [acc + fold(product) for acc, product in zip(accs, products)]
        return accs

    def last(i, carry):
        z, before, accs = carry
        accs = gather(jnp.maximum(i - 1, 0) * UNROLL, accs)
        accs = tuple(jnp.where(i > 0, acc, 0.0) for acc in accs)
        for k in range(UNROLL):
            n = i * UNROLL + k
            z = z * inverse
            guess = (1.0 - damping) * g_ref[n, inner, :] + (y_ref[UNROLL + n] + z)
            g_ref[n, inner, :] = guess
            w_ref[n] = center * guess - around(n, guess) - before
            before = damping * guess
        return (z, before, accs)

    fields = 2 * (j + 1) + (1 if final else 0)
    _, _, accs = lax.fori_loop(0, here // UNROLL, last, (start, before, (low_zero,) * fields))
    accs = gather(here - UNROLL, list(accs))
    places = [0] + [1 + i for i in range(j)] + [KRYLOV + i for i in range(j + 1)] + [2 * KRYLOV]
    owned = (low_spot >= halo) & (low_spot < halo + own)
    record = jnp.zeros((1, LANE), jnp.float32)
    record_lane = lane_of((1, LANE))
    for place, acc in zip(places, accs):
        value = jnp.sum(jnp.where(owned, acc, 0.0), axis=0, keepdims=True)
        value = jnp.sum(value, axis=1, keepdims=True)
        record = jnp.where(record_lane == place, value, record)
    sum_ref[...] = jnp.broadcast_to(record, sum_ref.shape)


def combine_kernel(plan, *refs):
    z_refs = refs[:KRYLOV]
    sums = refs[KRYLOV : 2 * KRYLOV]
    out_ref = refs[-1]
    totals = [totals_of(ref) for ref in sums]
    along = Scalars(totals).finish(pick(totals[-1], 2 * KRYLOV))
    own, halo, window, groups = plan.own, plan.halo, plan.window, plan.groups
    lane = lane_of((SUB, LANE))
    front = lane % window < own
    size = plan.outward

    def start_of(p, s):
        return (p * plan.space + s) * size

    def value(n, s):
        here = slice((s + 1) * SUB, (s + 2) * SUB)
        return sum(c * ref[n, here, :] for c, ref in zip(along, z_refs))

    def body(aa, carry):
        for s in range(plan.space):
            pieces = []
            for i in range(SUB):
                n = aa * 2 * SUB + 2 * i
                pieces.append(
                    jnp.where(front, spin(value(n, s), -halo), spin(value(n + 1, s), own - halo))
                )
            for p, piece in enumerate(exchange_blocks(pieces, window, SUB)):
                out_ref[pl.ds(start_of(p, s) + aa * SUB, SUB), :] = piece
                if s + 1 < plan.space:
                    at = start_of(p, s + 1) + groups * SUB + aa
                    out_ref[pl.ds(at, 1), :] = piece[SUB - 1 :]
                if s > 0:
                    at = start_of(p, s - 1) + groups * SUB + groups + aa
                    out_ref[pl.ds(at, 1), :] = piece[:1]
        return carry

    lax.fori_loop(0, groups, body, 0)
    nothing = jnp.zeros((groups, LANE), jnp.float32)
    sub = lax.broadcasted_iota(jnp.int32, (SUB, LANE), 0)
    for p in range(plan.tm):
        at = start_of(p, 0) + groups * SUB
        out_ref[at : at + groups, :] = nothing
        at = start_of(p, plan.space - 1) + groups * SUB + groups
        out_ref[at : at + groups, :] = nothing
    for s in range(plan.space):
        ending = value(plan.here - 1, s)
        for p in range(plan.tm):
            line = nothing[:1]
            if p > 0:
                turned = spin(ending, -(p - 1) * window - halo)
                turned = pltpu.roll(turned, 0, 1, stride=own, stride_axis=0)
                line = jnp.sum(jnp.where(lane // own == sub, turned, 0.0), axis=0, keepdims=True)
            at = start_of(p, s) + size - 1
            out_ref[at : at + 1, :] = line


def finish_kernel(plan, recv_ref, right_ref, diff_ref, vel_ref, out_ref, rest_ref, rim_ref):
    groups, own, size = plan.groups, plan.own, plan.outward
    count = LANE // own
    parts = plan.cols // LANE
    shape = (SUB, plan.cols)
    lane = lane_of((SUB, LANE))
    diff, vel_col, vel_row = diff_ref[...], vel_ref[0], vel_ref[1]
    col = lane_of(shape)
    sub = lax.broadcasted_iota(jnp.int32, shape, 0)
    center = 1.0 + 4.0 * diff
    north = diff + vel_row
    south = diff - vel_row
    west = jnp.where(col > 0, diff + vel_col, 0.0)
    east = jnp.where(col < plan.cols - 1, diff - vel_col, 0.0)

    def start_of(part, m):
        return plan.holder[part * count + m] * size

    def spread(offset):
        wide = []
        for part in range(parts):
            pieces = [
                recv_ref[pl.ds(start_of(part, m) + offset, SUB), :] for m in range(count)
            ]
            wide.append(exchange_blocks(pieces, own, 4))
        return [jnp.concatenate(pair, axis=1) for pair in zip(*wide)]

    for i, field in enumerate(spread(groups * SUB)):
        rim_ref[i] = field
    halves = []
    row = lax.broadcasted_iota(jnp.int32, (SUB, LANE), 0)
    for part in range(parts):
        tiles = []
        for first in range(0, count, SUB):
            tile = jnp.zeros((SUB, LANE), jnp.float32)
            for q in range(SUB):
                at = start_of(part, first + q) + size - 1
                line = jnp.broadcast_to(recv_ref[at : at + 1, :], (SUB, LANE))
                tile = jnp.where(row == q, line, tile)
            tile = spin(tile, first * own)
            tiles.append((first, pltpu.roll(tile, 0, 1, stride=own, stride_axis=0)))
        total = jnp.zeros((SUB, LANE), jnp.float32)
        for r in range(SUB):
            line = sum(
                jnp.where(lane // own == row + first, spin(tile, -r * own), 0.0)
                for first, tile in tiles
            )
            line = jnp.sum(line, axis=0, keepdims=True)
            total = jnp.where(row == r, jnp.broadcast_to(line, (SUB, LANE)), total)
        halves.append(total)
    before = jnp.concatenate(halves, axis=1)

    def body(aa, before):
        for i, field in enumerate(spread(aa * SUB)):
            n = aa * count + i
            above = rim_ref[i, pl.ds(aa, 1), :]
            below = rim_ref[i, pl.ds(groups + aa, 1), :]
            out_ref[n] = field
            around = (
                north * jnp.where(sub == 0, above, spin(field, 1, 0))
                + south * jnp.where(sub == SUB - 1, below, spin(field, -1, 0))
                + west * spin(field, 1)
                + east * spin(field, -1)
            )
            rest_ref[n] = right_ref[n] - (center * field - around - before)
            before = field
        return before

    lax.fori_loop(0, groups, body, before)


def call(kernel, shapes, operands, scalars=0, scratch=()):
    vmem = pl.BlockSpec(memory_space=pltpu.VMEM)
    smem = pl.BlockSpec(memory_space=pltpu.SMEM)
    return pl.pallas_call(
        kernel,
        out_shape=[jax.ShapeDtypeStruct(shape, jnp.float32) for shape in shapes],
        in_specs=[smem] * scalars + [vmem] * (len(operands) - scalars),
        out_specs=[vmem] * len(shapes),
        scratch_shapes=[pltpu.VMEM(shape, jnp.float32) for shape in scratch],
        compiler_params=pltpu.CompilerParams(vmem_limit_bytes=16 * 1024 * 1024),
    )(*operands)


def everyone(block, devices):
    lines = block.shape[0] // devices
    parts = block.reshape(devices, lines, 1, LANE)
    return lax.all_to_all(parts, AXES, split_axis=0, concat_axis=0, tiled=True).reshape(block.shape)


def strip_device(plan, right_side, diffusion, velocity):
    t = lax.axis_index("tm")
    s = lax.axis_index("space")
    strip = plan.strip_of(t, s).astype(jnp.int32).reshape(1)
    count = plan.devices
    hold = plan.holder
    near_route = []
    far_route = []
    for k in range(0, count, 2):
        near_route += [(hold[k], hold[k + 1]), (hold[k + 1], hold[k])]
    for k in range(1, count - 1, 2):
        far_route += [(hold[k], hold[k + 1]), (hold[k + 1], hold[k])]
    bind = lambda kernel, *more: (lambda *refs: kernel(plan, *more, *refs))
    full = (plan.here, plan.rows, LANE)
    padded = (plan.here, plan.rows + 2 * SUB, LANE)
    delayed = (plan.here + UNROLL, plan.rows, LANE)
    side = (plan.here, SUB, LANE)
    small = (count, LANE)
    given = [right_side, diffusion, velocity]
    sent = call(
        bind(pack_kernel),
        [(count * plan.inward, LANE)],
        [t.astype(jnp.int32).reshape(1), *given],
        scalars=1,
        scratch=[(count, SUB, LANE)],
    )[0]
    table, q, z, image, near, far, sums = call(
        bind(krylov_kernel, 0),
        [(6, plan.rows, LANE), full, padded, full, side, side, small],
        [strip, everyone(sent, count)],
        scalars=1,
        scratch=[delayed, (count, SUB, LANE)],
    )
    qs, zs, totals = [q], [z], []
    for j in range(1, KRYLOV):
        near = lax.ppermute(near, AXES, near_route)
        far = lax.ppermute(far, AXES, far_route)
        totals.append(everyone(sums, count))
        sides = [side, side] if j < KRYLOV - 1 else []
        q, z, image, *sides, sums = call(
            bind(krylov_kernel, j),
            [full, padded, full, *sides, small],
            [strip, table, image, near, far, *qs, *totals],
            scalars=1,
            scratch=[delayed],
        )
        if sides:
            near, far = sides
        qs.append(q)
        zs.append(z)
    totals.append(everyone(sums, count))
    packed = call(bind(combine_kernel), [(count * plan.outward, LANE)], [*zs, *totals])[0]
    shape = right_side.shape
    return tuple(
        call(
            bind(finish_kernel),
            [shape, shape],
            [everyone(packed, count), *given],
            scratch=[(2 * SUB, SUB, plan.cols)],
        )
    )


def per_device(mesh):
    def run(right_side, diffusion, velocity):
        rows = right_side.shape[1] * mesh.shape["space"]
        steps = right_side.shape[0] * mesh.shape["tm"]
        plan = Plan(mesh, steps, rows, right_side.shape[2])
        if plan.fits():
            return strip_device(plan, right_side, diffusion, velocity)
        return generic_device(right_side, diffusion, velocity)

    return run


def solution(mesh):
    placed = (P("tm", "space", None), P("space", None), P(None, "space", None))
    return jax.shard_map(
        per_device(mesh),
        mesh=mesh,
        in_specs=placed,
        out_specs=(P("tm", "space", None), P("tm", "space", None)),
        check_vma=False,
    )
```

```python
import math

import jax
import jax.numpy as jnp
from jax import lax
from jax.experimental import pallas as pl
from jax.experimental.pallas import tpu as pltpu
from jax.sharding import PartitionSpec as P

L = 512
KRYLOV = 3
SWEEPS = 3


alpha_corner = 0.05
damping = 0.8
epsilon = 1e-06
highest = lax.Precision.HIGHEST


def extended(block, sides, width):
    for axis, dim in sides:
        count = lax.axis_size(axis)
        forward = [(i, i + 1) for i in range(count - 1)]
        backward = [(target, source) for source, target in forward]
        low = lax.ppermute(
            lax.slice_in_dim(block, block.shape[dim] - width, None, axis=dim), axis, forward
        )
        high = lax.ppermute(lax.slice_in_dim(block, 0, width, axis=dim), axis, backward)
        block = jnp.concatenate([low, block, high], axis=dim)
    return block


def from_behind(block, axis, distance):
    devices = range(lax.axis_size(axis))
    route = [(i - distance, i) for i in devices if i - distance in devices]
    return lax.ppermute(block, axis, route)


def shifted(padded, row_dim, col_dim, rows, cols, row_start, col_start):
    piece = lax.slice_in_dim(padded, row_start, row_start + rows, axis=row_dim)
    return lax.slice_in_dim(piece, col_start, col_start + cols, axis=col_dim)


def stencil(field, padded, row_dim, col_dim, diffusion, velocity_col, velocity_row):
    rows = field.shape[row_dim]
    cols = field.shape[col_dim]
    north = shifted(padded, row_dim, col_dim, rows, cols, 0, 1)
    south = shifted(padded, row_dim, col_dim, rows, cols, 2, 1)
    west = shifted(padded, row_dim, col_dim, rows, cols, 1, 0)
    east = shifted(padded, row_dim, col_dim, rows, cols, 1, 2)
    return (
        (1.0 + 4.0 * diffusion) * field
        - diffusion * (north + south + west + east)
        + velocity_col * (east - west)
        + velocity_row * (south - north)
    )


def divided(real_part, imag_part, diag_real, diag_imag, modulus):
    return (
        damping * (real_part * diag_real + imag_part * diag_imag) / modulus,
        damping * (imag_part * diag_real - real_part * diag_imag) / modulus,
    )


def remainder(
    source_real, source_imag, image_real, image_imag, guess_real, guess_imag, shift_real, shift_imag
):
    return (
        source_real - (image_real - (shift_real * guess_real + shift_imag * guess_imag)),
        source_imag - (image_imag - (shift_real * guess_imag - shift_imag * guess_real)),
    )


def dft_tables(length):
    index = jnp.arange(length, dtype=jnp.int32)
    product = index[:, None] * index[None, :] % length
    angle = product.astype(jnp.float32) * (2.0 * math.pi / length)
    return (jnp.cos(angle), jnp.sin(angle))


def least_squares(hessen, beta):
    ortho = []
    upper = [[None] * KRYLOV for row in range(KRYLOV)]
    for column in range(KRYLOV):
        current = hessen[:, column]
        for row in range(column):
            factor = jnp.sum(ortho[row] * current)
            upper[row][column] = factor
            current = current - factor * ortho[row]
        length = jnp.sqrt(jnp.sum(current * current))
        upper[column][column] = length
        ortho.append(current / length)
    target = [ortho[row][0] * beta for row in range(KRYLOV)]
    values = [None] * KRYLOV
    for row in reversed(range(KRYLOV)):
        accum = target[row]
        for later in range(row + 1, KRYLOV):
            accum = accum - upper[row][later] * values[later]
        values[row] = accum / upper[row][row]
    return jnp.stack(values)


def generic_device(right_side, diffusion, velocity):
    steps_here = right_side.shape[0]
    devices_tm = lax.axis_size("tm")
    position = lax.axis_index("tm")
    log_decay = math.log(alpha_corner) / L
    decay = math.exp(log_decay)
    local_steps = position * steps_here + jnp.arange(steps_here, dtype=jnp.int32)
    times = local_steps.astype(jnp.float32)
    weights = jnp.exp(times * log_decay)[:, None, None]
    unweights = jnp.exp(-times * log_decay)[:, None, None]
    cosine, sine = dft_tables(L)
    velocity_col = velocity[0]
    velocity_row = velocity[1]
    width = right_side.shape[2] // devices_tm
    start = position * width
    diff_strip = lax.dynamic_slice_in_dim(diffusion, start, width, 1)[:, :, None]
    col_strip = lax.dynamic_slice_in_dim(velocity_col, start, width, 1)[:, :, None]
    row_strip = lax.dynamic_slice_in_dim(velocity_row, start, width, 1)[:, :, None]
    angles = jnp.arange(L, dtype=jnp.int32).astype(jnp.float32) * (2.0 * math.pi / L)
    shift_real = decay * jnp.cos(angles)
    shift_imag = decay * jnp.sin(angles)
    diag_real = 1.0 + 4.0 * diff_strip - shift_real
    modulus = diag_real * diag_real + shift_imag * shift_imag

    def forward(block):
        real_part = jnp.dot(block, cosine, precision=highest)
        imag_part = -jnp.dot(block, sine, precision=highest)
        return jnp.concatenate([real_part, imag_part], axis=2)

    total = lax.psum(jnp.sum(right_side * right_side), ("tm", "space"))
    beta = jnp.sqrt(total + epsilon)
    basis = [right_side / beta]
    prepared = []
    hessen = jnp.zeros((KRYLOV + 1, KRYLOV), jnp.float32)
    for column in range(KRYLOV):
        moved = jnp.transpose(basis[column] * weights, (1, 2, 0))
        spectrum = forward(lax.all_to_all(moved, "tm", split_axis=1, concat_axis=2, tiled=True))
        source_real = spectrum[:, :, :L]
        source_imag = spectrum[:, :, L:]
        guess_real, guess_imag = divided(source_real, source_imag, diag_real, shift_imag, modulus)
        for sweep in range(SWEEPS - 1):
            joined = jnp.concatenate([guess_real, guess_imag], axis=2)
            padded = extended(joined, (("tm", 1), ("space", 0)), 1)
            image = stencil(joined, padded, 0, 1, diff_strip, col_strip, row_strip)
            left_real, left_imag = remainder(
                source_real,
                source_imag,
                image[:, :, :L],
                image[:, :, L:],
                guess_real,
                guess_imag,
                shift_real,
                shift_imag,
            )
            step_real, step_imag = divided(left_real, left_imag, diag_real, shift_imag, modulus)
            guess_real = guess_real + step_real
            guess_imag = guess_imag + step_imag
        back = (
            jnp.dot(guess_real, cosine, precision=highest)
            - jnp.dot(guess_imag, sine, precision=highest)
        ) / L
        back = lax.all_to_all(back, "tm", split_axis=2, concat_axis=1, tiled=True)
        direction = jnp.transpose(back, (2, 0, 1)) * unweights
        prepared.append(direction)
        apply_padded = extended(direction, (("space", 1),), 1)
        apply_padded = jnp.pad(apply_padded, ((0, 0), (0, 0), (1, 1)))
        apply_image = stencil(direction, apply_padded, 1, 2, diffusion, velocity_col, velocity_row)
        earlier = from_behind(direction[-1:], "tm", 1)
        image = apply_image - jnp.concatenate([earlier, direction[:-1]], axis=0)
        local = jnp.stack([jnp.sum(vector * image) for vector in basis])
        projections = lax.psum(local, ("tm", "space"))
        for row in range(column + 1):
            image = image - projections[row] * basis[row]
        squares = lax.psum(jnp.sum(image * image), ("tm", "space"))
        length = jnp.sqrt(squares + epsilon)
        hessen = hessen.at[: column + 1, column].set(projections)
        hessen = hessen.at[column + 1, column].set(length)
        basis.append(image / length)
    coeffs = least_squares(hessen, beta)
    solution = prepared[0] * coeffs[0]
    for column in range(1, KRYLOV):
        solution = solution + prepared[column] * coeffs[column]
    first = (jnp.arange(KRYLOV + 1) == 0).astype(jnp.float32)
    target = beta * first - jnp.sum(hessen * coeffs[None, :], axis=1)
    residual = basis[0] * target[0]
    for row in range(1, KRYLOV + 1):
        residual = residual + basis[row] * target[row]
    return (solution, residual)


SUB = 8
LANE = 128
AXES = ("tm", "space")
UNROLL = 16


def spin(block, amount, axis=1):
    return pltpu.roll(block, amount % block.shape[axis], axis)


def lane_of(shape):
    return lax.broadcasted_iota(jnp.int32, shape, 1)


def exchange_blocks(pieces, width, radix):
    pieces = list(pieces)
    lane = lane_of(pieces[0].shape)
    step = 1
    while step < len(pieces):
        digit = lane // (width * step) % radix
        result = list(pieces)
        for i in range(len(pieces)):
            e = i // step % radix
            total = None
            for d in range(radix):
                moved = pieces[i + (d - e) * step]
                if d != e:
                    moved = spin(moved, (d - e) * step * width)
                total = moved if total is None else jnp.where(digit == d, moved, total)
            result[i] = total
        pieces = result
        step *= radix
    return pieces


class Plan:
    def __init__(self, mesh, steps, rows, cols):
        self.tm = mesh.shape["tm"]
        self.space = mesh.shape["space"]
        self.devices = self.tm * self.space
        self.steps = steps
        self.rows = rows
        self.cols = cols
        self.here = steps // self.tm
        self.window = LANE // self.tm
        self.own = cols // self.devices
        self.halo = SWEEPS
        self.slot = self.window // self.space
        self.used = self.own + 2 * self.halo
        self.spare = self.window - self.used
        self.tiles = self.here // SUB
        self.inward = (self.tiles - 1) * SUB + 1
        self.groups = self.here // (2 * SUB)
        self.outward = self.groups * SUB + 2 * self.groups + 1
        self.ring = [self.strip_of(d // self.space, d % self.space) for d in range(self.devices)]
        self.holder = [self.ring.index(j) for j in range(self.devices)]

    def fits(self):
        return (
            LANE % self.tm == 0
            and self.tm == SUB
            and self.rows == SUB * self.space
            and self.cols % self.devices == 0
            and self.cols == 2 * LANE
            and self.steps % (self.tm * 2 * SUB) == 0
            and self.window == 2 * self.own
            and self.spare * (self.tiles - 1) == self.used
            and self.here % UNROLL == 0
            and self.groups * 2 == SUB
            and self.slot >= self.halo
            and self.space % 2 == 0
            and KRYLOV == 3
            and self.tiles % (UNROLL // SUB) == 0
        )

    def strip_of(self, t, s):
        turn = t ^ ((t >> 1) & 1)
        half = self.space // 2
        x, core = s // 2, s % 2
        odd = turn % 2
        return (turn * half + x + odd * (half - 1 - 2 * x)) * 2 + core


def pack_kernel(plan, place_ref, right_ref, diff_ref, vel_ref, out_ref, tail_ref):
    window, own, halo = plan.window, plan.own, plan.halo
    parts = plan.cols // LANE
    lane = lane_of((SUB, LANE))
    group, spot = lane // window, lane % window
    edge = LANE - (SUB - 1) * window - own + halo

    def strips():
        for parity in range(2):
            for part in range(parts):
                for m in range(SUB):
                    yield parity, part, m, plan.holder[2 * (part * SUB + m) + parity]

    def body(k, carry):
        a = plan.tiles - 1 - k
        fields = [right_ref[a * SUB + i] for i in range(SUB)]
        cache = {}

        def turned(i, part, amount):
            key = (i, part % parts, amount % LANE)
            if key not in cache:
                block = fields[i][:, key[1] * LANE : (key[1] + 1) * LANE]
                cache[key] = spin(block, amount)
            return cache[key]

        pieces = []
        for parity, part, m, _ in strips():
            base = parity * own - halo
            total = None
            for i in range(SUB):
                amount = window * (i - m) - base
                value = turned(i, part, amount)
                if parity == 0 and m == 0:
                    value = jnp.where(spot < halo, turned(i, part - 1, amount), value)
                if parity == 1 and m == SUB - 1:
                    value = jnp.where(spot >= edge, turned(i, part + 1, amount), value)
                total = value if total is None else jnp.where(group == i, value, total)
            pieces.append(total)

        @pl.when(k == 0)
        def _():
            for index, piece in enumerate(pieces):
                tail_ref[index] = piece

        @pl.when(k > 0)
        def _():
            amount = plan.used - plan.spare * a
            for index, (_, _, _, target) in enumerate(strips()):
                tail = pltpu.roll(tail_ref[index], amount, 1)
                piece = jnp.where(spot >= plan.used, tail, pieces[index])
                out_ref[pl.ds(target * plan.inward + a * SUB, SUB), :] = piece

        return carry

    lax.fori_loop(0, plan.tiles, body, 0)
    row = pl.ds(place_ref[0], 1)
    lines = [diff_ref[row, :], vel_ref[0, row, :], vel_ref[1, row, :]]
    sub = lax.broadcasted_iota(jnp.int32, (SUB, LANE), 0)
    blocks = [
        [jnp.broadcast_to(line[:, h * LANE : (h + 1) * LANE], (SUB, LANE)) for h in range(parts)]
        for line in lines
    ]
    for parity in range(2):
        base = parity * own - halo
        for part in range(parts):
            total = jnp.zeros((SUB, LANE), jnp.float32)
            for f in range(len(lines)):
                amount = (f + 1) * window - base

                def slanted(h):
                    flat = spin(blocks[f][h % parts], amount)
                    return pltpu.roll(flat, 0, 1, stride=window, stride_axis=0)

                value = slanted(part)
                if parity == 0:
                    value = jnp.where((sub == SUB - 1) & (spot < halo), slanted(part - 1), value)
                else:
                    value = jnp.where((sub == 0) & (spot >= edge), slanted(part + 1), value)
                total = jnp.where(group == f, value, total)
            for m in range(SUB):
                target = plan.holder[2 * (part * SUB + m) + parity]
                at = target * plan.inward + plan.inward - 1
                out_ref[at : at + 1, :] = total[SUB - 1 - m : SUB - m]


def totals_of(ref):
    return jnp.sum(ref[...], axis=0, keepdims=True) * (1.0 / (damping * damping))


def pick(totals, k):
    lane = lane_of(totals.shape)
    value = jnp.sum(jnp.where(lane == k, totals, 0.0), axis=1, keepdims=True)
    return jnp.broadcast_to(value, (1, LANE))


def middle(totals):
    aa, ab, bb, ac, bc = (pick(totals, k) for k in range(5))
    scale = 1.0 / (aa + epsilon)
    drop = scale * ab
    norm = jnp.maximum(bb - drop * (2.0 * ab - drop * aa), 1e-5 * bb)
    over = ac - drop * ab
    along = bc - drop * (bb + ac - drop * ab)
    return aa, drop, scale * over, scale * along / (scale * norm + epsilon)


def iterate(middle_totals, totals):
    aa, drop, over, along = middle(middle_totals)
    pairs = [(0, 1), (1, 1), (0, 2), (1, 2), (2, 2), (0, 3), (1, 3), (2, 3), (3, 3)]
    gram = {(0, 0): aa}
    for k, (i, j) in enumerate(pairs):
        gram[i, j] = gram[j, i] = pick(totals, k)
    zero = jnp.zeros_like(aa)
    one = jnp.ones_like(aa)
    images = [[drop, one, zero, zero], [over, along, one, zero], [zero, zero, zero, one]]
    size = KRYLOV + 1

    def product(left, right):
        return sum(left[i] * right[j] * gram[i, j] for i in range(size) for j in range(size))

    beta = jnp.sqrt(aa + epsilon)
    basis = [[1.0 / beta, zero, zero, zero]]
    hessen = [[zero] * KRYLOV for row in range(size)]
    for j in range(KRYLOV):
        image = [sum(basis[j][k] * images[k][i] for k in range(KRYLOV)) for i in range(size)]
        found = [product(basis[i], image) for i in range(j + 1)]
        for i in range(j + 1):
            hessen[i][j] = found[i]
            image = [w - found[i] * v for w, v in zip(image, basis[i])]
        length = jnp.sqrt(jnp.maximum(product(image, image), 0.0) + epsilon)
        hessen[j + 1][j] = length
        basis.append([w / length for w in image])
    ortho = []
    upper = [[None] * KRYLOV for row in range(KRYLOV)]
    for column in range(KRYLOV):
        current = [hessen[row][column] for row in range(size)]
        for row in range(column):
            factor = sum(x * y for x, y in zip(ortho[row], current))
            upper[row][column] = factor
            current = [y - factor * x for x, y in zip(ortho[row], current)]
        length = jnp.sqrt(sum(y * y for y in current))
        upper[column][column] = length
        ortho.append([y / length for y in current])
    values = [None] * KRYLOV
    for row in reversed(range(KRYLOV)):
        accum = ortho[row][0] * beta
        for later in range(row + 1, KRYLOV):
            accum = accum - upper[row][later] * values[later]
        values[row] = accum / upper[row][row]
    weights = [sum(values[j] * basis[j][k] for j in range(KRYLOV)) for k in range(KRYLOV)]
    weights[0] = weights[0] - drop * weights[1]
    return weights


def coefficients(plan, recv_ref, strip, table_ref):
    window = plan.window
    lane = lane_of((SUB, LANE))
    stride = plan.space * plan.inward
    lines = [
        recv_ref[pl.ds(s * plan.inward + plan.inward - 1, SUB, stride), :]
        for s in range(plan.space)
    ]
    fields = []
    for f in range(3):
        parts = []
        for line in lines:
            part = None
            for g in range(plan.tm):
                moved = spin(line, (g - f) * window)
                part = moved if g == 0 else jnp.where(lane // window == g, moved, part)
            parts.append(part)
        fields.append(jnp.concatenate(parts, axis=0))
    diff, vel_col, vel_row = fields
    shape = (plan.rows, LANE)
    row = lax.broadcasted_iota(jnp.int32, shape, 0)
    col = strip * plan.own - plan.halo + lane_of(shape) % window
    center = 1.0 + 4.0 * diff
    table_ref[0] = damping * center
    table_ref[1] = 1.0 / center
    table_ref[2] = jnp.where(row > 0, damping * (diff + vel_row), 0.0)
    table_ref[3] = jnp.where(row < plan.rows - 1, damping * (diff - vel_row), 0.0)
    table_ref[4] = jnp.where(col > 0, damping * (diff + vel_col), 0.0)
    table_ref[5] = jnp.where(col < plan.cols - 1, damping * (diff - vel_col), 0.0)


def krylov_kernel(plan, j, *refs):
    refs = list(refs)
    strip = refs.pop(0)[0]
    here, window, rows, halo, own = plan.here, plan.window, plan.rows, plan.halo, plan.own
    slot = plan.slot
    final = j == KRYLOV - 1
    shape = (rows, LANE)
    lane = lane_of(shape)
    low_lane = lane_of((SUB, LANE))
    low_spot = low_lane % window
    even = strip % 2 == 0
    if j == 0:
        recv_ref, table_ref, q_ref, g_ref, w_ref, near_ref, far_ref, y_ref, tail_ref = refs
        coefficients(plan, recv_ref, strip, table_ref)
    elif not final:
        table_ref, image_ref, near_in, far_in, first_ref = refs[:5]
        q_ref, g_ref, w_ref, near_ref, far_ref, sum_ref, y_ref = refs[5:]
    else:
        table_ref, image_ref, near_in, far_in, first_ref, second_ref, mid_ref = refs[:7]
        g_ref, sum_ref, y_ref, q_ref, w_ref, rest_ref = refs[7:]
        _, drop, over, along = middle(totals_of(mid_ref))
    center = table_ref[0]
    inverse = table_ref[1]
    north, south, west, east = (table_ref[2 + k] for k in range(4))
    zero = jnp.zeros(shape, jnp.float32)
    low_zero = jnp.zeros((SUB, LANE), jnp.float32)
    inner = slice(SUB, SUB + rows)

    def around(n, field):
        return (
            north * g_ref[n, SUB - 1 : SUB - 1 + rows, :]
            + south * g_ref[n, SUB + 1 : SUB + 1 + rows, :]
            + west * spin(field, 1)
            + east * spin(field, -1)
        )

    power = inverse
    for _ in range(int(math.log2(here))):
        power = power * power
    whole = power
    for _ in range(int(math.log2(plan.tm))):
        whole = whole * whole
    closing = 1.0 / (1.0 - alpha_corner * whole)

    def entering(ends):
        total = alpha_corner * ends
        for k in reversed(range(1, plan.tm)):
            back = spin(ends, k * window)
            total = total * power + jnp.where(lane < k * window, alpha_corner * back, back)
        return total * closing

    def settle(base, y):
        for k in range(UNROLL):
            y = (y_ref[base + k] + y) * inverse
            y_ref[base + k] = y
        return y

    for k in range(UNROLL):
        y_ref[k] = zero

    def blank(n):
        g_ref[n] = jnp.zeros((rows + 2 * SUB, LANE), jnp.float32)

    if j == 0:
        last_tile = plan.tiles - 1

        def tails(k, carry):
            for p in (2 * k, 2 * k + 1):
                for s in range(plan.space):
                    source = p * plan.space + s
                    total = low_zero
                    for a in range(last_tile):
                        tile = recv_ref[pl.ds(source * plan.inward + a * SUB, SUB), :]
                        moved = spin(tile, plan.spare * a - plan.used)
                        total = jnp.where(low_spot // plan.spare == a, moved, total)
                    tail_ref[source] = total
            return carry

        lax.fori_loop(0, plan.tm // 2, tails, 0)

        pair = UNROLL // SUB

        def first(k, y):
            parts = [[] for _ in range(pair)]
            for t in range(pair):
                a = k * pair + t
                whole = a < last_tile
                at = jnp.minimum(a, last_tile - 1) * SUB
                for s in range(plan.space):
                    cut = []
                    for p in range(plan.tm):
                        source = p * plan.space + s
                        tile = recv_ref[pl.ds(source * plan.inward + at, SUB), :]
                        cut.append(damping * jnp.where(whole, tile, tail_ref[source]))
                    parts[t].append(exchange_blocks(cut, window, 2))
            for t in range(pair):
                for i in range(SUB):
                    n = k * UNROLL + t * SUB + i
                    q = jnp.concatenate([part[i] for part in parts[t]], axis=0)
                    q_ref[n] = q
                    y = (q + y) * inverse
                    y_ref[UNROLL + n] = y
                    blank(n)
            return y

        y = lax.fori_loop(0, plan.tiles // pair, first, zero)
    else:
        near_side = jnp.where(even, halo + own, 0)
        far_side = jnp.where(even, 0, halo + own)
        near_mask = (low_spot >= near_side) & (low_spot < near_side + halo)
        far_mask = (low_spot >= far_side) & (low_spot < far_side + halo)

        def first(i, y):
            base = i * UNROLL
            y = settle(base, y)
            for k in range(UNROLL):
                n = base + k
                near, far = near_in[n], far_in[n]
                image = image_ref[n]
                parts = []
                for s in range(plan.space):
                    part = image[s * SUB : (s + 1) * SUB]
                    shift = LANE - slot * s
                    part = jnp.where(near_mask, pltpu.roll(near, (near_side + shift) % LANE, 1), part)
                    part = jnp.where(far_mask, pltpu.roll(far, (far_side + shift) % LANE, 1), part)
                    parts.append(part)
                q = jnp.concatenate(parts, axis=0)
                if final:
                    start, later = first_ref[n], second_ref[n]
                    rest = later - drop * start
                    rest_ref[n] = rest
                    q = (q - drop * later) - over * start - along * rest
                q_ref[n] = q
                y_ref[UNROLL + n] = q
                blank(n)
            return y

        y = settle(here, lax.fori_loop(0, here // UNROLL, first, zero))

    def sweep(_, ends):
        def body(i, carry):
            y, z = carry
            base = i * UNROLL
            olds = [y_ref[UNROLL + base + k] for k in range(UNROLL)]
            y = settle(base, y)
            for k in range(UNROLL):
                n = base + k
                z = z * inverse
                guess = (1.0 - damping) * g_ref[n, inner, :] + (olds[k] + z)
                g_ref[n, inner, :] = guess
                y_ref[UNROLL + n] = q_ref[n] + around(n, guess)
            return (y, z)

        y, _ = lax.fori_loop(0, here // UNROLL, body, (zero, entering(ends)))
        return settle(here, y)

    y = lax.fori_loop(0, SWEEPS - 1, sweep, y)
    start = entering(y)
    ending = (1.0 - damping) * g_ref[here - 1, inner, :] + (y + start * power)
    before = jnp.where(lane < window, 0.0, damping * spin(ending, window))

    near_from = jnp.where(even, own, halo)
    far_from = jnp.where(even, halo, own)

    def fold(block):
        return sum(block[s * SUB : (s + 1) * SUB] for s in range(plan.space))

    size = KRYLOV + 1

    def gather(base, accs):
        for k in range(UNROLL):
            n = base + k
            image = w_ref[n]
            if not final:
                near = far = None
                for s in range(plan.space):
                    part = image[s * SUB : (s + 1) * SUB]
                    a = pltpu.roll(part, (slot * s - near_from + LANE) % LANE, 1)
                    b = pltpu.roll(part, (slot * s - far_from + LANE) % LANE, 1)
                    inside = low_spot // slot == s
                    near = a if near is None else jnp.where(inside, a, near)
                    far = b if far is None else jnp.where(inside, b, far)
                near_ref[n] = near
                far_ref[n] = far
            if j == 0:
                continue
            q = q_ref[n]
            start = first_ref[n]
            if not final:
                pairs = [(start, start), (start, q), (q, q), (start, image), (q, image)]
            else:
                rest = rest_ref[n]
                held = [start, rest, q, image]
                pairs = [(held[i], held[k]) for k in range(1, size) for i in range(k + 1)]
            accs = [acc + fold(x * y) for acc, (x, y) in zip(accs, pairs)]
        return accs

    def last(i, carry):
        z, before, accs = carry
        accs = gather(jnp.maximum(i - 1, 0) * UNROLL, accs)
        accs = tuple(jnp.where(i > 0, acc, 0.0) for acc in accs)
        for k in range(UNROLL):
            n = i * UNROLL + k
            z = z * inverse
            guess = (1.0 - damping) * g_ref[n, inner, :] + (y_ref[UNROLL + n] + z)
            g_ref[n, inner, :] = guess
            w_ref[n] = center * guess - around(n, guess) - before
            before = damping * guess
        return (z, before, accs)

    fields = (0, 5, 9)[j]
    _, _, accs = lax.fori_loop(0, here // UNROLL, last, (start, before, (low_zero,) * fields))
    accs = gather(here - UNROLL, list(accs))
    if j == 0:
        return
    owned = (low_spot >= halo) & (low_spot < halo + own)
    record = jnp.zeros((1, LANE), jnp.float32)
    record_lane = lane_of((1, LANE))
    for place, acc in enumerate(accs):
        value = jnp.sum(jnp.where(owned, acc, 0.0), axis=0, keepdims=True)
        value = jnp.sum(value, axis=1, keepdims=True)
        record = jnp.where(record_lane == place, value, record)
    sum_ref[...] = jnp.broadcast_to(record, sum_ref.shape)


def combine_kernel(plan, *refs):
    z_refs = refs[:KRYLOV]
    mid_ref, end_ref, out_ref = refs[KRYLOV:]
    along = iterate(totals_of(mid_ref), totals_of(end_ref))
    own, halo, window, groups = plan.own, plan.halo, plan.window, plan.groups
    lane = lane_of((SUB, LANE))
    front = lane % window < own
    size = plan.outward

    def start_of(p, s):
        return (p * plan.space + s) * size

    def value(n, s):
        here = slice((s + 1) * SUB, (s + 2) * SUB)
        return sum(c * ref[n, here, :] for c, ref in zip(along, z_refs))

    def body(aa, carry):
        for s in range(plan.space):
            pieces = []
            for i in range(SUB):
                n = aa * 2 * SUB + 2 * i
                pieces.append(
                    jnp.where(front, spin(value(n, s), -halo), spin(value(n + 1, s), own - halo))
                )
            for p, piece in enumerate(exchange_blocks(pieces, window, SUB)):
                out_ref[pl.ds(start_of(p, s) + aa * SUB, SUB), :] = piece
                if s + 1 < plan.space:
                    at = start_of(p, s + 1) + groups * SUB + aa
                    out_ref[pl.ds(at, 1), :] = piece[SUB - 1 :]
                if s > 0:
                    at = start_of(p, s - 1) + groups * SUB + groups + aa
                    out_ref[pl.ds(at, 1), :] = piece[:1]
        return carry

    lax.fori_loop(0, groups, body, 0)
    nothing = jnp.zeros((groups, LANE), jnp.float32)
    sub = lax.broadcasted_iota(jnp.int32, (SUB, LANE), 0)
    for p in range(plan.tm):
        at = start_of(p, 0) + groups * SUB
        out_ref[at : at + groups, :] = nothing
        at = start_of(p, plan.space - 1) + groups * SUB + groups
        out_ref[at : at + groups, :] = nothing
    for s in range(plan.space):
        ending = value(plan.here - 1, s)
        for p in range(plan.tm):
            line = nothing[:1]
            if p > 0:
                turned = spin(ending, -(p - 1) * window - halo)
                turned = pltpu.roll(turned, 0, 1, stride=own, stride_axis=0)
                line = jnp.sum(jnp.where(lane // own == sub, turned, 0.0), axis=0, keepdims=True)
            at = start_of(p, s) + size - 1
            out_ref[at : at + 1, :] = line


def finish_kernel(plan, recv_ref, right_ref, diff_ref, vel_ref, out_ref, rest_ref, rim_ref):
    groups, own, size = plan.groups, plan.own, plan.outward
    count = LANE // own
    parts = plan.cols // LANE
    shape = (SUB, plan.cols)
    lane = lane_of((SUB, LANE))
    diff, vel_col, vel_row = diff_ref[...], vel_ref[0], vel_ref[1]
    col = lane_of(shape)
    sub = lax.broadcasted_iota(jnp.int32, shape, 0)
    center = 1.0 + 4.0 * diff
    north = diff + vel_row
    south = diff - vel_row
    west = jnp.where(col > 0, diff + vel_col, 0.0)
    east = jnp.where(col < plan.cols - 1, diff - vel_col, 0.0)

    def start_of(part, m):
        return plan.holder[part * count + m] * size

    def spread(offset):
        wide = []
        for part in range(parts):
            pieces = [
                recv_ref[pl.ds(start_of(part, m) + offset, SUB), :] for m in range(count)
            ]
            wide.append(exchange_blocks(pieces, own, 4))
        return [jnp.concatenate(pair, axis=1) for pair in zip(*wide)]

    for i, field in enumerate(spread(groups * SUB)):
        rim_ref[i] = field
    halves = []
    row = lax.broadcasted_iota(jnp.int32, (SUB, LANE), 0)
    for part in range(parts):
        tiles = []
        for first in range(0, count, SUB):
            tile = jnp.zeros((SUB, LANE), jnp.float32)
            for q in range(SUB):
                at = start_of(part, first + q) + size - 1
                line = jnp.broadcast_to(recv_ref[at : at + 1, :], (SUB, LANE))
                tile = jnp.where(row == q, line, tile)
            tile = spin(tile, first * own)
            tiles.append((first, pltpu.roll(tile, 0, 1, stride=own, stride_axis=0)))
        total = jnp.zeros((SUB, LANE), jnp.float32)
        for r in range(SUB):
            line = sum(
                jnp.where(lane // own == row + first, spin(tile, -r * own), 0.0)
                for first, tile in tiles
            )
            line = jnp.sum(line, axis=0, keepdims=True)
            total = jnp.where(row == r, jnp.broadcast_to(line, (SUB, LANE)), total)
        halves.append(total)
    before = jnp.concatenate(halves, axis=1)

    def body(aa, before):
        for i, field in enumerate(spread(aa * SUB)):
            n = aa * count + i
            above = rim_ref[i, pl.ds(aa, 1), :]
            below = rim_ref[i, pl.ds(groups + aa, 1), :]
            out_ref[n] = field
            around = (
                north * jnp.where(sub == 0, above, spin(field, 1, 0))
                + south * jnp.where(sub == SUB - 1, below, spin(field, -1, 0))
                + west * spin(field, 1)
                + east * spin(field, -1)
            )
            rest_ref[n] = right_ref[n] - (center * field - around - before)
            before = field
        return before

    lax.fori_loop(0, groups, body, before)


def call(kernel, shapes, operands, scalars=0, scratch=()):
    vmem = pl.BlockSpec(memory_space=pltpu.VMEM)
    smem = pl.BlockSpec(memory_space=pltpu.SMEM)
    return pl.pallas_call(
        kernel,
        out_shape=[jax.ShapeDtypeStruct(shape, jnp.float32) for shape in shapes],
        in_specs=[smem] * scalars + [vmem] * (len(operands) - scalars),
        out_specs=[vmem] * len(shapes),
        scratch_shapes=[pltpu.VMEM(shape, jnp.float32) for shape in scratch],
        compiler_params=pltpu.CompilerParams(vmem_limit_bytes=16 * 1024 * 1024),
    )(*operands)


def everyone(block, devices):
    lines = block.shape[0] // devices
    parts = block.reshape(devices, lines, 1, LANE)
    return lax.all_to_all(parts, AXES, split_axis=0, concat_axis=0, tiled=True).reshape(block.shape)


def strip_device(plan, right_side, diffusion, velocity):
    t = lax.axis_index("tm")
    s = lax.axis_index("space")
    strip = plan.strip_of(t, s).astype(jnp.int32).reshape(1)
    count = plan.devices
    hold = plan.holder
    near_route = []
    far_route = []
    for k in range(0, count, 2):
        near_route += [(hold[k], hold[k + 1]), (hold[k + 1], hold[k])]
    for k in range(1, count - 1, 2):
        far_route += [(hold[k], hold[k + 1]), (hold[k + 1], hold[k])]
    bind = lambda kernel, *more: (lambda *refs: kernel(plan, *more, *refs))
    full = (plan.here, plan.rows, LANE)
    padded = (plan.here, plan.rows + 2 * SUB, LANE)
    delayed = (plan.here + UNROLL, plan.rows, LANE)
    side = (plan.here, SUB, LANE)
    small = (count, LANE)
    given = [right_side, diffusion, velocity]
    sent = call(
        bind(pack_kernel),
        [(count * plan.inward, LANE)],
        [t.astype(jnp.int32).reshape(1), *given],
        scalars=1,
        scratch=[(count, SUB, LANE)],
    )[0]
    table, q0, z0, image, near, far = call(
        bind(krylov_kernel, 0),
        [(6, plan.rows, LANE), full, padded, full, side, side],
        [strip, everyone(sent, count)],
        scalars=1,
        scratch=[delayed, (count, SUB, LANE)],
    )
    near = lax.ppermute(near, AXES, near_route)
    far = lax.ppermute(far, AXES, far_route)
    q1, z1, image, near, far, sums = call(
        bind(krylov_kernel, 1),
        [full, padded, full, side, side, small],
        [strip, table, image, near, far, q0],
        scalars=1,
        scratch=[delayed],
    )
    near = lax.ppermute(near, AXES, near_route)
    far = lax.ppermute(far, AXES, far_route)
    mid = everyone(sums, count)
    z2, sums = call(
        bind(krylov_kernel, 2),
        [padded, small],
        [strip, table, image, near, far, q0, q1, mid],
        scalars=1,
        scratch=[delayed, full, full, full],
    )
    end = everyone(sums, count)
    packed = call(bind(combine_kernel), [(count * plan.outward, LANE)], [z0, z1, z2, mid, end])[0]
    shape = right_side.shape
    return tuple(
        call(
            bind(finish_kernel),
            [shape, shape],
            [everyone(packed, count), *given],
            scratch=[(2 * SUB, SUB, plan.cols)],
        )
    )


def per_device(mesh):
    def run(right_side, diffusion, velocity):
        rows = right_side.shape[1] * mesh.shape["space"]
        steps = right_side.shape[0] * mesh.shape["tm"]
        plan = Plan(mesh, steps, rows, right_side.shape[2])
        if plan.fits():
            return strip_device(plan, right_side, diffusion, velocity)
        return generic_device(right_side, diffusion, velocity)

    return run


def solution(mesh):
    placed = (P("tm", "space", None), P("space", None), P(None, "space", None))
    return jax.shard_map(
        per_device(mesh),
        mesh=mesh,
        in_specs=placed,
        out_specs=(P("tm", "space", None), P("tm", "space", None)),
        check_vma=False,
    )
```

```python
import math

import jax
import jax.numpy as jnp
from jax import lax
from jax.experimental import pallas as pl
from jax.experimental.pallas import tpu as pltpu
from jax.sharding import PartitionSpec as P

L = 512
KRYLOV = 3
SWEEPS = 3


alpha_corner = 0.05
damping = 0.8
epsilon = 1e-06
highest = lax.Precision.HIGHEST


def extended(block, sides, width):
    for axis, dim in sides:
        count = lax.axis_size(axis)
        forward = [(i, i + 1) for i in range(count - 1)]
        backward = [(target, source) for source, target in forward]
        low = lax.ppermute(
            lax.slice_in_dim(block, block.shape[dim] - width, None, axis=dim), axis, forward
        )
        high = lax.ppermute(lax.slice_in_dim(block, 0, width, axis=dim), axis, backward)
        block = jnp.concatenate([low, block, high], axis=dim)
    return block


def from_behind(block, axis, distance):
    devices = range(lax.axis_size(axis))
    route = [(i - distance, i) for i in devices if i - distance in devices]
    return lax.ppermute(block, axis, route)


def shifted(padded, row_dim, col_dim, rows, cols, row_start, col_start):
    piece = lax.slice_in_dim(padded, row_start, row_start + rows, axis=row_dim)
    return lax.slice_in_dim(piece, col_start, col_start + cols, axis=col_dim)


def stencil(field, padded, row_dim, col_dim, diffusion, velocity_col, velocity_row):
    rows = field.shape[row_dim]
    cols = field.shape[col_dim]
    north = shifted(padded, row_dim, col_dim, rows, cols, 0, 1)
    south = shifted(padded, row_dim, col_dim, rows, cols, 2, 1)
    west = shifted(padded, row_dim, col_dim, rows, cols, 1, 0)
    east = shifted(padded, row_dim, col_dim, rows, cols, 1, 2)
    return (
        (1.0 + 4.0 * diffusion) * field
        - diffusion * (north + south + west + east)
        + velocity_col * (east - west)
        + velocity_row * (south - north)
    )


def divided(real_part, imag_part, diag_real, diag_imag, modulus):
    return (
        damping * (real_part * diag_real + imag_part * diag_imag) / modulus,
        damping * (imag_part * diag_real - real_part * diag_imag) / modulus,
    )


def remainder(
    source_real, source_imag, image_real, image_imag, guess_real, guess_imag, shift_real, shift_imag
):
    return (
        source_real - (image_real - (shift_real * guess_real + shift_imag * guess_imag)),
        source_imag - (image_imag - (shift_real * guess_imag - shift_imag * guess_real)),
    )


def dft_tables(length):
    index = jnp.arange(length, dtype=jnp.int32)
    product = index[:, None] * index[None, :] % length
    angle = product.astype(jnp.float32) * (2.0 * math.pi / length)
    return (jnp.cos(angle), jnp.sin(angle))


def least_squares(hessen, beta):
    ortho = []
    upper = [[None] * KRYLOV for row in range(KRYLOV)]
    for column in range(KRYLOV):
        current = hessen[:, column]
        for row in range(column):
            factor = jnp.sum(ortho[row] * current)
            upper[row][column] = factor
            current = current - factor * ortho[row]
        length = jnp.sqrt(jnp.sum(current * current))
        upper[column][column] = length
        ortho.append(current / length)
    target = [ortho[row][0] * beta for row in range(KRYLOV)]
    values = [None] * KRYLOV
    for row in reversed(range(KRYLOV)):
        accum = target[row]
        for later in range(row + 1, KRYLOV):
            accum = accum - upper[row][later] * values[later]
        values[row] = accum / upper[row][row]
    return jnp.stack(values)


def generic_device(right_side, diffusion, velocity):
    steps_here = right_side.shape[0]
    devices_tm = lax.axis_size("tm")
    position = lax.axis_index("tm")
    log_decay = math.log(alpha_corner) / L
    decay = math.exp(log_decay)
    local_steps = position * steps_here + jnp.arange(steps_here, dtype=jnp.int32)
    times = local_steps.astype(jnp.float32)
    weights = jnp.exp(times * log_decay)[:, None, None]
    unweights = jnp.exp(-times * log_decay)[:, None, None]
    cosine, sine = dft_tables(L)
    velocity_col = velocity[0]
    velocity_row = velocity[1]
    width = right_side.shape[2] // devices_tm
    start = position * width
    diff_strip = lax.dynamic_slice_in_dim(diffusion, start, width, 1)[:, :, None]
    col_strip = lax.dynamic_slice_in_dim(velocity_col, start, width, 1)[:, :, None]
    row_strip = lax.dynamic_slice_in_dim(velocity_row, start, width, 1)[:, :, None]
    angles = jnp.arange(L, dtype=jnp.int32).astype(jnp.float32) * (2.0 * math.pi / L)
    shift_real = decay * jnp.cos(angles)
    shift_imag = decay * jnp.sin(angles)
    diag_real = 1.0 + 4.0 * diff_strip - shift_real
    modulus = diag_real * diag_real + shift_imag * shift_imag

    def forward(block):
        real_part = jnp.dot(block, cosine, precision=highest)
        imag_part = -jnp.dot(block, sine, precision=highest)
        return jnp.concatenate([real_part, imag_part], axis=2)

    total = lax.psum(jnp.sum(right_side * right_side), ("tm", "space"))
    beta = jnp.sqrt(total + epsilon)
    basis = [right_side / beta]
    prepared = []
    hessen = jnp.zeros((KRYLOV + 1, KRYLOV), jnp.float32)
    for column in range(KRYLOV):
        moved = jnp.transpose(basis[column] * weights, (1, 2, 0))
        spectrum = forward(lax.all_to_all(moved, "tm", split_axis=1, concat_axis=2, tiled=True))
        source_real = spectrum[:, :, :L]
        source_imag = spectrum[:, :, L:]
        guess_real, guess_imag = divided(source_real, source_imag, diag_real, shift_imag, modulus)
        for sweep in range(SWEEPS - 1):
            joined = jnp.concatenate([guess_real, guess_imag], axis=2)
            padded = extended(joined, (("tm", 1), ("space", 0)), 1)
            image = stencil(joined, padded, 0, 1, diff_strip, col_strip, row_strip)
            left_real, left_imag = remainder(
                source_real,
                source_imag,
                image[:, :, :L],
                image[:, :, L:],
                guess_real,
                guess_imag,
                shift_real,
                shift_imag,
            )
            step_real, step_imag = divided(left_real, left_imag, diag_real, shift_imag, modulus)
            guess_real = guess_real + step_real
            guess_imag = guess_imag + step_imag
        back = (
            jnp.dot(guess_real, cosine, precision=highest)
            - jnp.dot(guess_imag, sine, precision=highest)
        ) / L
        back = lax.all_to_all(back, "tm", split_axis=2, concat_axis=1, tiled=True)
        direction = jnp.transpose(back, (2, 0, 1)) * unweights
        prepared.append(direction)
        apply_padded = extended(direction, (("space", 1),), 1)
        apply_padded = jnp.pad(apply_padded, ((0, 0), (0, 0), (1, 1)))
        apply_image = stencil(direction, apply_padded, 1, 2, diffusion, velocity_col, velocity_row)
        earlier = from_behind(direction[-1:], "tm", 1)
        image = apply_image - jnp.concatenate([earlier, direction[:-1]], axis=0)
        local = jnp.stack([jnp.sum(vector * image) for vector in basis])
        projections = lax.psum(local, ("tm", "space"))
        for row in range(column + 1):
            image = image - projections[row] * basis[row]
        squares = lax.psum(jnp.sum(image * image), ("tm", "space"))
        length = jnp.sqrt(squares + epsilon)
        hessen = hessen.at[: column + 1, column].set(projections)
        hessen = hessen.at[column + 1, column].set(length)
        basis.append(image / length)
    coeffs = least_squares(hessen, beta)
    solution = prepared[0] * coeffs[0]
    for column in range(1, KRYLOV):
        solution = solution + prepared[column] * coeffs[column]
    first = (jnp.arange(KRYLOV + 1) == 0).astype(jnp.float32)
    target = beta * first - jnp.sum(hessen * coeffs[None, :], axis=1)
    residual = basis[0] * target[0]
    for row in range(1, KRYLOV + 1):
        residual = residual + basis[row] * target[row]
    return (solution, residual)


SUB = 8
LANE = 128
AXES = ("tm", "space")
UNROLL = 32
PAIR = 2


def spin(block, amount, axis=1):
    return pltpu.roll(block, amount % block.shape[axis], axis)


def lane_of(shape):
    return lax.broadcasted_iota(jnp.int32, shape, 1)


def exchange_blocks(pieces, width, radix):
    pieces = list(pieces)
    lane = lane_of(pieces[0].shape)
    step = 1
    while step < len(pieces):
        digit = lane // (width * step) % radix
        result = list(pieces)
        for i in range(len(pieces)):
            e = i // step % radix
            total = None
            for d in range(radix):
                moved = pieces[i + (d - e) * step]
                if d != e:
                    moved = spin(moved, (d - e) * step * width)
                total = moved if total is None else jnp.where(digit == d, moved, total)
            result[i] = total
        pieces = result
        step *= radix
    return pieces


class Plan:
    def __init__(self, mesh, steps, rows, cols):
        self.tm = mesh.shape["tm"]
        self.space = mesh.shape["space"]
        self.devices = self.tm * self.space
        self.steps = steps
        self.rows = rows
        self.cols = cols
        self.here = steps // self.tm
        self.window = LANE // self.tm
        self.own = cols // self.devices
        self.halo = SWEEPS
        self.slot = self.window // self.space
        self.used = self.own + 2 * self.halo
        self.spare = self.window - self.used
        self.tiles = self.here // SUB
        self.inward = (self.tiles - 1) * SUB + 1
        self.groups = self.here // (2 * SUB)
        self.outward = self.groups * SUB + 2 * self.groups + 1
        self.ring = [self.strip_of(d // self.space, d % self.space) for d in range(self.devices)]
        self.holder = [self.ring.index(j) for j in range(self.devices)]

    def fits(self):
        return (
            LANE % self.tm == 0
            and self.tm == SUB
            and self.rows == SUB * self.space
            and self.cols % self.devices == 0
            and self.cols == 2 * LANE
            and self.steps % (self.tm * 2 * SUB) == 0
            and self.window == 2 * self.own
            and self.spare * (self.tiles - 1) == self.used
            and self.here % UNROLL == 0
            and self.groups * 2 == SUB
            and self.slot >= self.halo
            and self.space % 2 == 0
            and KRYLOV == 3
            and self.tiles % PAIR == 0
            and self.groups % PAIR == 0
            and self.tm % 4 == 0
        )

    def strip_of(self, t, s):
        turn = t ^ ((t >> 1) & 1)
        half = self.space // 2
        x, core = s // 2, s % 2
        odd = turn % 2
        return (turn * half + x + odd * (half - 1 - 2 * x)) * 2 + core


def pack_kernel(plan, place_ref, right_in, diff_in, vel_in, out_ref, *scratch):
    tail_ref, right_ref, diff_ref, vel_ref, sems = scratch
    split = plan.here - SUB
    copies = [
        pltpu.make_async_copy(right_in.at[split:], right_ref.at[split:], sems.at[0]),
        pltpu.make_async_copy(right_in.at[:split], right_ref.at[:split], sems.at[1]),
        pltpu.make_async_copy(diff_in, diff_ref, sems.at[2]),
        pltpu.make_async_copy(vel_in, vel_ref, sems.at[3]),
    ]
    for copy in copies:
        copy.start()
    copies[0].wait()
    window, own, halo = plan.window, plan.own, plan.halo
    parts = plan.cols // LANE
    lane = lane_of((SUB, LANE))
    group, spot = lane // window, lane % window
    edge = LANE - (SUB - 1) * window - own + halo

    def strips():
        for parity in range(2):
            for part in range(parts):
                for m in range(SUB):
                    yield parity, part, m, plan.holder[2 * (part * SUB + m) + parity]

    def body(k, carry):
        a = plan.tiles - 1 - k
        fields = [right_ref[a * SUB + i] for i in range(SUB)]
        cache = {}

        def turned(i, part, amount):
            key = (i, part % parts, amount % LANE)
            if key not in cache:
                block = fields[i][:, key[1] * LANE : (key[1] + 1) * LANE]
                cache[key] = spin(block, amount)
            return cache[key]

        pieces = []
        for parity, part, m, _ in strips():
            base = parity * own - halo
            total = None
            for i in range(SUB):
                amount = window * (i - m) - base
                value = turned(i, part, amount)
                if parity == 0 and m == 0:
                    value = jnp.where(spot < halo, turned(i, part - 1, amount), value)
                if parity == 1 and m == SUB - 1:
                    value = jnp.where(spot >= edge, turned(i, part + 1, amount), value)
                total = value if total is None else jnp.where(group == i, value, total)
            pieces.append(total)

        @pl.when(k == 0)
        def _():
            for index, piece in enumerate(pieces):
                tail_ref[index] = piece
            copies[1].wait()

        @pl.when(k > 0)
        def _():
            amount = plan.used - plan.spare * a
            for index, (_, _, _, target) in enumerate(strips()):
                tail = pltpu.roll(tail_ref[index], amount, 1)
                piece = jnp.where(spot >= plan.used, tail, pieces[index])
                out_ref[pl.ds(target * plan.inward + a * SUB, SUB), :] = piece

        return carry

    lax.fori_loop(0, plan.tiles, body, 0)
    copies[2].wait()
    copies[3].wait()
    row = pl.ds(place_ref[0], 1)
    lines = [diff_ref[row, :], vel_ref[0, row, :], vel_ref[1, row, :]]
    sub = lax.broadcasted_iota(jnp.int32, (SUB, LANE), 0)
    blocks = [
        [jnp.broadcast_to(line[:, h * LANE : (h + 1) * LANE], (SUB, LANE)) for h in range(parts)]
        for line in lines
    ]
    for parity in range(2):
        base = parity * own - halo
        for part in range(parts):
            total = jnp.zeros((SUB, LANE), jnp.float32)
            for f in range(len(lines)):
                amount = (f + 1) * window - base

                def slanted(h):
                    flat = spin(blocks[f][h % parts], amount)
                    return pltpu.roll(flat, 0, 1, stride=window, stride_axis=0)

                value = slanted(part)
                if parity == 0:
                    value = jnp.where((sub == SUB - 1) & (spot < halo), slanted(part - 1), value)
                else:
                    value = jnp.where((sub == 0) & (spot >= edge), slanted(part + 1), value)
                total = jnp.where(group == f, value, total)
            for m in range(SUB):
                target = plan.holder[2 * (part * SUB + m) + parity]
                at = target * plan.inward + plan.inward - 1
                out_ref[at : at + 1, :] = total[SUB - 1 - m : SUB - m]


def totals_of(ref):
    return jnp.sum(ref[...], axis=0, keepdims=True) * (1.0 / (damping * damping))


def pick(totals, k):
    lane = lane_of(totals.shape)
    value = jnp.sum(jnp.where(lane == k, totals, 0.0), axis=1, keepdims=True)
    return jnp.broadcast_to(value, (1, LANE))


def middle(totals):
    aa, ab, bb, ac, bc = (pick(totals, k) for k in range(5))
    scale = 1.0 / (aa + epsilon)
    drop = scale * ab
    norm = jnp.maximum(bb - drop * (2.0 * ab - drop * aa), 1e-5 * bb)
    over = ac - drop * ab
    along = bc - drop * (bb + ac - drop * ab)
    return aa, drop, scale * over, scale * along / (scale * norm + epsilon)


def iterate(middle_totals, totals):
    aa, drop, over, along = middle(middle_totals)
    pairs = [(0, 1), (1, 1), (0, 2), (1, 2), (2, 2), (0, 3), (1, 3), (2, 3), (3, 3)]
    gram = {(0, 0): aa}
    for k, (i, j) in enumerate(pairs):
        gram[i, j] = gram[j, i] = pick(totals, k)
    zero = jnp.zeros_like(aa)
    one = jnp.ones_like(aa)
    images = [[drop, one, zero, zero], [over, along, one, zero], [zero, zero, zero, one]]
    size = KRYLOV + 1

    def product(left, right):
        return sum(left[i] * right[j] * gram[i, j] for i in range(size) for j in range(size))

    beta = jnp.sqrt(aa + epsilon)
    basis = [[1.0 / beta, zero, zero, zero]]
    hessen = [[zero] * KRYLOV for row in range(size)]
    for j in range(KRYLOV):
        image = [sum(basis[j][k] * images[k][i] for k in range(KRYLOV)) for i in range(size)]
        found = [product(basis[i], image) for i in range(j + 1)]
        for i in range(j + 1):
            hessen[i][j] = found[i]
            image = [w - found[i] * v for w, v in zip(image, basis[i])]
        length = jnp.sqrt(jnp.maximum(product(image, image), 0.0) + epsilon)
        hessen[j + 1][j] = length
        basis.append([w / length for w in image])
    ortho = []
    upper = [[None] * KRYLOV for row in range(KRYLOV)]
    for column in range(KRYLOV):
        current = [hessen[row][column] for row in range(size)]
        for row in range(column):
            factor = sum(x * y for x, y in zip(ortho[row], current))
            upper[row][column] = factor
            current = [y - factor * x for x, y in zip(ortho[row], current)]
        length = jnp.sqrt(sum(y * y for y in current))
        upper[column][column] = length
        ortho.append([y / length for y in current])
    values = [None] * KRYLOV
    for row in reversed(range(KRYLOV)):
        accum = ortho[row][0] * beta
        for later in range(row + 1, KRYLOV):
            accum = accum - upper[row][later] * values[later]
        values[row] = accum / upper[row][row]
    weights = [sum(values[j] * basis[j][k] for j in range(KRYLOV)) for k in range(KRYLOV)]
    weights[0] = weights[0] - drop * weights[1]
    return weights


def coefficients(plan, recv_ref, strip, table_ref):
    window = plan.window
    lane = lane_of((SUB, LANE))
    stride = plan.space * plan.inward
    lines = [
        recv_ref[pl.ds(s * plan.inward + plan.inward - 1, SUB, stride), :]
        for s in range(plan.space)
    ]
    fields = []
    for f in range(3):
        parts = []
        for line in lines:
            part = None
            for g in range(plan.tm):
                moved = spin(line, (g - f) * window)
                part = moved if g == 0 else jnp.where(lane // window == g, moved, part)
            parts.append(part)
        fields.append(jnp.concatenate(parts, axis=0))
    diff, vel_col, vel_row = fields
    shape = (plan.rows, LANE)
    row = lax.broadcasted_iota(jnp.int32, shape, 0)
    col = strip * plan.own - plan.halo + lane_of(shape) % window
    center = 1.0 + 4.0 * diff
    table_ref[0] = damping * center
    table_ref[1] = 1.0 / center
    table_ref[2] = jnp.where(row > 0, damping * (diff + vel_row), 0.0)
    table_ref[3] = jnp.where(row < plan.rows - 1, damping * (diff - vel_row), 0.0)
    table_ref[4] = jnp.where(col > 0, damping * (diff + vel_col), 0.0)
    table_ref[5] = jnp.where(col < plan.cols - 1, damping * (diff - vel_col), 0.0)


def krylov_kernel(plan, j, *refs):
    refs = list(refs)
    strip = refs.pop(0)[0]
    here, window, rows, halo, own = plan.here, plan.window, plan.rows, plan.halo, plan.own
    slot = plan.slot
    final = j == KRYLOV - 1
    shape = (rows, LANE)
    lane = lane_of(shape)
    low_lane = lane_of((SUB, LANE))
    low_spot = low_lane % window
    even = strip % 2 == 0
    if j == 0:
        recv_ref, table_ref, q_ref, g_ref, w_ref, near_ref, far_ref, y_ref, tail_ref = refs
        coefficients(plan, recv_ref, strip, table_ref)
    elif not final:
        table_ref, image_ref, near_in, far_in, first_ref = refs[:5]
        q_ref, g_ref, w_ref, near_ref, far_ref, sum_ref, y_ref = refs[5:]
    else:
        table_ref, image_ref, near_in, far_in, first_ref, second_ref, mid_ref = refs[:7]
        g_ref, sum_ref, y_ref, q_ref, w_ref, rest_ref = refs[7:]
        _, drop, over, along = middle(totals_of(mid_ref))
    center = table_ref[0]
    inverse = table_ref[1]
    north, south, west, east = (table_ref[2 + k] for k in range(4))
    zero = jnp.zeros(shape, jnp.float32)
    low_zero = jnp.zeros((SUB, LANE), jnp.float32)
    inner = slice(SUB, SUB + rows)

    def around(n, field):
        return (
            north * g_ref[n, SUB - 1 : SUB - 1 + rows, :]
            + south * g_ref[n, SUB + 1 : SUB + 1 + rows, :]
            + west * spin(field, 1)
            + east * spin(field, -1)
        )

    power = inverse
    for _ in range(int(math.log2(here))):
        power = power * power
    whole = power
    for _ in range(int(math.log2(plan.tm))):
        whole = whole * whole
    closing = 1.0 / (1.0 - alpha_corner * whole)

    def entering(ends):
        total = alpha_corner * ends
        for k in reversed(range(1, plan.tm)):
            back = spin(ends, k * window)
            total = total * power + jnp.where(lane < k * window, alpha_corner * back, back)
        return total * closing

    def settle(base, y):
        for k in range(UNROLL):
            y = (y_ref[base + k] + y) * inverse
            y_ref[base + k] = y
        return y

    for k in range(UNROLL):
        y_ref[k] = zero

    def blank(n):
        g_ref[n] = jnp.zeros((rows + 2 * SUB, LANE), jnp.float32)

    if j == 0:
        last_tile = plan.tiles - 1

        def tails(k, carry):
            for p in (4 * k, 4 * k + 1, 4 * k + 2, 4 * k + 3):
                for s in range(plan.space):
                    source = p * plan.space + s
                    total = low_zero
                    for a in range(last_tile):
                        tile = recv_ref[pl.ds(source * plan.inward + a * SUB, SUB), :]
                        moved = spin(tile, plan.spare * a - plan.used)
                        total = jnp.where(low_spot // plan.spare == a, moved, total)
                    tail_ref[source] = total
            return carry

        lax.fori_loop(0, plan.tm // 4, tails, 0)

        def first(k, y):
            parts = [[] for _ in range(PAIR)]
            for t in range(PAIR):
                a = k * PAIR + t
                whole = a < last_tile
                at = jnp.minimum(a, last_tile - 1) * SUB
                for s in range(plan.space):
                    cut = []
                    for p in range(plan.tm):
                        source = p * plan.space + s
                        tile = recv_ref[pl.ds(source * plan.inward + at, SUB), :]
                        cut.append(damping * jnp.where(whole, tile, tail_ref[source]))
                    parts[t].append(exchange_blocks(cut, window, 2))
            for t in range(PAIR):
                for i in range(SUB):
                    n = (k * PAIR + t) * SUB + i
                    q = jnp.concatenate([part[i] for part in parts[t]], axis=0)
                    q_ref[n] = q
                    y = (q + y) * inverse
                    y_ref[UNROLL + n] = y
                    blank(n)
            return y

        y = lax.fori_loop(0, plan.tiles // PAIR, first, zero)
    else:
        near_side = jnp.where(even, halo + own, 0)
        far_side = jnp.where(even, 0, halo + own)
        near_mask = (low_spot >= near_side) & (low_spot < near_side + halo)
        far_mask = (low_spot >= far_side) & (low_spot < far_side + halo)

        def first(i, y):
            base = i * UNROLL
            y = settle(base, y)
            for k in range(UNROLL):
                n = base + k
                near, far = near_in[n], far_in[n]
                image = image_ref[n]
                parts = []
                for s in range(plan.space):
                    part = image[s * SUB : (s + 1) * SUB]
                    shift = LANE - slot * s
                    part = jnp.where(near_mask, pltpu.roll(near, (near_side + shift) % LANE, 1), part)
                    part = jnp.where(far_mask, pltpu.roll(far, (far_side + shift) % LANE, 1), part)
                    parts.append(part)
                q = jnp.concatenate(parts, axis=0)
                if final:
                    start, later = first_ref[n], second_ref[n]
                    rest = later - drop * start
                    rest_ref[n] = rest
                    q = (q - drop * later) - over * start - along * rest
                q_ref[n] = q
                y_ref[UNROLL + n] = q
                blank(n)
            return y

        y = settle(here, lax.fori_loop(0, here // UNROLL, first, zero))

    def sweep(_, ends):
        def body(i, carry):
            y, z = carry
            base = i * UNROLL
            olds = [y_ref[UNROLL + base + k] for k in range(UNROLL)]
            y = settle(base, y)
            for k in range(UNROLL):
                n = base + k
                z = z * inverse
                guess = (1.0 - damping) * g_ref[n, inner, :] + (olds[k] + z)
                g_ref[n, inner, :] = guess
                y_ref[UNROLL + n] = q_ref[n] + around(n, guess)
            return (y, z)

        y, _ = lax.fori_loop(0, here // UNROLL, body, (zero, entering(ends)))
        return settle(here, y)

    y = lax.fori_loop(0, SWEEPS - 1, sweep, y)
    start = entering(y)
    ending = (1.0 - damping) * g_ref[here - 1, inner, :] + (y + start * power)
    before = jnp.where(lane < window, 0.0, damping * spin(ending, window))

    near_from = jnp.where(even, own, halo)
    far_from = jnp.where(even, halo, own)

    def fold(block):
        return sum(block[s * SUB : (s + 1) * SUB] for s in range(plan.space))

    size = KRYLOV + 1

    def gather(base, accs):
        for k in range(UNROLL):
            n = base + k
            image = w_ref[n]
            if not final:
                near = far = None
                for s in range(plan.space):
                    part = image[s * SUB : (s + 1) * SUB]
                    a = pltpu.roll(part, (slot * s - near_from + LANE) % LANE, 1)
                    b = pltpu.roll(part, (slot * s - far_from + LANE) % LANE, 1)
                    inside = low_spot // slot == s
                    near = a if near is None else jnp.where(inside, a, near)
                    far = b if far is None else jnp.where(inside, b, far)
                near_ref[n] = near
                far_ref[n] = far
            if j == 0:
                continue
            q = q_ref[n]
            start = first_ref[n]
            if not final:
                pairs = [(start, start), (start, q), (q, q), (start, image), (q, image)]
            else:
                rest = rest_ref[n]
                held = [start, rest, q, image]
                pairs = [(held[i], held[k]) for k in range(1, size) for i in range(k + 1)]
            accs = [acc + fold(x * y) for acc, (x, y) in zip(accs, pairs)]
        return accs

    def last(i, carry):
        z, before, accs = carry
        accs = gather(jnp.maximum(i - 1, 0) * UNROLL, accs)
        accs = tuple(jnp.where(i > 0, acc, 0.0) for acc in accs)
        for k in range(UNROLL):
            n = i * UNROLL + k
            z = z * inverse
            guess = (1.0 - damping) * g_ref[n, inner, :] + (y_ref[UNROLL + n] + z)
            g_ref[n, inner, :] = guess
            w_ref[n] = center * guess - around(n, guess) - before
            before = damping * guess
        return (z, before, accs)

    fields = (0, 5, 9)[j]
    _, _, accs = lax.fori_loop(0, here // UNROLL, last, (start, before, (low_zero,) * fields))
    accs = gather(here - UNROLL, list(accs))
    if j == 0:
        return
    owned = (low_spot >= halo) & (low_spot < halo + own)
    record = jnp.zeros((1, LANE), jnp.float32)
    record_lane = lane_of((1, LANE))
    for place, acc in enumerate(accs):
        value = jnp.sum(jnp.where(owned, acc, 0.0), axis=0, keepdims=True)
        value = jnp.sum(value, axis=1, keepdims=True)
        record = jnp.where(record_lane == place, value, record)
    sum_ref[...] = jnp.broadcast_to(record, sum_ref.shape)


def combine_kernel(plan, *refs):
    z_refs = refs[:KRYLOV]
    mid_ref, end_ref, out_ref = refs[KRYLOV:]
    along = iterate(totals_of(mid_ref), totals_of(end_ref))
    own, halo, window, groups = plan.own, plan.halo, plan.window, plan.groups
    lane = lane_of((SUB, LANE))
    front = lane % window < own
    size = plan.outward

    def start_of(p, s):
        return (p * plan.space + s) * size

    def value(n, s):
        here = slice((s + 1) * SUB, (s + 2) * SUB)
        return sum(c * ref[n, here, :] for c, ref in zip(along, z_refs))

    def body(k, carry):
        for t in range(PAIR):
            aa = k * PAIR + t
            for s in range(plan.space):
                pieces = []
                for i in range(SUB):
                    n = aa * 2 * SUB + 2 * i
                    left, right = spin(value(n, s), -halo), spin(value(n + 1, s), own - halo)
                    pieces.append(jnp.where(front, left, right))
                for p, piece in enumerate(exchange_blocks(pieces, window, 2)):
                    out_ref[pl.ds(start_of(p, s) + aa * SUB, SUB), :] = piece
                    if s + 1 < plan.space:
                        at = start_of(p, s + 1) + groups * SUB + aa
                        out_ref[pl.ds(at, 1), :] = piece[SUB - 1 :]
                    if s > 0:
                        at = start_of(p, s - 1) + groups * SUB + groups + aa
                        out_ref[pl.ds(at, 1), :] = piece[:1]
        return carry

    lax.fori_loop(0, groups // PAIR, body, 0)
    nothing = jnp.zeros((groups, LANE), jnp.float32)
    sub = lax.broadcasted_iota(jnp.int32, (SUB, LANE), 0)
    for p in range(plan.tm):
        at = start_of(p, 0) + groups * SUB
        out_ref[at : at + groups, :] = nothing
        at = start_of(p, plan.space - 1) + groups * SUB + groups
        out_ref[at : at + groups, :] = nothing
    for s in range(plan.space):
        ending = value(plan.here - 1, s)
        for p in range(plan.tm):
            line = nothing[:1]
            if p > 0:
                turned = spin(ending, -(p - 1) * window - halo)
                turned = pltpu.roll(turned, 0, 1, stride=own, stride_axis=0)
                line = jnp.sum(jnp.where(lane // own == sub, turned, 0.0), axis=0, keepdims=True)
            at = start_of(p, s) + size - 1
            out_ref[at : at + 1, :] = line


def finish_kernel(plan, recv_ref, right_ref, diff_ref, vel_ref, *refs):
    results, (rim_ref, out_ref, rest_ref, sems) = refs[:2], refs[2:]
    groups, own, size = plan.groups, plan.own, plan.outward
    count = LANE // own
    parts = plan.cols // LANE
    shape = (SUB, plan.cols)
    lane = lane_of((SUB, LANE))
    diff, vel_col, vel_row = diff_ref[...], vel_ref[0], vel_ref[1]
    col = lane_of(shape)
    sub = lax.broadcasted_iota(jnp.int32, shape, 0)
    center = 1.0 + 4.0 * diff
    north = diff + vel_row
    south = diff - vel_row
    west = jnp.where(col > 0, diff + vel_col, 0.0)
    east = jnp.where(col < plan.cols - 1, diff - vel_col, 0.0)

    def start_of(part, m):
        return plan.holder[part * count + m] * size

    def spread(offset):
        wide = []
        for part in range(parts):
            pieces = [
                recv_ref[pl.ds(start_of(part, m) + offset, SUB), :] for m in range(count)
            ]
            wide.append(exchange_blocks(pieces, own, 2))
        return [jnp.concatenate(pair, axis=1) for pair in zip(*wide)]

    for i, field in enumerate(spread(groups * SUB)):
        rim_ref[i] = field
    halves = []
    row = lax.broadcasted_iota(jnp.int32, (SUB, LANE), 0)
    for part in range(parts):
        tiles = []
        for first in range(0, count, SUB):
            tile = jnp.zeros((SUB, LANE), jnp.float32)
            for q in range(SUB):
                at = start_of(part, first + q) + size - 1
                line = jnp.broadcast_to(recv_ref[at : at + 1, :], (SUB, LANE))
                tile = jnp.where(row == q, line, tile)
            tile = spin(tile, first * own)
            tiles.append((first, pltpu.roll(tile, 0, 1, stride=own, stride_axis=0)))
        total = jnp.zeros((SUB, LANE), jnp.float32)
        for r in range(SUB):
            line = sum(
                jnp.where(lane // own == row + first, spin(tile, -r * own), 0.0)
                for first, tile in tiles
            )
            line = jnp.sum(line, axis=0, keepdims=True)
            total = jnp.where(row == r, jnp.broadcast_to(line, (SUB, LANE)), total)
        halves.append(total)
    before = jnp.concatenate(halves, axis=1)

    size_of = PAIR * count

    def copies(k):
        at = pl.ds(k * size_of, size_of)
        return [
            pltpu.make_async_copy(ref.at[at], result.at[at], sems.at[k, f])
            for f, (ref, result) in enumerate(zip((out_ref, rest_ref), results))
        ]

    def body(k, before):
        for t in range(PAIR):
            aa = k * PAIR + t
            for i, field in enumerate(spread(aa * SUB)):
                n = aa * count + i
                above = rim_ref[i, pl.ds(aa, 1), :]
                below = rim_ref[i, pl.ds(groups + aa, 1), :]
                out_ref[n] = field
                around = (
                    north * jnp.where(sub == 0, above, spin(field, 1, 0))
                    + south * jnp.where(sub == SUB - 1, below, spin(field, -1, 0))
                    + west * spin(field, 1)
                    + east * spin(field, -1)
                )
                rest_ref[n] = right_ref[n] - (center * field - around - before)
                before = field
        for copy in copies(k):
            copy.start()
        return before

    lax.fori_loop(0, groups // PAIR, body, before)
    for k in range(groups // PAIR):
        for copy in copies(k):
            copy.wait()


def call(kernel, shapes, operands, scalars=0, scratch=(), sems=None, far_in=False, far_out=False, room=16):
    vmem = pl.BlockSpec(memory_space=pltpu.VMEM)
    smem = pl.BlockSpec(memory_space=pltpu.SMEM)
    hbm = pl.BlockSpec(memory_space=pltpu.HBM)
    held = [pltpu.VMEM(shape, jnp.float32) for shape in scratch]
    if sems:
        held.append(pltpu.SemaphoreType.DMA(sems))
    return pl.pallas_call(
        kernel,
        out_shape=[jax.ShapeDtypeStruct(shape, jnp.float32) for shape in shapes],
        in_specs=[smem] * scalars + [hbm if far_in else vmem] * (len(operands) - scalars),
        out_specs=[hbm if far_out else vmem] * len(shapes),
        scratch_shapes=held,
        compiler_params=pltpu.CompilerParams(vmem_limit_bytes=room * 1024 * 1024),
    )(*operands)


def everyone(block, devices):
    lines = block.shape[0] // devices
    parts = block.reshape(devices, lines, 1, LANE)
    return lax.all_to_all(parts, AXES, split_axis=0, concat_axis=0, tiled=True).reshape(block.shape)


def strip_device(plan, right_side, diffusion, velocity):
    t = lax.axis_index("tm")
    s = lax.axis_index("space")
    strip = plan.strip_of(t, s).astype(jnp.int32).reshape(1)
    count = plan.devices
    hold = plan.holder
    near_route = []
    far_route = []
    for k in range(0, count, 2):
        near_route += [(hold[k], hold[k + 1]), (hold[k + 1], hold[k])]
    for k in range(1, count - 1, 2):
        far_route += [(hold[k], hold[k + 1]), (hold[k + 1], hold[k])]
    bind = lambda kernel, *more: (lambda *refs: kernel(plan, *more, *refs))
    full = (plan.here, plan.rows, LANE)
    padded = (plan.here, plan.rows + 2 * SUB, LANE)
    delayed = (plan.here + UNROLL, plan.rows, LANE)
    side = (plan.here, SUB, LANE)
    small = (count, LANE)
    given = [right_side, diffusion, velocity]
    sent = call(
        bind(pack_kernel),
        [(count * plan.inward, LANE)],
        [t.astype(jnp.int32).reshape(1), *given],
        scalars=1,
        scratch=[(count, SUB, LANE), *(block.shape for block in given)],
        sems=(4,),
        far_in=True,
        room=63,
    )[0]
    table, q0, z0, image, near, far = call(
        bind(krylov_kernel, 0),
        [(6, plan.rows, LANE), full, padded, full, side, side],
        [strip, everyone(sent, count)],
        scalars=1,
        scratch=[delayed, (count, SUB, LANE)],
    )
    near = lax.ppermute(near, AXES, near_route)
    far = lax.ppermute(far, AXES, far_route)
    q1, z1, image, near, far, sums = call(
        bind(krylov_kernel, 1),
        [full, padded, full, side, side, small],
        [strip, table, image, near, far, q0],
        scalars=1,
        scratch=[delayed],
    )
    near = lax.ppermute(near, AXES, near_route)
    far = lax.ppermute(far, AXES, far_route)
    mid = everyone(sums, count)
    z2, sums = call(
        bind(krylov_kernel, 2),
        [padded, small],
        [strip, table, image, near, far, q0, q1, mid],
        scalars=1,
        scratch=[delayed, full, full, full],
    )
    end = everyone(sums, count)
    packed = call(bind(combine_kernel), [(count * plan.outward, LANE)], [z0, z1, z2, mid, end])[0]
    shape = right_side.shape
    return tuple(
        call(
            bind(finish_kernel),
            [shape, shape],
            [everyone(packed, count), *given],
            scratch=[(2 * SUB, SUB, plan.cols), shape, shape],
            sems=(plan.groups // PAIR, 2),
            far_out=True,
        )
    )


def per_device(mesh):
    def run(right_side, diffusion, velocity):
        rows = right_side.shape[1] * mesh.shape["space"]
        steps = right_side.shape[0] * mesh.shape["tm"]
        plan = Plan(mesh, steps, rows, right_side.shape[2])
        if plan.fits():
            return strip_device(plan, right_side, diffusion, velocity)
        return generic_device(right_side, diffusion, velocity)

    return run


def solution(mesh):
    placed = (P("tm", "space", None), P("space", None), P(None, "space", None))
    return jax.shard_map(
        per_device(mesh),
        mesh=mesh,
        in_specs=placed,
        out_specs=(P("tm", "space", None), P("tm", "space", None)),
        check_vma=False,
    )
```

```python
import math

import jax
import jax.numpy as jnp
from jax import lax
from jax.experimental import pallas as pl
from jax.experimental.pallas import tpu as pltpu
from jax.sharding import PartitionSpec as P

L = 512
KRYLOV = 3
SWEEPS = 3


alpha_corner = 0.05
damping = 0.8
epsilon = 1e-06
highest = lax.Precision.HIGHEST


def extended(block, sides, width):
    for axis, dim in sides:
        count = lax.axis_size(axis)
        forward = [(i, i + 1) for i in range(count - 1)]
        backward = [(target, source) for source, target in forward]
        low = lax.ppermute(
            lax.slice_in_dim(block, block.shape[dim] - width, None, axis=dim), axis, forward
        )
        high = lax.ppermute(lax.slice_in_dim(block, 0, width, axis=dim), axis, backward)
        block = jnp.concatenate([low, block, high], axis=dim)
    return block


def from_behind(block, axis, distance):
    devices = range(lax.axis_size(axis))
    route = [(i - distance, i) for i in devices if i - distance in devices]
    return lax.ppermute(block, axis, route)


def shifted(padded, row_dim, col_dim, rows, cols, row_start, col_start):
    piece = lax.slice_in_dim(padded, row_start, row_start + rows, axis=row_dim)
    return lax.slice_in_dim(piece, col_start, col_start + cols, axis=col_dim)


def stencil(field, padded, row_dim, col_dim, diffusion, velocity_col, velocity_row):
    rows = field.shape[row_dim]
    cols = field.shape[col_dim]
    north = shifted(padded, row_dim, col_dim, rows, cols, 0, 1)
    south = shifted(padded, row_dim, col_dim, rows, cols, 2, 1)
    west = shifted(padded, row_dim, col_dim, rows, cols, 1, 0)
    east = shifted(padded, row_dim, col_dim, rows, cols, 1, 2)
    return (
        (1.0 + 4.0 * diffusion) * field
        - diffusion * (north + south + west + east)
        + velocity_col * (east - west)
        + velocity_row * (south - north)
    )


def divided(real_part, imag_part, diag_real, diag_imag, modulus):
    return (
        damping * (real_part * diag_real + imag_part * diag_imag) / modulus,
        damping * (imag_part * diag_real - real_part * diag_imag) / modulus,
    )


def remainder(
    source_real, source_imag, image_real, image_imag, guess_real, guess_imag, shift_real, shift_imag
):
    return (
        source_real - (image_real - (shift_real * guess_real + shift_imag * guess_imag)),
        source_imag - (image_imag - (shift_real * guess_imag - shift_imag * guess_real)),
    )


def dft_tables(length):
    index = jnp.arange(length, dtype=jnp.int32)
    product = index[:, None] * index[None, :] % length
    angle = product.astype(jnp.float32) * (2.0 * math.pi / length)
    return (jnp.cos(angle), jnp.sin(angle))


def least_squares(hessen, beta):
    ortho = []
    upper = [[None] * KRYLOV for row in range(KRYLOV)]
    for column in range(KRYLOV):
        current = hessen[:, column]
        for row in range(column):
            factor = jnp.sum(ortho[row] * current)
            upper[row][column] = factor
            current = current - factor * ortho[row]
        length = jnp.sqrt(jnp.sum(current * current))
        upper[column][column] = length
        ortho.append(current / length)
    target = [ortho[row][0] * beta for row in range(KRYLOV)]
    values = [None] * KRYLOV
    for row in reversed(range(KRYLOV)):
        accum = target[row]
        for later in range(row + 1, KRYLOV):
            accum = accum - upper[row][later] * values[later]
        values[row] = accum / upper[row][row]
    return jnp.stack(values)


def generic_device(right_side, diffusion, velocity):
    steps_here = right_side.shape[0]
    devices_tm = lax.axis_size("tm")
    position = lax.axis_index("tm")
    log_decay = math.log(alpha_corner) / L
    decay = math.exp(log_decay)
    local_steps = position * steps_here + jnp.arange(steps_here, dtype=jnp.int32)
    times = local_steps.astype(jnp.float32)
    weights = jnp.exp(times * log_decay)[:, None, None]
    unweights = jnp.exp(-times * log_decay)[:, None, None]
    cosine, sine = dft_tables(L)
    velocity_col = velocity[0]
    velocity_row = velocity[1]
    width = right_side.shape[2] // devices_tm
    start = position * width
    diff_strip = lax.dynamic_slice_in_dim(diffusion, start, width, 1)[:, :, None]
    col_strip = lax.dynamic_slice_in_dim(velocity_col, start, width, 1)[:, :, None]
    row_strip = lax.dynamic_slice_in_dim(velocity_row, start, width, 1)[:, :, None]
    angles = jnp.arange(L, dtype=jnp.int32).astype(jnp.float32) * (2.0 * math.pi / L)
    shift_real = decay * jnp.cos(angles)
    shift_imag = decay * jnp.sin(angles)
    diag_real = 1.0 + 4.0 * diff_strip - shift_real
    modulus = diag_real * diag_real + shift_imag * shift_imag

    def forward(block):
        real_part = jnp.dot(block, cosine, precision=highest)
        imag_part = -jnp.dot(block, sine, precision=highest)
        return jnp.concatenate([real_part, imag_part], axis=2)

    total = lax.psum(jnp.sum(right_side * right_side), ("tm", "space"))
    beta = jnp.sqrt(total + epsilon)
    basis = [right_side / beta]
    prepared = []
    hessen = jnp.zeros((KRYLOV + 1, KRYLOV), jnp.float32)
    for column in range(KRYLOV):
        moved = jnp.transpose(basis[column] * weights, (1, 2, 0))
        spectrum = forward(lax.all_to_all(moved, "tm", split_axis=1, concat_axis=2, tiled=True))
        source_real = spectrum[:, :, :L]
        source_imag = spectrum[:, :, L:]
        guess_real, guess_imag = divided(source_real, source_imag, diag_real, shift_imag, modulus)
        for sweep in range(SWEEPS - 1):
            joined = jnp.concatenate([guess_real, guess_imag], axis=2)
            padded = extended(joined, (("tm", 1), ("space", 0)), 1)
            image = stencil(joined, padded, 0, 1, diff_strip, col_strip, row_strip)
            left_real, left_imag = remainder(
                source_real,
                source_imag,
                image[:, :, :L],
                image[:, :, L:],
                guess_real,
                guess_imag,
                shift_real,
                shift_imag,
            )
            step_real, step_imag = divided(left_real, left_imag, diag_real, shift_imag, modulus)
            guess_real = guess_real + step_real
            guess_imag = guess_imag + step_imag
        back = (
            jnp.dot(guess_real, cosine, precision=highest)
            - jnp.dot(guess_imag, sine, precision=highest)
        ) / L
        back = lax.all_to_all(back, "tm", split_axis=2, concat_axis=1, tiled=True)
        direction = jnp.transpose(back, (2, 0, 1)) * unweights
        prepared.append(direction)
        apply_padded = extended(direction, (("space", 1),), 1)
        apply_padded = jnp.pad(apply_padded, ((0, 0), (0, 0), (1, 1)))
        apply_image = stencil(direction, apply_padded, 1, 2, diffusion, velocity_col, velocity_row)
        earlier = from_behind(direction[-1:], "tm", 1)
        image = apply_image - jnp.concatenate([earlier, direction[:-1]], axis=0)
        local = jnp.stack([jnp.sum(vector * image) for vector in basis])
        projections = lax.psum(local, ("tm", "space"))
        for row in range(column + 1):
            image = image - projections[row] * basis[row]
        squares = lax.psum(jnp.sum(image * image), ("tm", "space"))
        length = jnp.sqrt(squares + epsilon)
        hessen = hessen.at[: column + 1, column].set(projections)
        hessen = hessen.at[column + 1, column].set(length)
        basis.append(image / length)
    coeffs = least_squares(hessen, beta)
    solution = prepared[0] * coeffs[0]
    for column in range(1, KRYLOV):
        solution = solution + prepared[column] * coeffs[column]
    first = (jnp.arange(KRYLOV + 1) == 0).astype(jnp.float32)
    target = beta * first - jnp.sum(hessen * coeffs[None, :], axis=1)
    residual = basis[0] * target[0]
    for row in range(1, KRYLOV + 1):
        residual = residual + basis[row] * target[row]
    return (solution, residual)


SUB = 8
LANE = 128
AXES = ("tm", "space")
UNROLL = 32
PAIR = 2


def spin(block, amount, axis=1):
    return pltpu.roll(block, amount % block.shape[axis], axis)


def lane_of(shape):
    return lax.broadcasted_iota(jnp.int32, shape, 1)


def exchange_blocks(pieces, width, radix):
    pieces = list(pieces)
    lane = lane_of(pieces[0].shape)
    step = 1
    while step < len(pieces):
        digit = lane // (width * step) % radix
        result = list(pieces)
        for i in range(len(pieces)):
            e = i // step % radix
            total = None
            for d in range(radix):
                moved = pieces[i + (d - e) * step]
                if d != e:
                    moved = spin(moved, (d - e) * step * width)
                total = moved if total is None else jnp.where(digit == d, moved, total)
            result[i] = total
        pieces = result
        step *= radix
    return pieces


class Plan:
    def __init__(self, mesh, steps, rows, cols):
        self.tm = mesh.shape["tm"]
        self.space = mesh.shape["space"]
        self.devices = self.tm * self.space
        self.steps = steps
        self.rows = rows
        self.cols = cols
        self.here = steps // self.tm
        self.window = LANE // self.tm
        self.own = cols // self.devices
        self.halo = SWEEPS
        self.slot = self.window // self.space
        self.used = self.own + 2 * self.halo
        self.spare = self.window - self.used
        self.tiles = self.here // SUB
        self.inward = (self.tiles - 1) * SUB + 1
        self.groups = self.here // (2 * SUB)
        self.outward = self.groups * SUB + 2 * self.groups + 1
        self.ring = [self.strip_of(d // self.space, d % self.space) for d in range(self.devices)]
        self.holder = [self.ring.index(j) for j in range(self.devices)]

    def fits(self):
        return (
            LANE % self.tm == 0
            and self.tm == SUB
            and self.rows == SUB * self.space
            and self.cols % self.devices == 0
            and self.cols == 2 * LANE
            and self.steps % (self.tm * 2 * SUB) == 0
            and self.window == 2 * self.own
            and self.spare * (self.tiles - 1) == self.used
            and self.here % UNROLL == 0
            and self.groups * 2 == SUB
            and self.slot >= self.halo
            and self.space % 2 == 0
            and KRYLOV == 3
            and self.tiles % PAIR == 0
            and self.groups % PAIR == 0
            and self.tm % 4 == 0
        )

    def strip_of(self, t, s):
        turn = t ^ ((t >> 1) & 1)
        half = self.space // 2
        x, core = s // 2, s % 2
        odd = turn % 2
        return (turn * half + x + odd * (half - 1 - 2 * x)) * 2 + core


def pack_kernel(plan, right_in, diff_in, vel_in, out_ref, *scratch):
    tail_ref, right_ref, diff_ref, vel_ref, sems = scratch
    split = plan.here - SUB
    copies = [
        pltpu.make_async_copy(right_in.at[split:], right_ref.at[split:], sems.at[0]),
        pltpu.make_async_copy(right_in.at[:split], right_ref.at[:split], sems.at[1]),
        pltpu.make_async_copy(diff_in, diff_ref, sems.at[2]),
        pltpu.make_async_copy(vel_in, vel_ref, sems.at[3]),
    ]
    for copy in copies:
        copy.start()
    copies[0].wait()
    window, own, halo = plan.window, plan.own, plan.halo
    parts = plan.cols // LANE
    lane = lane_of((SUB, LANE))
    group, spot = lane // window, lane % window
    edge = LANE - (SUB - 1) * window - own + halo

    def strips():
        for parity in range(2):
            for part in range(parts):
                for m in range(SUB):
                    yield parity, part, m, plan.holder[2 * (part * SUB + m) + parity]

    def body(k, carry):
        a = plan.tiles - 1 - k
        fields = [right_ref[a * SUB + i] for i in range(SUB)]
        cache = {}

        def turned(i, part, amount):
            key = (i, part % parts, amount % LANE)
            if key not in cache:
                block = fields[i][:, key[1] * LANE : (key[1] + 1) * LANE]
                cache[key] = spin(block, amount)
            return cache[key]

        pieces = []
        for parity, part, m, _ in strips():
            base = parity * own - halo
            total = None
            for i in range(SUB):
                amount = window * (i - m) - base
                value = turned(i, part, amount)
                if parity == 0 and m == 0:
                    value = jnp.where(spot < halo, turned(i, part - 1, amount), value)
                if parity == 1 and m == SUB - 1:
                    value = jnp.where(spot >= edge, turned(i, part + 1, amount), value)
                total = value if total is None else jnp.where(group == i, value, total)
            pieces.append(total)

        @pl.when(k == 0)
        def _():
            for index, piece in enumerate(pieces):
                tail_ref[index] = piece
            copies[1].wait()

        @pl.when(k > 0)
        def _():
            amount = plan.used - plan.spare * a
            for index, (_, _, _, target) in enumerate(strips()):
                tail = pltpu.roll(tail_ref[index], amount, 1)
                piece = jnp.where(spot >= plan.used, tail, pieces[index])
                out_ref[pl.ds(target * plan.inward + a * SUB, SUB), :] = piece

        return carry

    lax.fori_loop(0, plan.tiles, body, 0)
    copies[2].wait()
    copies[3].wait()
    row = pl.ds(lax.axis_index("tm"), 1)
    lines = [diff_ref[row, :], vel_ref[0, row, :], vel_ref[1, row, :]]
    sub = lax.broadcasted_iota(jnp.int32, (SUB, LANE), 0)
    blocks = [
        [jnp.broadcast_to(line[:, h * LANE : (h + 1) * LANE], (SUB, LANE)) for h in range(parts)]
        for line in lines
    ]
    for parity in range(2):
        base = parity * own - halo
        for part in range(parts):
            total = jnp.zeros((SUB, LANE), jnp.float32)
            for f in range(len(lines)):
                amount = (f + 1) * window - base

                def slanted(h):
                    flat = spin(blocks[f][h % parts], amount)
                    return pltpu.roll(flat, 0, 1, stride=window, stride_axis=0)

                value = slanted(part)
                if parity == 0:
                    value = jnp.where((sub == SUB - 1) & (spot < halo), slanted(part - 1), value)
                else:
                    value = jnp.where((sub == 0) & (spot >= edge), slanted(part + 1), value)
                total = jnp.where(group == f, value, total)
            for m in range(SUB):
                target = plan.holder[2 * (part * SUB + m) + parity]
                at = target * plan.inward + plan.inward - 1
                out_ref[at : at + 1, :] = total[SUB - 1 - m : SUB - m]


def totals_of(ref):
    return jnp.sum(ref[...], axis=0, keepdims=True) * (1.0 / (damping * damping))


def pick(totals, k):
    lane = lane_of(totals.shape)
    value = jnp.sum(jnp.where(lane == k, totals, 0.0), axis=1, keepdims=True)
    return jnp.broadcast_to(value, (1, LANE))


def middle(totals):
    aa, ab, bb, ac, bc = (pick(totals, k) for k in range(5))
    scale = 1.0 / (aa + epsilon)
    drop = scale * ab
    norm = jnp.maximum(bb - drop * (2.0 * ab - drop * aa), 1e-5 * bb)
    over = ac - drop * ab
    along = bc - drop * (bb + ac - drop * ab)
    return aa, drop, scale * over, scale * along / (scale * norm + epsilon)


def iterate(middle_totals, totals):
    aa, drop, over, along = middle(middle_totals)
    pairs = [(0, 1), (1, 1), (0, 2), (1, 2), (2, 2), (0, 3), (1, 3), (2, 3), (3, 3)]
    gram = {(0, 0): aa}
    for k, (i, j) in enumerate(pairs):
        gram[i, j] = gram[j, i] = pick(totals, k)
    zero = jnp.zeros_like(aa)
    one = jnp.ones_like(aa)
    images = [[drop, one, zero, zero], [over, along, one, zero], [zero, zero, zero, one]]
    size = KRYLOV + 1

    def product(left, right):
        return sum(left[i] * right[j] * gram[i, j] for i in range(size) for j in range(size))

    beta = jnp.sqrt(aa + epsilon)
    basis = [[1.0 / beta, zero, zero, zero]]
    hessen = [[zero] * KRYLOV for row in range(size)]
    for j in range(KRYLOV):
        image = [sum(basis[j][k] * images[k][i] for k in range(KRYLOV)) for i in range(size)]
        found = [product(basis[i], image) for i in range(j + 1)]
        for i in range(j + 1):
            hessen[i][j] = found[i]
            image = [w - found[i] * v for w, v in zip(image, basis[i])]
        length = jnp.sqrt(jnp.maximum(product(image, image), 0.0) + epsilon)
        hessen[j + 1][j] = length
        basis.append([w / length for w in image])
    ortho = []
    upper = [[None] * KRYLOV for row in range(KRYLOV)]
    for column in range(KRYLOV):
        current = [hessen[row][column] for row in range(size)]
        for row in range(column):
            factor = sum(x * y for x, y in zip(ortho[row], current))
            upper[row][column] = factor
            current = [y - factor * x for x, y in zip(ortho[row], current)]
        length = jnp.sqrt(sum(y * y for y in current))
        upper[column][column] = length
        ortho.append([y / length for y in current])
    values = [None] * KRYLOV
    for row in reversed(range(KRYLOV)):
        accum = ortho[row][0] * beta
        for later in range(row + 1, KRYLOV):
            accum = accum - upper[row][later] * values[later]
        values[row] = accum / upper[row][row]
    weights = [sum(values[j] * basis[j][k] for j in range(KRYLOV)) for k in range(KRYLOV)]
    weights[0] = weights[0] - drop * weights[1]
    return weights


def coefficients(plan, recv_ref, strip, table_ref):
    window = plan.window
    lane = lane_of((SUB, LANE))
    stride = plan.space * plan.inward
    lines = [
        recv_ref[pl.ds(s * plan.inward + plan.inward - 1, SUB, stride), :]
        for s in range(plan.space)
    ]
    fields = []
    for f in range(3):
        parts = []
        for line in lines:
            part = None
            for g in range(plan.tm):
                moved = spin(line, (g - f) * window)
                part = moved if g == 0 else jnp.where(lane // window == g, moved, part)
            parts.append(part)
        fields.append(jnp.concatenate(parts, axis=0))
    diff, vel_col, vel_row = fields
    shape = (plan.rows, LANE)
    row = lax.broadcasted_iota(jnp.int32, shape, 0)
    col = strip * plan.own - plan.halo + lane_of(shape) % window
    center = 1.0 + 4.0 * diff
    table_ref[0] = damping * center
    table_ref[1] = 1.0 / center
    table_ref[2] = jnp.where(row > 0, damping * (diff + vel_row), 0.0)
    table_ref[3] = jnp.where(row < plan.rows - 1, damping * (diff - vel_row), 0.0)
    table_ref[4] = jnp.where(col > 0, damping * (diff + vel_col), 0.0)
    table_ref[5] = jnp.where(col < plan.cols - 1, damping * (diff - vel_col), 0.0)


def krylov_kernel(plan, j, *refs):
    refs = list(refs)
    strip = plan.strip_of(lax.axis_index("tm"), lax.axis_index("space"))
    here, window, rows, halo, own = plan.here, plan.window, plan.rows, plan.halo, plan.own
    slot = plan.slot
    final = j == KRYLOV - 1
    shape = (rows, LANE)
    lane = lane_of(shape)
    low_lane = lane_of((SUB, LANE))
    low_spot = low_lane & (window - 1)
    even = strip % 2 == 0
    if j == 0:
        recv_ref, table_ref, q_ref, g_ref, w_ref, near_ref, far_ref, y_ref, tail_ref = refs
        coefficients(plan, recv_ref, strip, table_ref)
    elif not final:
        table_ref, image_ref, near_in, far_in, first_ref = refs[:5]
        q_ref, g_ref, w_ref, near_ref, far_ref, sum_ref, y_ref = refs[5:]
    else:
        table_ref, image_ref, near_in, far_in, first_ref, second_ref, mid_ref = refs[:7]
        g_ref, sum_ref, y_ref, q_ref, w_ref, rest_ref = refs[7:]
        _, drop, over, along = middle(totals_of(mid_ref))
    center = table_ref[0]
    inverse = table_ref[1]
    north, south, west, east = (table_ref[2 + k] for k in range(4))
    zero = jnp.zeros(shape, jnp.float32)
    low_zero = jnp.zeros((SUB, LANE), jnp.float32)
    inner = slice(SUB, SUB + rows)

    def around(n, field):
        return (
            north * g_ref[n, SUB - 1 : SUB - 1 + rows, :]
            + south * g_ref[n, SUB + 1 : SUB + 1 + rows, :]
            + west * spin(field, 1)
            + east * spin(field, -1)
        )

    power = inverse
    for _ in range(int(math.log2(here))):
        power = power * power
    whole = power
    for _ in range(int(math.log2(plan.tm))):
        whole = whole * whole
    closing = 1.0 / (1.0 - alpha_corner * whole)

    def entering(ends):
        total = alpha_corner * ends
        for k in reversed(range(1, plan.tm)):
            back = spin(ends, k * window)
            total = total * power + jnp.where(lane < k * window, alpha_corner * back, back)
        return total * closing

    def settle(base, y):
        for k in range(UNROLL):
            y = (y_ref[base + k] + y) * inverse
            y_ref[base + k] = y
        return y

    for k in range(UNROLL):
        y_ref[k] = zero

    def blank(n):
        g_ref[n] = jnp.zeros((rows + 2 * SUB, LANE), jnp.float32)

    if j == 0:
        last_tile = plan.tiles - 1

        def tails(k, carry):
            for p in (4 * k, 4 * k + 1, 4 * k + 2, 4 * k + 3):
                for s in range(plan.space):
                    source = p * plan.space + s
                    total = low_zero
                    for a in range(last_tile):
                        tile = recv_ref[pl.ds(source * plan.inward + a * SUB, SUB), :]
                        moved = spin(tile, plan.spare * a - plan.used)
                        total = jnp.where(low_spot // plan.spare == a, moved, total)
                    tail_ref[source] = total
            return carry

        lax.fori_loop(0, plan.tm // 4, tails, 0)

        def first(k, y):
            parts = [[] for _ in range(PAIR)]
            for t in range(PAIR):
                a = k * PAIR + t
                whole = a < last_tile
                at = jnp.minimum(a, last_tile - 1) * SUB
                for s in range(plan.space):
                    cut = []
                    for p in range(plan.tm):
                        source = p * plan.space + s
                        tile = recv_ref[pl.ds(source * plan.inward + at, SUB), :]
                        cut.append(damping * jnp.where(whole, tile, tail_ref[source]))
                    parts[t].append(exchange_blocks(cut, window, 2))
            for t in range(PAIR):
                for i in range(SUB):
                    n = (k * PAIR + t) * SUB + i
                    q = jnp.concatenate([part[i] for part in parts[t]], axis=0)
                    q_ref[n] = q
                    y = (q + y) * inverse
                    y_ref[UNROLL + n] = y
                    blank(n)
            return y

        y = lax.fori_loop(0, plan.tiles // PAIR, first, zero)
    else:
        right_mask = (low_spot >= halo + own) & (low_spot < halo + own + halo)
        left_mask = low_spot < halo

        def first(i, y):
            base = i * UNROLL
            y = settle(base, y)
            for k in range(UNROLL):
                n = base + k
                near, far = near_in[n], far_in[n]
                right = jnp.where(even, near, far)
                left = jnp.where(even, far, near)
                image = image_ref[n]
                parts = []
                for s in range(plan.space):
                    part = image[s * SUB : (s + 1) * SUB]
                    part = jnp.where(right_mask, spin(right, halo + own - slot * s), part)
                    part = jnp.where(left_mask, spin(left, halo - own - slot * s), part)
                    parts.append(part)
                q = jnp.concatenate(parts, axis=0)
                if final:
                    start, later = first_ref[n], second_ref[n]
                    rest = later - drop * start
                    rest_ref[n] = rest
                    q = (q - drop * later) - over * start - along * rest
                q_ref[n] = q
                y_ref[UNROLL + n] = q
                blank(n)
            return y

        y = settle(here, lax.fori_loop(0, here // UNROLL, first, zero))

    def sweep(_, ends):
        def body(i, carry):
            y, z = carry
            base = i * UNROLL
            olds = [y_ref[UNROLL + base + k] for k in range(UNROLL)]
            y = settle(base, y)
            for k in range(UNROLL):
                n = base + k
                z = z * inverse
                guess = (1.0 - damping) * g_ref[n, inner, :] + (olds[k] + z)
                g_ref[n, inner, :] = guess
                y_ref[UNROLL + n] = q_ref[n] + around(n, guess)
            return (y, z)

        y, _ = lax.fori_loop(0, here // UNROLL, body, (zero, entering(ends)))
        return settle(here, y)

    y = lax.fori_loop(0, SWEEPS - 1, sweep, y)
    start = entering(y)
    ending = (1.0 - damping) * g_ref[here - 1, inner, :] + (y + start * power)
    before = jnp.where(lane < window, 0.0, damping * spin(ending, window))

    ahead = [
        ((low_lane - slot * s - (own - halo)) & (window - 1)) < halo for s in range(plan.space)
    ]

    def fold(block):
        return sum(block[s * SUB : (s + 1) * SUB] for s in range(plan.space))

    size = KRYLOV + 1

    def gather(base, accs):
        for k in range(UNROLL):
            n = base + k
            image = w_ref[n]
            if not final:
                left = right = None
                for s in range(plan.space):
                    moved = spin(image[s * SUB : (s + 1) * SUB], slot * s - halo)
                    left = moved if s == 0 else jnp.where(low_spot // slot == s, moved, left)
                    right = moved if s == 0 else jnp.where(ahead[s], moved, right)
                near_ref[n] = jnp.where(even, right, left)
                far_ref[n] = jnp.where(even, left, right)
            if j == 0:
                continue
            q = q_ref[n]
            start = first_ref[n]
            if not final:
                pairs = [(start, start), (start, q), (q, q), (start, image), (q, image)]
            else:
                rest = rest_ref[n]
                held = [start, rest, q, image]
                pairs = [(held[i], held[k]) for k in range(1, size) for i in range(k + 1)]
            accs = [acc + fold(x * y) for acc, (x, y) in zip(accs, pairs)]
        return accs

    def last(i, carry):
        z, before, accs = carry
        accs = gather(jnp.maximum(i - 1, 0) * UNROLL, accs)
        accs = tuple(jnp.where(i > 0, acc, 0.0) for acc in accs)
        for k in range(UNROLL):
            n = i * UNROLL + k
            z = z * inverse
            guess = (1.0 - damping) * g_ref[n, inner, :] + (y_ref[UNROLL + n] + z)
            g_ref[n, inner, :] = guess
            w_ref[n] = center * guess - around(n, guess) - before
            before = damping * guess
        return (z, before, accs)

    fields = (0, 5, 9)[j]
    _, _, accs = lax.fori_loop(0, here // UNROLL, last, (start, before, (low_zero,) * fields))
    accs = gather(here - UNROLL, list(accs))
    if j == 0:
        return
    owned = (low_spot >= halo) & (low_spot < halo + own)
    record = jnp.zeros((1, LANE), jnp.float32)
    record_lane = lane_of((1, LANE))
    for place, acc in enumerate(accs):
        value = jnp.sum(jnp.where(owned, acc, 0.0), axis=0, keepdims=True)
        value = jnp.sum(value, axis=1, keepdims=True)
        record = jnp.where(record_lane == place, value, record)
    sum_ref[...] = jnp.broadcast_to(record, sum_ref.shape)


def combine_kernel(plan, *refs):
    z_refs = refs[:KRYLOV]
    mid_ref, end_ref, out_ref = refs[KRYLOV:]
    along = iterate(totals_of(mid_ref), totals_of(end_ref))
    own, halo, window, groups = plan.own, plan.halo, plan.window, plan.groups
    lane = lane_of((SUB, LANE))
    front = lane % window < own
    size = plan.outward

    def start_of(p, s):
        return (p * plan.space + s) * size

    def value(n, s):
        here = slice((s + 1) * SUB, (s + 2) * SUB)
        return sum(c * ref[n, here, :] for c, ref in zip(along, z_refs))

    def body(k, carry):
        for t in range(PAIR):
            aa = k * PAIR + t
            for s in range(plan.space):
                pieces = []
                for i in range(SUB):
                    n = aa * 2 * SUB + 2 * i
                    left, right = spin(value(n, s), -halo), spin(value(n + 1, s), own - halo)
                    pieces.append(jnp.where(front, left, right))
                for p, piece in enumerate(exchange_blocks(pieces, window, 2)):
                    out_ref[pl.ds(start_of(p, s) + aa * SUB, SUB), :] = piece
                    if s + 1 < plan.space:
                        at = start_of(p, s + 1) + groups * SUB + aa
                        out_ref[pl.ds(at, 1), :] = piece[SUB - 1 :]
                    if s > 0:
                        at = start_of(p, s - 1) + groups * SUB + groups + aa
                        out_ref[pl.ds(at, 1), :] = piece[:1]
        return carry

    lax.fori_loop(0, groups // PAIR, body, 0)
    nothing = jnp.zeros((groups, LANE), jnp.float32)
    sub = lax.broadcasted_iota(jnp.int32, (SUB, LANE), 0)
    for p in range(plan.tm):
        at = start_of(p, 0) + groups * SUB
        out_ref[at : at + groups, :] = nothing
        at = start_of(p, plan.space - 1) + groups * SUB + groups
        out_ref[at : at + groups, :] = nothing
    for s in range(plan.space):
        ending = value(plan.here - 1, s)
        for p in range(plan.tm):
            line = nothing[:1]
            if p > 0:
                turned = spin(ending, -(p - 1) * window - halo)
                turned = pltpu.roll(turned, 0, 1, stride=own, stride_axis=0)
                line = jnp.sum(jnp.where(lane // own == sub, turned, 0.0), axis=0, keepdims=True)
            at = start_of(p, s) + size - 1
            out_ref[at : at + 1, :] = line


def finish_kernel(plan, recv_ref, right_ref, diff_ref, vel_ref, *refs):
    results, (rim_ref, out_ref, rest_ref, sems) = refs[:2], refs[2:]
    groups, own, size = plan.groups, plan.own, plan.outward
    count = LANE // own
    parts = plan.cols // LANE
    shape = (SUB, plan.cols)
    lane = lane_of((SUB, LANE))
    diff, vel_col, vel_row = diff_ref[...], vel_ref[0], vel_ref[1]
    col = lane_of(shape)
    sub = lax.broadcasted_iota(jnp.int32, shape, 0)
    center = 1.0 + 4.0 * diff
    north = diff + vel_row
    south = diff - vel_row
    west = jnp.where(col > 0, diff + vel_col, 0.0)
    east = jnp.where(col < plan.cols - 1, diff - vel_col, 0.0)

    def start_of(part, m):
        return plan.holder[part * count + m] * size

    def spread(offset):
        wide = []
        for part in range(parts):
            pieces = [
                recv_ref[pl.ds(start_of(part, m) + offset, SUB), :] for m in range(count)
            ]
            wide.append(exchange_blocks(pieces, own, 2))
        return [jnp.concatenate(pair, axis=1) for pair in zip(*wide)]

    for i, field in enumerate(spread(groups * SUB)):
        rim_ref[i] = field
    halves = []
    row = lax.broadcasted_iota(jnp.int32, (SUB, LANE), 0)
    for part in range(parts):
        tiles = []
        for first in range(0, count, SUB):
            tile = jnp.zeros((SUB, LANE), jnp.float32)
            for q in range(SUB):
                at = start_of(part, first + q) + size - 1
                line = jnp.broadcast_to(recv_ref[at : at + 1, :], (SUB, LANE))
                tile = jnp.where(row == q, line, tile)
            tile = spin(tile, first * own)
            tiles.append((first, pltpu.roll(tile, 0, 1, stride=own, stride_axis=0)))
        total = jnp.zeros((SUB, LANE), jnp.float32)
        for r in range(SUB):
            line = sum(
                jnp.where(lane // own == row + first, spin(tile, -r * own), 0.0)
                for first, tile in tiles
            )
            line = jnp.sum(line, axis=0, keepdims=True)
            total = jnp.where(row == r, jnp.broadcast_to(line, (SUB, LANE)), total)
        halves.append(total)
    before = jnp.concatenate(halves, axis=1)

    size_of = PAIR * count

    def copies(k):
        at = pl.ds(k * size_of, size_of)
        return [
            pltpu.make_async_copy(ref.at[at], result.at[at], sems.at[k, f])
            for f, (ref, result) in enumerate(zip((out_ref, rest_ref), results))
        ]

    def body(k, before):
        for t in range(PAIR):
            aa = k * PAIR + t
            for i, field in enumerate(spread(aa * SUB)):
                n = aa * count + i
                above = rim_ref[i, pl.ds(aa, 1), :]
                below = rim_ref[i, pl.ds(groups + aa, 1), :]
                out_ref[n] = field
                around = (
                    north * jnp.where(sub == 0, above, spin(field, 1, 0))
                    + south * jnp.where(sub == SUB - 1, below, spin(field, -1, 0))
                    + west * spin(field, 1)
                    + east * spin(field, -1)
                )
                rest_ref[n] = right_ref[n] - (center * field - around - before)
                before = field
        for copy in copies(k):
            copy.start()
        return before

    lax.fori_loop(0, groups // PAIR, body, before)
    for k in range(groups // PAIR):
        for copy in copies(k):
            copy.wait()


def call(kernel, shapes, operands, scratch=(), sems=None, far_in=False, far_out=False, room=16):
    vmem = pl.BlockSpec(memory_space=pltpu.VMEM)
    hbm = pl.BlockSpec(memory_space=pltpu.HBM)
    held = [pltpu.VMEM(shape, jnp.float32) for shape in scratch]
    if sems:
        held.append(pltpu.SemaphoreType.DMA(sems))
    return pl.pallas_call(
        kernel,
        out_shape=[jax.ShapeDtypeStruct(shape, jnp.float32) for shape in shapes],
        in_specs=[hbm if far_in else vmem] * len(operands),
        out_specs=[hbm if far_out else vmem] * len(shapes),
        scratch_shapes=held,
        compiler_params=pltpu.CompilerParams(vmem_limit_bytes=room * 1024 * 1024),
    )(*operands)


def everyone(block, devices):
    lines = block.shape[0] // devices
    parts = block.reshape(devices, lines, 1, LANE)
    return lax.all_to_all(parts, AXES, split_axis=0, concat_axis=0, tiled=True).reshape(block.shape)


def strip_device(plan, right_side, diffusion, velocity):
    count = plan.devices
    hold = plan.holder
    near_route = []
    far_route = []
    for k in range(0, count, 2):
        near_route += [(hold[k], hold[k + 1]), (hold[k + 1], hold[k])]
    for k in range(1, count - 1, 2):
        far_route += [(hold[k], hold[k + 1]), (hold[k + 1], hold[k])]
    bind = lambda kernel, *more: (lambda *refs: kernel(plan, *more, *refs))
    full = (plan.here, plan.rows, LANE)
    padded = (plan.here, plan.rows + 2 * SUB, LANE)
    delayed = (plan.here + UNROLL, plan.rows, LANE)
    side = (plan.here, SUB, LANE)
    small = (count, LANE)
    given = [right_side, diffusion, velocity]
    sent = call(
        bind(pack_kernel),
        [(count * plan.inward, LANE)],
        given,
        scratch=[(count, SUB, LANE), *(block.shape for block in given)],
        sems=(4,),
        far_in=True,
        room=63,
    )[0]
    table, q0, z0, image, near, far = call(
        bind(krylov_kernel, 0),
        [(6, plan.rows, LANE), full, padded, full, side, side],
        [everyone(sent, count)],
        scratch=[delayed, (count, SUB, LANE)],
    )
    near = lax.ppermute(near, AXES, near_route)
    far = lax.ppermute(far, AXES, far_route)
    q1, z1, image, near, far, sums = call(
        bind(krylov_kernel, 1),
        [full, padded, full, side, side, small],
        [table, image, near, far, q0],
        scratch=[delayed],
    )
    near = lax.ppermute(near, AXES, near_route)
    far = lax.ppermute(far, AXES, far_route)
    mid = everyone(sums, count)
    z2, sums = call(
        bind(krylov_kernel, 2),
        [padded, small],
        [table, image, near, far, q0, q1, mid],
        scratch=[delayed, full, full, full],
    )
    end = everyone(sums, count)
    packed = call(bind(combine_kernel), [(count * plan.outward, LANE)], [z0, z1, z2, mid, end])[0]
    shape = right_side.shape
    return tuple(
        call(
            bind(finish_kernel),
            [shape, shape],
            [everyone(packed, count), *given],
            scratch=[(2 * SUB, SUB, plan.cols), shape, shape],
            sems=(plan.groups // PAIR, 2),
            far_out=True,
        )
    )


def per_device(mesh):
    def run(right_side, diffusion, velocity):
        rows = right_side.shape[1] * mesh.shape["space"]
        steps = right_side.shape[0] * mesh.shape["tm"]
        plan = Plan(mesh, steps, rows, right_side.shape[2])
        if plan.fits():
            return strip_device(plan, right_side, diffusion, velocity)
        return generic_device(right_side, diffusion, velocity)

    return run


def solution(mesh):
    placed = (P("tm", "space", None), P("space", None), P(None, "space", None))
    return jax.shard_map(
        per_device(mesh),
        mesh=mesh,
        in_specs=placed,
        out_specs=(P("tm", "space", None), P("tm", "space", None)),
        check_vma=False,
    )
```

```python
import math

import jax
import jax.numpy as jnp
from jax import lax
from jax.experimental import pallas as pl
from jax.experimental.pallas import tpu as pltpu
from jax.sharding import PartitionSpec as P

L = 512
KRYLOV = 3
SWEEPS = 3


alpha_corner = 0.05
damping = 0.8
epsilon = 1e-06
highest = lax.Precision.HIGHEST


def extended(block, sides, width):
    for axis, dim in sides:
        count = lax.axis_size(axis)
        forward = [(i, i + 1) for i in range(count - 1)]
        backward = [(target, source) for source, target in forward]
        low = lax.ppermute(
            lax.slice_in_dim(block, block.shape[dim] - width, None, axis=dim), axis, forward
        )
        high = lax.ppermute(lax.slice_in_dim(block, 0, width, axis=dim), axis, backward)
        block = jnp.concatenate([low, block, high], axis=dim)
    return block


def from_behind(block, axis, distance):
    devices = range(lax.axis_size(axis))
    route = [(i - distance, i) for i in devices if i - distance in devices]
    return lax.ppermute(block, axis, route)


def shifted(padded, row_dim, col_dim, rows, cols, row_start, col_start):
    piece = lax.slice_in_dim(padded, row_start, row_start + rows, axis=row_dim)
    return lax.slice_in_dim(piece, col_start, col_start + cols, axis=col_dim)


def stencil(field, padded, row_dim, col_dim, diffusion, velocity_col, velocity_row):
    rows = field.shape[row_dim]
    cols = field.shape[col_dim]
    north = shifted(padded, row_dim, col_dim, rows, cols, 0, 1)
    south = shifted(padded, row_dim, col_dim, rows, cols, 2, 1)
    west = shifted(padded, row_dim, col_dim, rows, cols, 1, 0)
    east = shifted(padded, row_dim, col_dim, rows, cols, 1, 2)
    return (
        (1.0 + 4.0 * diffusion) * field
        - diffusion * (north + south + west + east)
        + velocity_col * (east - west)
        + velocity_row * (south - north)
    )


def divided(real_part, imag_part, diag_real, diag_imag, modulus):
    return (
        damping * (real_part * diag_real + imag_part * diag_imag) / modulus,
        damping * (imag_part * diag_real - real_part * diag_imag) / modulus,
    )


def remainder(
    source_real, source_imag, image_real, image_imag, guess_real, guess_imag, shift_real, shift_imag
):
    return (
        source_real - (image_real - (shift_real * guess_real + shift_imag * guess_imag)),
        source_imag - (image_imag - (shift_real * guess_imag - shift_imag * guess_real)),
    )


def dft_tables(length):
    index = jnp.arange(length, dtype=jnp.int32)
    product = index[:, None] * index[None, :] % length
    angle = product.astype(jnp.float32) * (2.0 * math.pi / length)
    return (jnp.cos(angle), jnp.sin(angle))


def least_squares(hessen, beta):
    ortho = []
    upper = [[None] * KRYLOV for row in range(KRYLOV)]
    for column in range(KRYLOV):
        current = hessen[:, column]
        for row in range(column):
            factor = jnp.sum(ortho[row] * current)
            upper[row][column] = factor
            current = current - factor * ortho[row]
        length = jnp.sqrt(jnp.sum(current * current))
        upper[column][column] = length
        ortho.append(current / length)
    target = [ortho[row][0] * beta for row in range(KRYLOV)]
    values = [None] * KRYLOV
    for row in reversed(range(KRYLOV)):
        accum = target[row]
        for later in range(row + 1, KRYLOV):
            accum = accum - upper[row][later] * values[later]
        values[row] = accum / upper[row][row]
    return jnp.stack(values)


def generic_device(right_side, diffusion, velocity):
    steps_here = right_side.shape[0]
    devices_tm = lax.axis_size("tm")
    position = lax.axis_index("tm")
    log_decay = math.log(alpha_corner) / L
    decay = math.exp(log_decay)
    local_steps = position * steps_here + jnp.arange(steps_here, dtype=jnp.int32)
    times = local_steps.astype(jnp.float32)
    weights = jnp.exp(times * log_decay)[:, None, None]
    unweights = jnp.exp(-times * log_decay)[:, None, None]
    cosine, sine = dft_tables(L)
    velocity_col = velocity[0]
    velocity_row = velocity[1]
    width = right_side.shape[2] // devices_tm
    start = position * width
    diff_strip = lax.dynamic_slice_in_dim(diffusion, start, width, 1)[:, :, None]
    col_strip = lax.dynamic_slice_in_dim(velocity_col, start, width, 1)[:, :, None]
    row_strip = lax.dynamic_slice_in_dim(velocity_row, start, width, 1)[:, :, None]
    angles = jnp.arange(L, dtype=jnp.int32).astype(jnp.float32) * (2.0 * math.pi / L)
    shift_real = decay * jnp.cos(angles)
    shift_imag = decay * jnp.sin(angles)
    diag_real = 1.0 + 4.0 * diff_strip - shift_real
    modulus = diag_real * diag_real + shift_imag * shift_imag

    def forward(block):
        real_part = jnp.dot(block, cosine, precision=highest)
        imag_part = -jnp.dot(block, sine, precision=highest)
        return jnp.concatenate([real_part, imag_part], axis=2)

    total = lax.psum(jnp.sum(right_side * right_side), ("tm", "space"))
    beta = jnp.sqrt(total + epsilon)
    basis = [right_side / beta]
    prepared = []
    hessen = jnp.zeros((KRYLOV + 1, KRYLOV), jnp.float32)
    for column in range(KRYLOV):
        moved = jnp.transpose(basis[column] * weights, (1, 2, 0))
        spectrum = forward(lax.all_to_all(moved, "tm", split_axis=1, concat_axis=2, tiled=True))
        source_real = spectrum[:, :, :L]
        source_imag = spectrum[:, :, L:]
        guess_real, guess_imag = divided(source_real, source_imag, diag_real, shift_imag, modulus)
        for sweep in range(SWEEPS - 1):
            joined = jnp.concatenate([guess_real, guess_imag], axis=2)
            padded = extended(joined, (("tm", 1), ("space", 0)), 1)
            image = stencil(joined, padded, 0, 1, diff_strip, col_strip, row_strip)
            left_real, left_imag = remainder(
                source_real,
                source_imag,
                image[:, :, :L],
                image[:, :, L:],
                guess_real,
                guess_imag,
                shift_real,
                shift_imag,
            )
            step_real, step_imag = divided(left_real, left_imag, diag_real, shift_imag, modulus)
            guess_real = guess_real + step_real
            guess_imag = guess_imag + step_imag
        back = (
            jnp.dot(guess_real, cosine, precision=highest)
            - jnp.dot(guess_imag, sine, precision=highest)
        ) / L
        back = lax.all_to_all(back, "tm", split_axis=2, concat_axis=1, tiled=True)
        direction = jnp.transpose(back, (2, 0, 1)) * unweights
        prepared.append(direction)
        apply_padded = extended(direction, (("space", 1),), 1)
        apply_padded = jnp.pad(apply_padded, ((0, 0), (0, 0), (1, 1)))
        apply_image = stencil(direction, apply_padded, 1, 2, diffusion, velocity_col, velocity_row)
        earlier = from_behind(direction[-1:], "tm", 1)
        image = apply_image - jnp.concatenate([earlier, direction[:-1]], axis=0)
        local = jnp.stack([jnp.sum(vector * image) for vector in basis])
        projections = lax.psum(local, ("tm", "space"))
        for row in range(column + 1):
            image = image - projections[row] * basis[row]
        squares = lax.psum(jnp.sum(image * image), ("tm", "space"))
        length = jnp.sqrt(squares + epsilon)
        hessen = hessen.at[: column + 1, column].set(projections)
        hessen = hessen.at[column + 1, column].set(length)
        basis.append(image / length)
    coeffs = least_squares(hessen, beta)
    solution = prepared[0] * coeffs[0]
    for column in range(1, KRYLOV):
        solution = solution + prepared[column] * coeffs[column]
    first = (jnp.arange(KRYLOV + 1) == 0).astype(jnp.float32)
    target = beta * first - jnp.sum(hessen * coeffs[None, :], axis=1)
    residual = basis[0] * target[0]
    for row in range(1, KRYLOV + 1):
        residual = residual + basis[row] * target[row]
    return (solution, residual)


SUB = 8
LANE = 128
AXES = ("tm", "space")
UNROLL = 32
PAIR = 2


def spin(block, amount, axis=1):
    return pltpu.roll(block, amount % block.shape[axis], axis)


def lane_of(shape):
    return lax.broadcasted_iota(jnp.int32, shape, 1)


def exchange_blocks(pieces, width, radix):
    pieces = list(pieces)
    lane = lane_of(pieces[0].shape)
    step = 1
    while step < len(pieces):
        digit = lane // (width * step) % radix
        result = list(pieces)
        for i in range(len(pieces)):
            e = i // step % radix
            total = None
            for d in range(radix):
                moved = pieces[i + (d - e) * step]
                if d != e:
                    moved = spin(moved, (d - e) * step * width)
                total = moved if total is None else jnp.where(digit == d, moved, total)
            result[i] = total
        pieces = result
        step *= radix
    return pieces


class Plan:
    def __init__(self, mesh, steps, rows, cols):
        self.tm = mesh.shape["tm"]
        self.space = mesh.shape["space"]
        self.devices = self.tm * self.space
        self.steps = steps
        self.rows = rows
        self.cols = cols
        self.here = steps // self.tm
        self.window = LANE // self.tm
        self.own = cols // self.devices
        self.halo = SWEEPS
        self.slot = self.window // self.space
        self.used = self.own + 2 * self.halo
        self.spare = self.window - self.used
        self.tiles = self.here // SUB
        self.inward = (self.tiles - 1) * SUB + 1
        self.groups = self.here // (2 * SUB)
        self.outward = self.groups * SUB + 2 * self.groups + 1
        self.ring = [self.strip_of(d // self.space, d % self.space) for d in range(self.devices)]
        self.holder = [self.ring.index(j) for j in range(self.devices)]

    def fits(self):
        return (
            LANE % self.tm == 0
            and self.tm == SUB
            and self.rows == SUB * self.space
            and self.cols % self.devices == 0
            and self.cols == 2 * LANE
            and self.steps % (self.tm * 2 * SUB) == 0
            and self.window == 2 * self.own
            and self.spare * (self.tiles - 1) == self.used
            and self.here % UNROLL == 0
            and self.groups * 2 == SUB
            and self.slot >= self.halo
            and self.space % 2 == 0
            and KRYLOV == 3
            and self.tiles % PAIR == 0
            and self.groups % PAIR == 0
            and self.tm % 4 == 0
        )

    def strip_of(self, t, s):
        turn = t ^ ((t >> 1) & 1)
        half = self.space // 2
        x, core = s // 2, s % 2
        odd = turn % 2
        return (turn * half + x + odd * (half - 1 - 2 * x)) * 2 + core


def pack_kernel(plan, right_in, diff_in, vel_in, out_ref, *scratch):
    tail_ref, right_ref, diff_ref, vel_ref, sems = scratch
    split = plan.here - SUB
    copies = [
        pltpu.make_async_copy(right_in.at[split:], right_ref.at[split:], sems.at[0]),
        pltpu.make_async_copy(right_in.at[:split], right_ref.at[:split], sems.at[1]),
        pltpu.make_async_copy(diff_in, diff_ref, sems.at[2]),
        pltpu.make_async_copy(vel_in, vel_ref, sems.at[3]),
    ]
    for copy in copies:
        copy.start()
    copies[0].wait()
    window, own, halo = plan.window, plan.own, plan.halo
    parts = plan.cols // LANE
    lane = lane_of((SUB, LANE))
    group, spot = lane // window, lane % window
    edge = LANE - (SUB - 1) * window - own + halo

    def strips():
        for parity in range(2):
            for part in range(parts):
                for m in range(SUB):
                    yield parity, part, m, plan.holder[2 * (part * SUB + m) + parity]

    def windows(a):
        pieces = []
        fields = [right_ref[a * SUB + i] for i in range(SUB)]
        for parity in range(2):
            turned = [spin(field, halo - parity * own) for field in fields]
            for part in range(parts):
                cut = [field[:, part * LANE : (part + 1) * LANE] for field in turned]
                pieces += exchange_blocks(cut, window, 2)
        return pieces

    def spread(a, pieces):
        amount = plan.used - plan.spare * a
        for index, (_, _, _, target) in enumerate(strips()):
            tail = pltpu.roll(tail_ref[index], amount, 1)
            piece = jnp.where(spot >= plan.used, tail, pieces[index])
            out_ref[pl.ds(target * plan.inward + a * SUB, SUB), :] = piece

    for index, piece in enumerate(windows(plan.tiles - 1)):
        tail_ref[index] = piece
    copies[1].wait()

    def body(k, carry):
        both = [(a, windows(a)) for a in (2 * k, 2 * k + 1)]
        for a, pieces in both:
            spread(a, pieces)
        return carry

    lax.fori_loop(0, (plan.tiles - 1) // 2, body, 0)
    for a in range((plan.tiles - 1) // 2 * 2, plan.tiles - 1):
        spread(a, windows(a))
    copies[2].wait()
    copies[3].wait()
    row = pl.ds(lax.axis_index("tm"), 1)
    lines = [diff_ref[row, :], vel_ref[0, row, :], vel_ref[1, row, :]]
    sub = lax.broadcasted_iota(jnp.int32, (SUB, LANE), 0)
    blocks = [
        [jnp.broadcast_to(line[:, h * LANE : (h + 1) * LANE], (SUB, LANE)) for h in range(parts)]
        for line in lines
    ]
    for parity in range(2):
        base = parity * own - halo
        for part in range(parts):
            total = jnp.zeros((SUB, LANE), jnp.float32)
            for f in range(len(lines)):
                amount = (f + 1) * window - base

                def slanted(h):
                    flat = spin(blocks[f][h % parts], amount)
                    return pltpu.roll(flat, 0, 1, stride=window, stride_axis=0)

                value = slanted(part)
                if parity == 0:
                    value = jnp.where((sub == SUB - 1) & (spot < halo), slanted(part - 1), value)
                else:
                    value = jnp.where((sub == 0) & (spot >= edge), slanted(part + 1), value)
                total = jnp.where(group == f, value, total)
            for m in range(SUB):
                target = plan.holder[2 * (part * SUB + m) + parity]
                at = target * plan.inward + plan.inward - 1
                out_ref[at : at + 1, :] = total[SUB - 1 - m : SUB - m]


def totals_of(ref):
    return jnp.sum(ref[...], axis=0, keepdims=True) * (1.0 / (damping * damping))


def pick(totals, k):
    lane = lane_of(totals.shape)
    value = jnp.sum(jnp.where(lane == k, totals, 0.0), axis=1, keepdims=True)
    return jnp.broadcast_to(value, (1, LANE))


def middle(totals):
    aa, ab, bb, ac, bc = (pick(totals, k) for k in range(5))
    scale = 1.0 / (aa + epsilon)
    drop = scale * ab
    norm = jnp.maximum(bb - drop * (2.0 * ab - drop * aa), 1e-5 * bb)
    over = ac - drop * ab
    along = bc - drop * (bb + ac - drop * ab)
    return aa, drop, scale * over, scale * along / (scale * norm + epsilon)


def iterate(middle_totals, totals):
    aa, drop, over, along = middle(middle_totals)
    pairs = [(0, 1), (1, 1), (0, 2), (1, 2), (2, 2), (0, 3), (1, 3), (2, 3), (3, 3)]
    gram = {(0, 0): aa}
    for k, (i, j) in enumerate(pairs):
        gram[i, j] = gram[j, i] = pick(totals, k)
    zero = jnp.zeros_like(aa)
    one = jnp.ones_like(aa)
    images = [[drop, one, zero, zero], [over, along, one, zero], [zero, zero, zero, one]]
    size = KRYLOV + 1

    def product(left, right):
        return sum(left[i] * right[j] * gram[i, j] for i in range(size) for j in range(size))

    beta = jnp.sqrt(aa + epsilon)
    basis = [[1.0 / beta, zero, zero, zero]]
    hessen = [[zero] * KRYLOV for row in range(size)]
    for j in range(KRYLOV):
        image = [sum(basis[j][k] * images[k][i] for k in range(KRYLOV)) for i in range(size)]
        found = [product(basis[i], image) for i in range(j + 1)]
        for i in range(j + 1):
            hessen[i][j] = found[i]
            image = [w - found[i] * v for w, v in zip(image, basis[i])]
        length = jnp.sqrt(jnp.maximum(product(image, image), 0.0) + epsilon)
        hessen[j + 1][j] = length
        basis.append([w / length for w in image])
    ortho = []
    upper = [[None] * KRYLOV for row in range(KRYLOV)]
    for column in range(KRYLOV):
        current = [hessen[row][column] for row in range(size)]
        for row in range(column):
            factor = sum(x * y for x, y in zip(ortho[row], current))
            upper[row][column] = factor
            current = [y - factor * x for x, y in zip(ortho[row], current)]
        length = jnp.sqrt(sum(y * y for y in current))
        upper[column][column] = length
        ortho.append([y / length for y in current])
    values = [None] * KRYLOV
    for row in reversed(range(KRYLOV)):
        accum = ortho[row][0] * beta
        for later in range(row + 1, KRYLOV):
            accum = accum - upper[row][later] * values[later]
        values[row] = accum / upper[row][row]
    weights = [sum(values[j] * basis[j][k] for j in range(KRYLOV)) for k in range(KRYLOV)]
    weights[0] = weights[0] - drop * weights[1]
    return weights


def coefficients(plan, recv_ref, strip, table_ref):
    window = plan.window
    lane = lane_of((SUB, LANE))
    stride = plan.space * plan.inward
    lines = [
        recv_ref[pl.ds(s * plan.inward + plan.inward - 1, SUB, stride), :]
        for s in range(plan.space)
    ]
    fields = []
    for f in range(3):
        parts = []
        for line in lines:
            part = None
            for g in range(plan.tm):
                moved = spin(line, (g - f) * window)
                part = moved if g == 0 else jnp.where(lane // window == g, moved, part)
            parts.append(part)
        fields.append(jnp.concatenate(parts, axis=0))
    diff, vel_col, vel_row = fields
    shape = (plan.rows, LANE)
    row = lax.broadcasted_iota(jnp.int32, shape, 0)
    col = strip * plan.own - plan.halo + lane_of(shape) % window
    center = 1.0 + 4.0 * diff
    table_ref[0] = damping * center
    table_ref[1] = 1.0 / center
    table_ref[2] = jnp.where(row > 0, damping * (diff + vel_row), 0.0)
    table_ref[3] = jnp.where(row < plan.rows - 1, damping * (diff - vel_row), 0.0)
    table_ref[4] = jnp.where(col > 0, damping * (diff + vel_col), 0.0)
    table_ref[5] = jnp.where(col < plan.cols - 1, damping * (diff - vel_col), 0.0)


def krylov_kernel(plan, j, *refs):
    refs = list(refs)
    strip = plan.strip_of(lax.axis_index("tm"), lax.axis_index("space"))
    here, window, rows, halo, own = plan.here, plan.window, plan.rows, plan.halo, plan.own
    slot = plan.slot
    final = j == KRYLOV - 1
    shape = (rows, LANE)
    lane = lane_of(shape)
    low_lane = lane_of((SUB, LANE))
    low_spot = low_lane & (window - 1)
    even = strip % 2 == 0
    if j == 0:
        recv_ref, table_ref, q_ref, g_ref, w_ref, near_ref, far_ref, y_ref, tail_ref = refs
        coefficients(plan, recv_ref, strip, table_ref)
    elif not final:
        table_ref, image_ref, near_in, far_in, first_ref = refs[:5]
        q_ref, g_ref, w_ref, near_ref, far_ref, sum_ref, y_ref = refs[5:]
    else:
        table_ref, image_ref, near_in, far_in, first_ref, second_ref, mid_ref = refs[:7]
        g_ref, sum_ref, y_ref, q_ref, w_ref, rest_ref = refs[7:]
        _, drop, over, along = middle(totals_of(mid_ref))
    center = table_ref[0]
    inverse = table_ref[1]
    north, south, west, east = (table_ref[2 + k] for k in range(4))
    zero = jnp.zeros(shape, jnp.float32)
    low_zero = jnp.zeros((SUB, LANE), jnp.float32)
    inner = slice(SUB, SUB + rows)

    def around(n, field):
        return (
            north * g_ref[n, SUB - 1 : SUB - 1 + rows, :]
            + south * g_ref[n, SUB + 1 : SUB + 1 + rows, :]
            + west * spin(field, 1)
            + east * spin(field, -1)
        )

    power = inverse
    for _ in range(int(math.log2(here))):
        power = power * power
    whole = power
    for _ in range(int(math.log2(plan.tm))):
        whole = whole * whole
    closing = 1.0 / (1.0 - alpha_corner * whole)

    def entering(ends):
        total = alpha_corner * ends
        for k in reversed(range(1, plan.tm)):
            back = spin(ends, k * window)
            total = total * power + jnp.where(lane < k * window, alpha_corner * back, back)
        return total * closing

    def settle(base, y):
        for k in range(UNROLL):
            y = (y_ref[base + k] + y) * inverse
            y_ref[base + k] = y
        return y

    for k in range(UNROLL):
        y_ref[k] = zero

    def blank(n):
        g_ref[n] = jnp.zeros((rows + 2 * SUB, LANE), jnp.float32)

    if j == 0:
        last_tile = plan.tiles - 1

        def tails(k, carry):
            for p in (4 * k, 4 * k + 1, 4 * k + 2, 4 * k + 3):
                for s in range(plan.space):
                    source = p * plan.space + s
                    total = low_zero
                    for a in range(last_tile):
                        tile = recv_ref[pl.ds(source * plan.inward + a * SUB, SUB), :]
                        moved = spin(tile, plan.spare * a - plan.used)
                        total = jnp.where(low_spot // plan.spare == a, moved, total)
                    tail_ref[source] = total
            return carry

        lax.fori_loop(0, plan.tm // 4, tails, 0)

        def first(k, y):
            parts = [[] for _ in range(PAIR)]
            for t in range(PAIR):
                a = k * PAIR + t
                whole = a < last_tile
                at = jnp.minimum(a, last_tile - 1) * SUB
                for s in range(plan.space):
                    cut = []
                    for p in range(plan.tm):
                        source = p * plan.space + s
                        tile = recv_ref[pl.ds(source * plan.inward + at, SUB), :]
                        cut.append(damping * jnp.where(whole, tile, tail_ref[source]))
                    parts[t].append(exchange_blocks(cut, window, 2))
            for t in range(PAIR):
                for i in range(SUB):
                    n = (k * PAIR + t) * SUB + i
                    q = jnp.concatenate([part[i] for part in parts[t]], axis=0)
                    q_ref[n] = q
                    y = (q + y) * inverse
                    y_ref[UNROLL + n] = y
                    blank(n)
            return y

        y = lax.fori_loop(0, plan.tiles // PAIR, first, zero)
    else:
        right_mask = (low_spot >= halo + own) & (low_spot < halo + own + halo)
        left_mask = low_spot < halo

        def first(i, y):
            base = i * UNROLL
            y = settle(base, y)
            for k in range(UNROLL):
                n = base + k
                near, far = near_in[n], far_in[n]
                right = jnp.where(even, near, far)
                left = jnp.where(even, far, near)
                image = image_ref[n]
                parts = []
                for s in range(plan.space):
                    part = image[s * SUB : (s + 1) * SUB]
                    part = jnp.where(right_mask, spin(right, halo + own - slot * s), part)
                    part = jnp.where(left_mask, spin(left, halo - own - slot * s), part)
                    parts.append(part)
                q = jnp.concatenate(parts, axis=0)
                if final:
                    start, later = first_ref[n], second_ref[n]
                    rest = later - drop * start
                    rest_ref[n] = rest
                    q = (q - drop * later) - over * start - along * rest
                q_ref[n] = q
                y_ref[UNROLL + n] = q
                blank(n)
            return y

        y = settle(here, lax.fori_loop(0, here // UNROLL, first, zero))

    def sweep(_, ends):
        def body(i, carry):
            y, z = carry
            base = i * UNROLL
            olds = [y_ref[UNROLL + base + k] for k in range(UNROLL)]
            y = settle(base, y)
            for k in range(UNROLL):
                n = base + k
                z = z * inverse
                guess = (1.0 - damping) * g_ref[n, inner, :] + (olds[k] + z)
                g_ref[n, inner, :] = guess
                y_ref[UNROLL + n] = q_ref[n] + around(n, guess)
            return (y, z)

        y, _ = lax.fori_loop(0, here // UNROLL, body, (zero, entering(ends)))
        return settle(here, y)

    y = lax.fori_loop(0, SWEEPS - 1, sweep, y)
    start = entering(y)
    ending = (1.0 - damping) * g_ref[here - 1, inner, :] + (y + start * power)
    before = jnp.where(lane < window, 0.0, damping * spin(ending, window))

    ahead = [
        ((low_lane - slot * s - (own - halo)) & (window - 1)) < halo for s in range(plan.space)
    ]

    def fold(block):
        return sum(block[s * SUB : (s + 1) * SUB] for s in range(plan.space))

    size = KRYLOV + 1

    def gather(base, accs):
        for k in range(UNROLL):
            n = base + k
            image = w_ref[n]
            if not final:
                left = right = None
                for s in range(plan.space):
                    moved = spin(image[s * SUB : (s + 1) * SUB], slot * s - halo)
                    left = moved if s == 0 else jnp.where(low_spot // slot == s, moved, left)
                    right = moved if s == 0 else jnp.where(ahead[s], moved, right)
                near_ref[n] = jnp.where(even, right, left)
                far_ref[n] = jnp.where(even, left, right)
            if j == 0:
                continue
            q = q_ref[n]
            start = first_ref[n]
            if not final:
                pairs = [(start, start), (start, q), (q, q), (start, image), (q, image)]
            else:
                rest = rest_ref[n]
                held = [start, rest, q, image]
                pairs = [(held[i], held[k]) for k in range(1, size) for i in range(k + 1)]
            accs = [acc + fold(x * y) for acc, (x, y) in zip(accs, pairs)]
        return accs

    def last(i, carry):
        z, before, accs = carry
        accs = gather(jnp.maximum(i - 1, 0) * UNROLL, accs)
        accs = tuple(jnp.where(i > 0, acc, 0.0) for acc in accs)
        for k in range(UNROLL):
            n = i * UNROLL + k
            z = z * inverse
            guess = (1.0 - damping) * g_ref[n, inner, :] + (y_ref[UNROLL + n] + z)
            g_ref[n, inner, :] = guess
            w_ref[n] = center * guess - around(n, guess) - before
            before = damping * guess
        return (z, before, accs)

    fields = (0, 5, 9)[j]
    _, _, accs = lax.fori_loop(0, here // UNROLL, last, (start, before, (low_zero,) * fields))
    accs = gather(here - UNROLL, list(accs))
    if j == 0:
        return
    owned = (low_spot >= halo) & (low_spot < halo + own)
    record = jnp.zeros((1, LANE), jnp.float32)
    record_lane = lane_of((1, LANE))
    for place, acc in enumerate(accs):
        value = jnp.sum(jnp.where(owned, acc, 0.0), axis=0, keepdims=True)
        value = jnp.sum(value, axis=1, keepdims=True)
        record = jnp.where(record_lane == place, value, record)
    sum_ref[...] = jnp.broadcast_to(record, sum_ref.shape)


def combine_kernel(plan, *refs):
    z_refs = refs[:KRYLOV]
    mid_ref, end_ref, out_ref = refs[KRYLOV:]
    along = iterate(totals_of(mid_ref), totals_of(end_ref))
    own, halo, window, groups = plan.own, plan.halo, plan.window, plan.groups
    lane = lane_of((SUB, LANE))
    front = lane % window < own
    size = plan.outward

    def start_of(p, s):
        return (p * plan.space + s) * size

    def value(n, s):
        here = slice((s + 1) * SUB, (s + 2) * SUB)
        return sum(c * ref[n, here, :] for c, ref in zip(along, z_refs))

    def body(k, carry):
        for t in range(PAIR):
            aa = k * PAIR + t
            for s in range(plan.space):
                pieces = []
                for i in range(SUB):
                    n = aa * 2 * SUB + 2 * i
                    left, right = spin(value(n, s), -halo), spin(value(n + 1, s), own - halo)
                    pieces.append(jnp.where(front, left, right))
                for p, piece in enumerate(exchange_blocks(pieces, window, 2)):
                    out_ref[pl.ds(start_of(p, s) + aa * SUB, SUB), :] = piece
                    if s + 1 < plan.space:
                        at = start_of(p, s + 1) + groups * SUB + aa
                        out_ref[pl.ds(at, 1), :] = piece[SUB - 1 :]
                    if s > 0:
                        at = start_of(p, s - 1) + groups * SUB + groups + aa
                        out_ref[pl.ds(at, 1), :] = piece[:1]
        return carry

    lax.fori_loop(0, groups // PAIR, body, 0)
    nothing = jnp.zeros((groups, LANE), jnp.float32)
    sub = lax.broadcasted_iota(jnp.int32, (SUB, LANE), 0)
    for p in range(plan.tm):
        at = start_of(p, 0) + groups * SUB
        out_ref[at : at + groups, :] = nothing
        at = start_of(p, plan.space - 1) + groups * SUB + groups
        out_ref[at : at + groups, :] = nothing
    for s in range(plan.space):
        ending = value(plan.here - 1, s)
        for p in range(plan.tm):
            line = nothing[:1]
            if p > 0:
                turned = spin(ending, -(p - 1) * window - halo)
                turned = pltpu.roll(turned, 0, 1, stride=own, stride_axis=0)
                line = jnp.sum(jnp.where(lane // own == sub, turned, 0.0), axis=0, keepdims=True)
            at = start_of(p, s) + size - 1
            out_ref[at : at + 1, :] = line


def finish_kernel(plan, recv_ref, right_ref, diff_ref, vel_ref, *refs):
    results, (rim_ref, out_ref, rest_ref, sems) = refs[:2], refs[2:]
    groups, own, size = plan.groups, plan.own, plan.outward
    count = LANE // own
    parts = plan.cols // LANE
    shape = (SUB, plan.cols)
    lane = lane_of((SUB, LANE))
    diff, vel_col, vel_row = diff_ref[...], vel_ref[0], vel_ref[1]
    col = lane_of(shape)
    sub = lax.broadcasted_iota(jnp.int32, shape, 0)
    center = 1.0 + 4.0 * diff
    north = diff + vel_row
    south = diff - vel_row
    west = jnp.where(col > 0, diff + vel_col, 0.0)
    east = jnp.where(col < plan.cols - 1, diff - vel_col, 0.0)

    def start_of(part, m):
        return plan.holder[part * count + m] * size

    def spread(offset):
        wide = []
        for part in range(parts):
            pieces = [
                recv_ref[pl.ds(start_of(part, m) + offset, SUB), :] for m in range(count)
            ]
            wide.append(exchange_blocks(pieces, own, 2))
        return [jnp.concatenate(pair, axis=1) for pair in zip(*wide)]

    for i, field in enumerate(spread(groups * SUB)):
        rim_ref[i] = field
    halves = []
    row = lax.broadcasted_iota(jnp.int32, (SUB, LANE), 0)
    for part in range(parts):
        tiles = []
        for first in range(0, count, SUB):
            tile = jnp.zeros((SUB, LANE), jnp.float32)
            for q in range(SUB):
                at = start_of(part, first + q) + size - 1
                line = jnp.broadcast_to(recv_ref[at : at + 1, :], (SUB, LANE))
                tile = jnp.where(row == q, line, tile)
            tile = spin(tile, first * own)
            tiles.append((first, pltpu.roll(tile, 0, 1, stride=own, stride_axis=0)))
        total = jnp.zeros((SUB, LANE), jnp.float32)
        for r in range(SUB):
            line = sum(
                jnp.where(lane // own == row + first, spin(tile, -r * own), 0.0)
                for first, tile in tiles
            )
            line = jnp.sum(line, axis=0, keepdims=True)
            total = jnp.where(row == r, jnp.broadcast_to(line, (SUB, LANE)), total)
        halves.append(total)
    before = jnp.concatenate(halves, axis=1)

    size_of = PAIR * count

    def copies(k):
        at = pl.ds(k * size_of, size_of)
        return [
            pltpu.make_async_copy(ref.at[at], result.at[at], sems.at[k, f])
            for f, (ref, result) in enumerate(zip((out_ref, rest_ref), results))
        ]

    def body(k, before):
        for t in range(PAIR):
            aa = k * PAIR + t
            for i, field in enumerate(spread(aa * SUB)):
                n = aa * count + i
                above = rim_ref[i, pl.ds(aa, 1), :]
                below = rim_ref[i, pl.ds(groups + aa, 1), :]
                out_ref[n] = field
                around = (
                    north * jnp.where(sub == 0, above, spin(field, 1, 0))
                    + south * jnp.where(sub == SUB - 1, below, spin(field, -1, 0))
                    + west * spin(field, 1)
                    + east * spin(field, -1)
                )
                rest_ref[n] = right_ref[n] - (center * field - around - before)
                before = field
        for copy in copies(k):
            copy.start()
        return before

    lax.fori_loop(0, groups // PAIR, body, before)
    for k in range(groups // PAIR):
        for copy in copies(k):
            copy.wait()


def call(kernel, shapes, operands, scratch=(), sems=None, far_in=False, far_out=False, room=16):
    vmem = pl.BlockSpec(memory_space=pltpu.VMEM)
    hbm = pl.BlockSpec(memory_space=pltpu.HBM)
    held = [pltpu.VMEM(shape, jnp.float32) for shape in scratch]
    if sems:
        held.append(pltpu.SemaphoreType.DMA(sems))
    return pl.pallas_call(
        kernel,
        out_shape=[jax.ShapeDtypeStruct(shape, jnp.float32) for shape in shapes],
        in_specs=[hbm if far_in else vmem] * len(operands),
        out_specs=[hbm if far_out else vmem] * len(shapes),
        scratch_shapes=held,
        compiler_params=pltpu.CompilerParams(vmem_limit_bytes=room * 1024 * 1024),
    )(*operands)


def everyone(block, devices):
    lines = block.shape[0] // devices
    parts = block.reshape(devices, lines, 1, LANE)
    return lax.all_to_all(parts, AXES, split_axis=0, concat_axis=0, tiled=True).reshape(block.shape)


def strip_device(plan, right_side, diffusion, velocity):
    count = plan.devices
    hold = plan.holder
    near_route = []
    far_route = []
    for k in range(0, count, 2):
        near_route += [(hold[k], hold[k + 1]), (hold[k + 1], hold[k])]
    for k in range(1, count - 1, 2):
        far_route += [(hold[k], hold[k + 1]), (hold[k + 1], hold[k])]
    bind = lambda kernel, *more: (lambda *refs: kernel(plan, *more, *refs))
    full = (plan.here, plan.rows, LANE)
    padded = (plan.here, plan.rows + 2 * SUB, LANE)
    delayed = (plan.here + UNROLL, plan.rows, LANE)
    side = (plan.here, SUB, LANE)
    small = (count, LANE)
    given = [right_side, diffusion, velocity]
    sent = call(
        bind(pack_kernel),
        [(count * plan.inward, LANE)],
        given,
        scratch=[(count, SUB, LANE), *(block.shape for block in given)],
        sems=(4,),
        far_in=True,
        room=63,
    )[0]
    table, q0, z0, image, near, far = call(
        bind(krylov_kernel, 0),
        [(6, plan.rows, LANE), full, padded, full, side, side],
        [everyone(sent, count)],
        scratch=[delayed, (count, SUB, LANE)],
    )
    near = lax.ppermute(near, AXES, near_route)
    far = lax.ppermute(far, AXES, far_route)
    q1, z1, image, near, far, sums = call(
        bind(krylov_kernel, 1),
        [full, padded, full, side, side, small],
        [table, image, near, far, q0],
        scratch=[delayed],
    )
    near = lax.ppermute(near, AXES, near_route)
    far = lax.ppermute(far, AXES, far_route)
    mid = everyone(sums, count)
    z2, sums = call(
        bind(krylov_kernel, 2),
        [padded, small],
        [table, image, near, far, q0, q1, mid],
        scratch=[delayed, full, full, full],
    )
    end = everyone(sums, count)
    packed = call(bind(combine_kernel), [(count * plan.outward, LANE)], [z0, z1, z2, mid, end])[0]
    shape = right_side.shape
    return tuple(
        call(
            bind(finish_kernel),
            [shape, shape],
            [everyone(packed, count), *given],
            scratch=[(2 * SUB, SUB, plan.cols), shape, shape],
            sems=(plan.groups // PAIR, 2),
            far_out=True,
        )
    )


def per_device(mesh):
    def run(right_side, diffusion, velocity):
        rows = right_side.shape[1] * mesh.shape["space"]
        steps = right_side.shape[0] * mesh.shape["tm"]
        plan = Plan(mesh, steps, rows, right_side.shape[2])
        if plan.fits():
            return strip_device(plan, right_side, diffusion, velocity)
        return generic_device(right_side, diffusion, velocity)

    return run


def solution(mesh):
    placed = (P("tm", "space", None), P("space", None), P(None, "space", None))
    return jax.shard_map(
        per_device(mesh),
        mesh=mesh,
        in_specs=placed,
        out_specs=(P("tm", "space", None), P("tm", "space", None)),
        check_vma=False,
    )
```

```python
import math

import jax
import jax.numpy as jnp
from jax import lax
from jax.experimental import pallas as pl
from jax.experimental.pallas import tpu as pltpu
from jax.sharding import PartitionSpec as P

L = 512
KRYLOV = 3
SWEEPS = 3


alpha_corner = 0.05
damping = 0.8
epsilon = 1e-06
highest = lax.Precision.HIGHEST


def extended(block, sides, width):
    for axis, dim in sides:
        count = lax.axis_size(axis)
        forward = [(i, i + 1) for i in range(count - 1)]
        backward = [(target, source) for source, target in forward]
        low = lax.ppermute(
            lax.slice_in_dim(block, block.shape[dim] - width, None, axis=dim), axis, forward
        )
        high = lax.ppermute(lax.slice_in_dim(block, 0, width, axis=dim), axis, backward)
        block = jnp.concatenate([low, block, high], axis=dim)
    return block


def from_behind(block, axis, distance):
    devices = range(lax.axis_size(axis))
    route = [(i - distance, i) for i in devices if i - distance in devices]
    return lax.ppermute(block, axis, route)


def shifted(padded, row_dim, col_dim, rows, cols, row_start, col_start):
    piece = lax.slice_in_dim(padded, row_start, row_start + rows, axis=row_dim)
    return lax.slice_in_dim(piece, col_start, col_start + cols, axis=col_dim)


def stencil(field, padded, row_dim, col_dim, diffusion, velocity_col, velocity_row):
    rows = field.shape[row_dim]
    cols = field.shape[col_dim]
    north = shifted(padded, row_dim, col_dim, rows, cols, 0, 1)
    south = shifted(padded, row_dim, col_dim, rows, cols, 2, 1)
    west = shifted(padded, row_dim, col_dim, rows, cols, 1, 0)
    east = shifted(padded, row_dim, col_dim, rows, cols, 1, 2)
    return (
        (1.0 + 4.0 * diffusion) * field
        - diffusion * (north + south + west + east)
        + velocity_col * (east - west)
        + velocity_row * (south - north)
    )


def divided(real_part, imag_part, diag_real, diag_imag, modulus):
    return (
        damping * (real_part * diag_real + imag_part * diag_imag) / modulus,
        damping * (imag_part * diag_real - real_part * diag_imag) / modulus,
    )


def remainder(
    source_real, source_imag, image_real, image_imag, guess_real, guess_imag, shift_real, shift_imag
):
    return (
        source_real - (image_real - (shift_real * guess_real + shift_imag * guess_imag)),
        source_imag - (image_imag - (shift_real * guess_imag - shift_imag * guess_real)),
    )


def dft_tables(length):
    index = jnp.arange(length, dtype=jnp.int32)
    product = index[:, None] * index[None, :] % length
    angle = product.astype(jnp.float32) * (2.0 * math.pi / length)
    return (jnp.cos(angle), jnp.sin(angle))


def least_squares(hessen, beta):
    ortho = []
    upper = [[None] * KRYLOV for row in range(KRYLOV)]
    for column in range(KRYLOV):
        current = hessen[:, column]
        for row in range(column):
            factor = jnp.sum(ortho[row] * current)
            upper[row][column] = factor
            current = current - factor * ortho[row]
        length = jnp.sqrt(jnp.sum(current * current))
        upper[column][column] = length
        ortho.append(current / length)
    target = [ortho[row][0] * beta for row in range(KRYLOV)]
    values = [None] * KRYLOV
    for row in reversed(range(KRYLOV)):
        accum = target[row]
        for later in range(row + 1, KRYLOV):
            accum = accum - upper[row][later] * values[later]
        values[row] = accum / upper[row][row]
    return jnp.stack(values)


def generic_device(right_side, diffusion, velocity):
    steps_here = right_side.shape[0]
    devices_tm = lax.axis_size("tm")
    position = lax.axis_index("tm")
    log_decay = math.log(alpha_corner) / L
    decay = math.exp(log_decay)
    local_steps = position * steps_here + jnp.arange(steps_here, dtype=jnp.int32)
    times = local_steps.astype(jnp.float32)
    weights = jnp.exp(times * log_decay)[:, None, None]
    unweights = jnp.exp(-times * log_decay)[:, None, None]
    cosine, sine = dft_tables(L)
    velocity_col = velocity[0]
    velocity_row = velocity[1]
    width = right_side.shape[2] // devices_tm
    start = position * width
    diff_strip = lax.dynamic_slice_in_dim(diffusion, start, width, 1)[:, :, None]
    col_strip = lax.dynamic_slice_in_dim(velocity_col, start, width, 1)[:, :, None]
    row_strip = lax.dynamic_slice_in_dim(velocity_row, start, width, 1)[:, :, None]
    angles = jnp.arange(L, dtype=jnp.int32).astype(jnp.float32) * (2.0 * math.pi / L)
    shift_real = decay * jnp.cos(angles)
    shift_imag = decay * jnp.sin(angles)
    diag_real = 1.0 + 4.0 * diff_strip - shift_real
    modulus = diag_real * diag_real + shift_imag * shift_imag

    def forward(block):
        real_part = jnp.dot(block, cosine, precision=highest)
        imag_part = -jnp.dot(block, sine, precision=highest)
        return jnp.concatenate([real_part, imag_part], axis=2)

    total = lax.psum(jnp.sum(right_side * right_side), ("tm", "space"))
    beta = jnp.sqrt(total + epsilon)
    basis = [right_side / beta]
    prepared = []
    hessen = jnp.zeros((KRYLOV + 1, KRYLOV), jnp.float32)
    for column in range(KRYLOV):
        moved = jnp.transpose(basis[column] * weights, (1, 2, 0))
        spectrum = forward(lax.all_to_all(moved, "tm", split_axis=1, concat_axis=2, tiled=True))
        source_real = spectrum[:, :, :L]
        source_imag = spectrum[:, :, L:]
        guess_real, guess_imag = divided(source_real, source_imag, diag_real, shift_imag, modulus)
        for sweep in range(SWEEPS - 1):
            joined = jnp.concatenate([guess_real, guess_imag], axis=2)
            padded = extended(joined, (("tm", 1), ("space", 0)), 1)
            image = stencil(joined, padded, 0, 1, diff_strip, col_strip, row_strip)
            left_real, left_imag = remainder(
                source_real,
                source_imag,
                image[:, :, :L],
                image[:, :, L:],
                guess_real,
                guess_imag,
                shift_real,
                shift_imag,
            )
            step_real, step_imag = divided(left_real, left_imag, diag_real, shift_imag, modulus)
            guess_real = guess_real + step_real
            guess_imag = guess_imag + step_imag
        back = (
            jnp.dot(guess_real, cosine, precision=highest)
            - jnp.dot(guess_imag, sine, precision=highest)
        ) / L
        back = lax.all_to_all(back, "tm", split_axis=2, concat_axis=1, tiled=True)
        direction = jnp.transpose(back, (2, 0, 1)) * unweights
        prepared.append(direction)
        apply_padded = extended(direction, (("space", 1),), 1)
        apply_padded = jnp.pad(apply_padded, ((0, 0), (0, 0), (1, 1)))
        apply_image = stencil(direction, apply_padded, 1, 2, diffusion, velocity_col, velocity_row)
        earlier = from_behind(direction[-1:], "tm", 1)
        image = apply_image - jnp.concatenate([earlier, direction[:-1]], axis=0)
        local = jnp.stack([jnp.sum(vector * image) for vector in basis])
        projections = lax.psum(local, ("tm", "space"))
        for row in range(column + 1):
            image = image - projections[row] * basis[row]
        squares = lax.psum(jnp.sum(image * image), ("tm", "space"))
        length = jnp.sqrt(squares + epsilon)
        hessen = hessen.at[: column + 1, column].set(projections)
        hessen = hessen.at[column + 1, column].set(length)
        basis.append(image / length)
    coeffs = least_squares(hessen, beta)
    solution = prepared[0] * coeffs[0]
    for column in range(1, KRYLOV):
        solution = solution + prepared[column] * coeffs[column]
    first = (jnp.arange(KRYLOV + 1) == 0).astype(jnp.float32)
    target = beta * first - jnp.sum(hessen * coeffs[None, :], axis=1)
    residual = basis[0] * target[0]
    for row in range(1, KRYLOV + 1):
        residual = residual + basis[row] * target[row]
    return (solution, residual)


SUB = 8
LANE = 128
AXES = ("tm", "space")
UNROLL = 32
PAIR = 2
TAIL = 16


def spin(block, amount, axis=1):
    return pltpu.roll(block, amount % block.shape[axis], axis)


def lane_of(shape):
    return lax.broadcasted_iota(jnp.int32, shape, 1)


def exchange_blocks(pieces, width, radix):
    pieces = list(pieces)
    lane = lane_of(pieces[0].shape)
    step = 1
    while step < len(pieces):
        digit = lane // (width * step) % radix
        result = list(pieces)
        for i in range(len(pieces)):
            e = i // step % radix
            total = None
            for d in range(radix):
                moved = pieces[i + (d - e) * step]
                if d != e:
                    moved = spin(moved, (d - e) * step * width)
                total = moved if total is None else jnp.where(digit == d, moved, total)
            result[i] = total
        pieces = result
        step *= radix
    return pieces


class Plan:
    def __init__(self, mesh, steps, rows, cols):
        self.tm = mesh.shape["tm"]
        self.space = mesh.shape["space"]
        self.devices = self.tm * self.space
        self.steps = steps
        self.rows = rows
        self.cols = cols
        self.here = steps // self.tm
        self.window = LANE // self.tm
        self.own = cols // self.devices
        self.halo = SWEEPS
        self.slot = self.window // self.space
        self.used = self.own + 2 * self.halo
        self.spare = self.window - self.used
        self.tiles = self.here // SUB
        self.inward = (self.tiles - 1) * SUB + 1
        self.groups = self.here // (2 * SUB)
        self.outward = self.groups * SUB + 2 * self.groups + 1
        self.ring = [self.strip_of(d // self.space, d % self.space) for d in range(self.devices)]
        self.holder = [self.ring.index(j) for j in range(self.devices)]

    def fits(self):
        return (
            LANE % self.tm == 0
            and self.tm == SUB
            and self.rows == SUB * self.space
            and self.cols % self.devices == 0
            and self.cols == 2 * LANE
            and self.steps % (self.tm * 2 * SUB) == 0
            and self.window == 2 * self.own
            and self.spare * (self.tiles - 1) == self.used
            and self.here % UNROLL == 0
            and self.here % TAIL == 0
            and self.groups * 2 == SUB
            and self.slot >= self.halo
            and self.space % 2 == 0
            and KRYLOV == 3
            and self.tiles % PAIR == 0
            and self.groups % PAIR == 0
            and self.tm % 4 == 0
        )

    def strip_of(self, t, s):
        turn = t ^ ((t >> 1) & 1)
        half = self.space // 2
        x, core = s // 2, s % 2
        odd = turn % 2
        return (turn * half + x + odd * (half - 1 - 2 * x)) * 2 + core


def pack_kernel(plan, right_in, diff_in, vel_in, out_ref, *scratch):
    tail_ref, right_ref, diff_ref, vel_ref, sems = scratch
    split = plan.here - SUB
    copies = [
        pltpu.make_async_copy(right_in.at[split:], right_ref.at[split:], sems.at[0]),
        pltpu.make_async_copy(right_in.at[:split], right_ref.at[:split], sems.at[1]),
        pltpu.make_async_copy(diff_in, diff_ref, sems.at[2]),
        pltpu.make_async_copy(vel_in, vel_ref, sems.at[3]),
    ]
    for copy in copies:
        copy.start()
    copies[0].wait()
    window, own, halo = plan.window, plan.own, plan.halo
    parts = plan.cols // LANE
    lane = lane_of((SUB, LANE))
    group, spot = lane // window, lane % window
    edge = LANE - (SUB - 1) * window - own + halo

    def strips():
        for parity in range(2):
            for part in range(parts):
                for m in range(SUB):
                    yield parity, part, m, plan.holder[2 * (part * SUB + m) + parity]

    def windows(a):
        pieces = []
        fields = [right_ref[a * SUB + i] for i in range(SUB)]
        for parity in range(2):
            turned = [spin(field, halo - parity * own) for field in fields]
            for part in range(parts):
                cut = [field[:, part * LANE : (part + 1) * LANE] for field in turned]
                pieces += exchange_blocks(cut, window, 2)
        return pieces

    def spread(a, pieces):
        amount = plan.used - plan.spare * a
        for index, (_, _, _, target) in enumerate(strips()):
            tail = pltpu.roll(tail_ref[index], amount, 1)
            piece = jnp.where(spot >= plan.used, tail, pieces[index])
            out_ref[pl.ds(target * plan.inward + a * SUB, SUB), :] = piece

    for index, piece in enumerate(windows(plan.tiles - 1)):
        tail_ref[index] = piece
    copies[1].wait()

    def body(k, carry):
        both = [(a, windows(a)) for a in (2 * k, 2 * k + 1)]
        for a, pieces in both:
            spread(a, pieces)
        return carry

    lax.fori_loop(0, (plan.tiles - 1) // 2, body, 0)
    for a in range((plan.tiles - 1) // 2 * 2, plan.tiles - 1):
        spread(a, windows(a))
    copies[2].wait()
    copies[3].wait()
    row = pl.ds(lax.axis_index("tm"), 1)
    lines = [diff_ref[row, :], vel_ref[0, row, :], vel_ref[1, row, :]]
    sub = lax.broadcasted_iota(jnp.int32, (SUB, LANE), 0)
    blocks = [
        [jnp.broadcast_to(line[:, h * LANE : (h + 1) * LANE], (SUB, LANE)) for h in range(parts)]
        for line in lines
    ]
    for parity in range(2):
        base = parity * own - halo
        for part in range(parts):
            total = jnp.zeros((SUB, LANE), jnp.float32)
            for f in range(len(lines)):
                amount = (f + 1) * window - base

                def slanted(h):
                    flat = spin(blocks[f][h % parts], amount)
                    return pltpu.roll(flat, 0, 1, stride=window, stride_axis=0)

                value = slanted(part)
                if parity == 0:
                    value = jnp.where((sub == SUB - 1) & (spot < halo), slanted(part - 1), value)
                else:
                    value = jnp.where((sub == 0) & (spot >= edge), slanted(part + 1), value)
                total = jnp.where(group == f, value, total)
            for m in range(SUB):
                target = plan.holder[2 * (part * SUB + m) + parity]
                at = target * plan.inward + plan.inward - 1
                out_ref[at : at + 1, :] = total[SUB - 1 - m : SUB - m]


def totals_of(ref):
    return jnp.sum(ref[...], axis=0, keepdims=True) * (1.0 / (damping * damping))


def pick(totals, k):
    lane = lane_of(totals.shape)
    value = jnp.sum(jnp.where(lane == k, totals, 0.0), axis=1, keepdims=True)
    return jnp.broadcast_to(value, (1, LANE))


def middle(totals):
    aa, ab, bb, ac, bc = (pick(totals, k) for k in range(5))
    scale = 1.0 / (aa + epsilon)
    drop = scale * ab
    norm = jnp.maximum(bb - drop * (2.0 * ab - drop * aa), 1e-5 * bb)
    over = ac - drop * ab
    along = bc - drop * (bb + ac - drop * ab)
    return aa, drop, scale * over, scale * along / (scale * norm + epsilon)


def iterate(middle_totals, totals):
    aa, drop, over, along = middle(middle_totals)
    pairs = [(0, 1), (1, 1), (0, 2), (1, 2), (2, 2), (0, 3), (1, 3), (2, 3), (3, 3)]
    gram = {(0, 0): aa}
    for k, (i, j) in enumerate(pairs):
        gram[i, j] = gram[j, i] = pick(totals, k)
    zero = jnp.zeros_like(aa)
    one = jnp.ones_like(aa)
    images = [[drop, one, zero, zero], [over, along, one, zero], [zero, zero, zero, one]]
    size = KRYLOV + 1

    def product(left, right):
        return sum(left[i] * right[j] * gram[i, j] for i in range(size) for j in range(size))

    beta = jnp.sqrt(aa + epsilon)
    basis = [[1.0 / beta, zero, zero, zero]]
    hessen = [[zero] * KRYLOV for row in range(size)]
    for j in range(KRYLOV):
        image = [sum(basis[j][k] * images[k][i] for k in range(KRYLOV)) for i in range(size)]
        found = [product(basis[i], image) for i in range(j + 1)]
        for i in range(j + 1):
            hessen[i][j] = found[i]
            image = [w - found[i] * v for w, v in zip(image, basis[i])]
        length = jnp.sqrt(jnp.maximum(product(image, image), 0.0) + epsilon)
        hessen[j + 1][j] = length
        basis.append([w / length for w in image])
    ortho = []
    upper = [[None] * KRYLOV for row in range(KRYLOV)]
    for column in range(KRYLOV):
        current = [hessen[row][column] for row in range(size)]
        for row in range(column):
            factor = sum(x * y for x, y in zip(ortho[row], current))
            upper[row][column] = factor
            current = [y - factor * x for x, y in zip(ortho[row], current)]
        length = jnp.sqrt(sum(y * y for y in current))
        upper[column][column] = length
        ortho.append([y / length for y in current])
    values = [None] * KRYLOV
    for row in reversed(range(KRYLOV)):
        accum = ortho[row][0] * beta
        for later in range(row + 1, KRYLOV):
            accum = accum - upper[row][later] * values[later]
        values[row] = accum / upper[row][row]
    weights = [sum(values[j] * basis[j][k] for j in range(KRYLOV)) for k in range(KRYLOV)]
    weights[0] = weights[0] - drop * weights[1]
    return weights


def coefficients(plan, recv_ref, strip, table_ref):
    window = plan.window
    lane = lane_of((SUB, LANE))
    stride = plan.space * plan.inward
    lines = [
        recv_ref[pl.ds(s * plan.inward + plan.inward - 1, SUB, stride), :]
        for s in range(plan.space)
    ]
    fields = []
    for f in range(3):
        parts = []
        for line in lines:
            part = None
            for g in range(plan.tm):
                moved = spin(line, (g - f) * window)
                part = moved if g == 0 else jnp.where(lane // window == g, moved, part)
            parts.append(part)
        fields.append(jnp.concatenate(parts, axis=0))
    diff, vel_col, vel_row = fields
    shape = (plan.rows, LANE)
    row = lax.broadcasted_iota(jnp.int32, shape, 0)
    col = strip * plan.own - plan.halo + lane_of(shape) % window
    center = 1.0 + 4.0 * diff
    table_ref[0] = damping * center
    table_ref[1] = 1.0 / center
    table_ref[2] = jnp.where(row > 0, damping * (diff + vel_row), 0.0)
    table_ref[3] = jnp.where(row < plan.rows - 1, damping * (diff - vel_row), 0.0)
    table_ref[4] = jnp.where(col > 0, damping * (diff + vel_col), 0.0)
    table_ref[5] = jnp.where(col < plan.cols - 1, damping * (diff - vel_col), 0.0)


def krylov_kernel(plan, j, *refs):
    refs = list(refs)
    strip = plan.strip_of(lax.axis_index("tm"), lax.axis_index("space"))
    here, window, rows, halo, own = plan.here, plan.window, plan.rows, plan.halo, plan.own
    slot = plan.slot
    final = j == KRYLOV - 1
    shape = (rows, LANE)
    lane = lane_of(shape)
    low_lane = lane_of((SUB, LANE))
    low_spot = low_lane & (window - 1)
    even = strip % 2 == 0
    if j == 0:
        recv_ref, table_ref, q_ref, g_ref, w_ref, near_ref, far_ref, y_ref, tail_ref = refs
        coefficients(plan, recv_ref, strip, table_ref)
    elif not final:
        table_ref, image_ref, near_in, far_in, first_ref = refs[:5]
        q_ref, g_ref, w_ref, near_ref, far_ref, sum_ref, y_ref = refs[5:]
    else:
        table_ref, image_ref, near_in, far_in, first_ref, second_ref, mid_ref = refs[:7]
        g_ref, sum_ref, y_ref, q_ref, w_ref, rest_ref = refs[7:]
        _, drop, over, along = middle(totals_of(mid_ref))
    center = table_ref[0]
    inverse = table_ref[1]
    north, south, west, east = (table_ref[2 + k] for k in range(4))
    zero = jnp.zeros(shape, jnp.float32)
    low_zero = jnp.zeros((SUB, LANE), jnp.float32)
    inner = slice(SUB, SUB + rows)

    def around(n, field):
        return (
            north * g_ref[n, SUB - 1 : SUB - 1 + rows, :]
            + south * g_ref[n, SUB + 1 : SUB + 1 + rows, :]
            + west * spin(field, 1)
            + east * spin(field, -1)
        )

    power = inverse
    for _ in range(int(math.log2(here))):
        power = power * power
    whole = power
    for _ in range(int(math.log2(plan.tm))):
        whole = whole * whole
    closing = 1.0 / (1.0 - alpha_corner * whole)

    def entering(ends):
        total = alpha_corner * ends
        for k in reversed(range(1, plan.tm)):
            back = spin(ends, k * window)
            total = total * power + jnp.where(lane < k * window, alpha_corner * back, back)
        return total * closing

    def settle(base, y):
        for k in range(UNROLL):
            y = (y_ref[base + k] + y) * inverse
            y_ref[base + k] = y
        return y

    for k in range(UNROLL):
        y_ref[k] = zero

    def blank(n):
        g_ref[n] = jnp.zeros((rows + 2 * SUB, LANE), jnp.float32)

    if j == 0:
        last_tile = plan.tiles - 1

        def tails(k, carry):
            for p in (4 * k, 4 * k + 1, 4 * k + 2, 4 * k + 3):
                for s in range(plan.space):
                    source = p * plan.space + s
                    total = low_zero
                    for a in range(last_tile):
                        tile = recv_ref[pl.ds(source * plan.inward + a * SUB, SUB), :]
                        moved = spin(tile, plan.spare * a - plan.used)
                        total = jnp.where(low_spot // plan.spare == a, moved, total)
                    tail_ref[source] = total
            return carry

        lax.fori_loop(0, plan.tm // 4, tails, 0)

        def first(k, y):
            parts = [[] for _ in range(PAIR)]
            for t in range(PAIR):
                a = k * PAIR + t
                whole = a < last_tile
                at = jnp.minimum(a, last_tile - 1) * SUB
                for s in range(plan.space):
                    cut = []
                    for p in range(plan.tm):
                        source = p * plan.space + s
                        tile = recv_ref[pl.ds(source * plan.inward + at, SUB), :]
                        cut.append(damping * jnp.where(whole, tile, tail_ref[source]))
                    parts[t].append(exchange_blocks(cut, window, 2))
            for t in range(PAIR):
                for i in range(SUB):
                    n = (k * PAIR + t) * SUB + i
                    q = jnp.concatenate([part[i] for part in parts[t]], axis=0)
                    q_ref[n] = q
                    y = (q + y) * inverse
                    y_ref[UNROLL + n] = y
                    blank(n)
            return y

        y = lax.fori_loop(0, plan.tiles // PAIR, first, zero)
    else:
        right_mask = (low_spot >= halo + own) & (low_spot < halo + own + halo)
        left_mask = low_spot < halo

        def first(i, y):
            base = i * UNROLL
            y = settle(base, y)
            for k in range(UNROLL):
                n = base + k
                near, far = near_in[n], far_in[n]
                right = jnp.where(even, near, far)
                left = jnp.where(even, far, near)
                image = image_ref[n]
                parts = []
                for s in range(plan.space):
                    part = image[s * SUB : (s + 1) * SUB]
                    part = jnp.where(right_mask, spin(right, halo + own - slot * s), part)
                    part = jnp.where(left_mask, spin(left, halo - own - slot * s), part)
                    parts.append(part)
                q = jnp.concatenate(parts, axis=0)
                if final:
                    start, later = first_ref[n], second_ref[n]
                    rest = later - drop * start
                    rest_ref[n] = rest
                    q = (q - drop * later) - over * start - along * rest
                q_ref[n] = q
                y_ref[UNROLL + n] = q
                blank(n)
            return y

        y = settle(here, lax.fori_loop(0, here // UNROLL, first, zero))

    def sweep(_, ends):
        def body(i, carry):
            y, z = carry
            base = i * UNROLL
            olds = [y_ref[UNROLL + base + k] for k in range(UNROLL)]
            y = settle(base, y)
            for k in range(UNROLL):
                n = base + k
                z = z * inverse
                guess = (1.0 - damping) * g_ref[n, inner, :] + (olds[k] + z)
                g_ref[n, inner, :] = guess
                y_ref[UNROLL + n] = q_ref[n] + around(n, guess)
            return (y, z)

        y, _ = lax.fori_loop(0, here // UNROLL, body, (zero, entering(ends)))
        return settle(here, y)

    y = lax.fori_loop(0, SWEEPS - 1, sweep, y)
    start = entering(y)
    ending = (1.0 - damping) * g_ref[here - 1, inner, :] + (y + start * power)
    before = jnp.where(lane < window, 0.0, damping * spin(ending, window))

    ahead = [
        ((low_lane - slot * s - (own - halo)) & (window - 1)) < halo for s in range(plan.space)
    ]

    def fold(block):
        return sum(block[s * SUB : (s + 1) * SUB] for s in range(plan.space))

    size = KRYLOV + 1

    def gather(base, accs):
        for k in range(TAIL):
            n = base + k
            image = w_ref[n]
            if not final:
                left = right = None
                for s in range(plan.space):
                    moved = spin(image[s * SUB : (s + 1) * SUB], slot * s - halo)
                    left = moved if s == 0 else jnp.where(low_spot // slot == s, moved, left)
                    right = moved if s == 0 else jnp.where(ahead[s], moved, right)
                near_ref[n] = jnp.where(even, right, left)
                far_ref[n] = jnp.where(even, left, right)
            if j == 0:
                continue
            q = q_ref[n]
            start = first_ref[n]
            if not final:
                pairs = [(start, start), (start, q), (q, q), (start, image), (q, image)]
            else:
                rest = rest_ref[n]
                held = [start, rest, q, image]
                pairs = [(held[i], held[k]) for k in range(1, size) for i in range(k + 1)]
            accs = [acc + fold(x * y) for acc, (x, y) in zip(accs, pairs)]
        return accs

    def last(i, carry):
        z, before, accs = carry
        accs = gather(jnp.maximum(i - 1, 0) * TAIL, accs)
        accs = tuple(jnp.where(i > 0, acc, 0.0) for acc in accs)
        for k in range(TAIL):
            n = i * TAIL + k
            z = z * inverse
            guess = (1.0 - damping) * g_ref[n, inner, :] + (y_ref[UNROLL + n] + z)
            g_ref[n, inner, :] = guess
            w_ref[n] = center * guess - around(n, guess) - before
            before = damping * guess
        return (z, before, accs)

    fields = (0, 5, 9)[j]
    _, _, accs = lax.fori_loop(0, here // TAIL, last, (start, before, (low_zero,) * fields))
    accs = gather(here - TAIL, list(accs))
    if j == 0:
        return
    owned = (low_spot >= halo) & (low_spot < halo + own)
    record = jnp.zeros((1, LANE), jnp.float32)
    record_lane = lane_of((1, LANE))
    for place, acc in enumerate(accs):
        value = jnp.sum(jnp.where(owned, acc, 0.0), axis=0, keepdims=True)
        value = jnp.sum(value, axis=1, keepdims=True)
        record = jnp.where(record_lane == place, value, record)
    sum_ref[...] = jnp.broadcast_to(record, sum_ref.shape)


def combine_kernel(plan, *refs):
    z_refs = refs[:KRYLOV]
    mid_ref, end_ref, out_ref = refs[KRYLOV:]
    along = iterate(totals_of(mid_ref), totals_of(end_ref))
    own, halo, window, groups = plan.own, plan.halo, plan.window, plan.groups
    lane = lane_of((SUB, LANE))
    front = lane % window < own
    size = plan.outward

    def start_of(p, s):
        return (p * plan.space + s) * size

    def value(n, s):
        here = slice((s + 1) * SUB, (s + 2) * SUB)
        return sum(c * ref[n, here, :] for c, ref in zip(along, z_refs))

    def body(k, carry):
        for t in range(PAIR):
            aa = k * PAIR + t
            for s in range(plan.space):
                pieces = []
                for i in range(SUB):
                    n = aa * 2 * SUB + 2 * i
                    left, right = spin(value(n, s), -halo), spin(value(n + 1, s), own - halo)
                    pieces.append(jnp.where(front, left, right))
                for p, piece in enumerate(exchange_blocks(pieces, window, 2)):
                    out_ref[pl.ds(start_of(p, s) + aa * SUB, SUB), :] = piece
                    if s + 1 < plan.space:
                        at = start_of(p, s + 1) + groups * SUB + aa
                        out_ref[pl.ds(at, 1), :] = piece[SUB - 1 :]
                    if s > 0:
                        at = start_of(p, s - 1) + groups * SUB + groups + aa
                        out_ref[pl.ds(at, 1), :] = piece[:1]
        return carry

    lax.fori_loop(0, groups // PAIR, body, 0)
    nothing = jnp.zeros((groups, LANE), jnp.float32)
    sub = lax.broadcasted_iota(jnp.int32, (SUB, LANE), 0)
    for p in range(plan.tm):
        at = start_of(p, 0) + groups * SUB
        out_ref[at : at + groups, :] = nothing
        at = start_of(p, plan.space - 1) + groups * SUB + groups
        out_ref[at : at + groups, :] = nothing
    for s in range(plan.space):
        ending = value(plan.here - 1, s)
        for p in range(plan.tm):
            line = nothing[:1]
            if p > 0:
                turned = spin(ending, -(p - 1) * window - halo)
                turned = pltpu.roll(turned, 0, 1, stride=own, stride_axis=0)
                line = jnp.sum(jnp.where(lane // own == sub, turned, 0.0), axis=0, keepdims=True)
            at = start_of(p, s) + size - 1
            out_ref[at : at + 1, :] = line


def finish_kernel(plan, recv_ref, right_ref, diff_ref, vel_ref, *refs):
    results, (rim_ref, out_ref, rest_ref, sems) = refs[:2], refs[2:]
    groups, own, size = plan.groups, plan.own, plan.outward
    count = LANE // own
    parts = plan.cols // LANE
    shape = (SUB, plan.cols)
    lane = lane_of((SUB, LANE))
    diff, vel_col, vel_row = diff_ref[...], vel_ref[0], vel_ref[1]
    col = lane_of(shape)
    sub = lax.broadcasted_iota(jnp.int32, shape, 0)
    center = 1.0 + 4.0 * diff
    north = diff + vel_row
    south = diff - vel_row
    west = jnp.where(col > 0, diff + vel_col, 0.0)
    east = jnp.where(col < plan.cols - 1, diff - vel_col, 0.0)

    def start_of(part, m):
        return plan.holder[part * count + m] * size

    def spread(offset):
        wide = []
        for part in range(parts):
            pieces = [
                recv_ref[pl.ds(start_of(part, m) + offset, SUB), :] for m in range(count)
            ]
            wide.append(exchange_blocks(pieces, own, 2))
        return [jnp.concatenate(pair, axis=1) for pair in zip(*wide)]

    for i, field in enumerate(spread(groups * SUB)):
        rim_ref[i] = field
    halves = []
    row = lax.broadcasted_iota(jnp.int32, (SUB, LANE), 0)
    for part in range(parts):
        tiles = []
        for first in range(0, count, SUB):
            tile = jnp.zeros((SUB, LANE), jnp.float32)
            for q in range(SUB):
                at = start_of(part, first + q) + size - 1
                line = jnp.broadcast_to(recv_ref[at : at + 1, :], (SUB, LANE))
                tile = jnp.where(row == q, line, tile)
            tile = spin(tile, first * own)
            tiles.append((first, pltpu.roll(tile, 0, 1, stride=own, stride_axis=0)))
        total = jnp.zeros((SUB, LANE), jnp.float32)
        for r in range(SUB):
            line = sum(
                jnp.where(lane // own == row + first, spin(tile, -r * own), 0.0)
                for first, tile in tiles
            )
            line = jnp.sum(line, axis=0, keepdims=True)
            total = jnp.where(row == r, jnp.broadcast_to(line, (SUB, LANE)), total)
        halves.append(total)
    before = jnp.concatenate(halves, axis=1)

    size_of = PAIR * count

    def copies(k):
        at = pl.ds(k * size_of, size_of)
        return [
            pltpu.make_async_copy(ref.at[at], result.at[at], sems.at[k, f])
            for f, (ref, result) in enumerate(zip((out_ref, rest_ref), results))
        ]

    def body(k, before):
        for t in range(PAIR):
            aa = k * PAIR + t
            for i, field in enumerate(spread(aa * SUB)):
                n = aa * count + i
                above = rim_ref[i, pl.ds(aa, 1), :]
                below = rim_ref[i, pl.ds(groups + aa, 1), :]
                out_ref[n] = field
                around = (
                    north * jnp.where(sub == 0, above, spin(field, 1, 0))
                    + south * jnp.where(sub == SUB - 1, below, spin(field, -1, 0))
                    + west * spin(field, 1)
                    + east * spin(field, -1)
                )
                rest_ref[n] = right_ref[n] - (center * field - around - before)
                before = field
        for copy in copies(k):
            copy.start()
        return before

    lax.fori_loop(0, groups // PAIR, body, before)
    for k in range(groups // PAIR):
        for copy in copies(k):
            copy.wait()


def call(kernel, shapes, operands, scratch=(), sems=None, far_in=False, far_out=False, room=16):
    vmem = pl.BlockSpec(memory_space=pltpu.VMEM)
    hbm = pl.BlockSpec(memory_space=pltpu.HBM)
    held = [pltpu.VMEM(shape, jnp.float32) for shape in scratch]
    if sems:
        held.append(pltpu.SemaphoreType.DMA(sems))
    return pl.pallas_call(
        kernel,
        out_shape=[jax.ShapeDtypeStruct(shape, jnp.float32) for shape in shapes],
        in_specs=[hbm if far_in else vmem] * len(operands),
        out_specs=[hbm if far_out else vmem] * len(shapes),
        scratch_shapes=held,
        compiler_params=pltpu.CompilerParams(vmem_limit_bytes=room * 1024 * 1024),
    )(*operands)


def everyone(block, devices):
    lines = block.shape[0] // devices
    parts = block.reshape(devices, lines, 1, LANE)
    return lax.all_to_all(parts, AXES, split_axis=0, concat_axis=0, tiled=True).reshape(block.shape)


def strip_device(plan, right_side, diffusion, velocity):
    count = plan.devices
    hold = plan.holder
    near_route = []
    far_route = []
    for k in range(0, count, 2):
        near_route += [(hold[k], hold[k + 1]), (hold[k + 1], hold[k])]
    for k in range(1, count - 1, 2):
        far_route += [(hold[k], hold[k + 1]), (hold[k + 1], hold[k])]
    bind = lambda kernel, *more: (lambda *refs: kernel(plan, *more, *refs))
    full = (plan.here, plan.rows, LANE)
    padded = (plan.here, plan.rows + 2 * SUB, LANE)
    delayed = (plan.here + UNROLL, plan.rows, LANE)
    side = (plan.here, SUB, LANE)
    small = (count, LANE)
    given = [right_side, diffusion, velocity]
    sent = call(
        bind(pack_kernel),
        [(count * plan.inward, LANE)],
        given,
        scratch=[(count, SUB, LANE), *(block.shape for block in given)],
        sems=(4,),
        far_in=True,
        room=63,
    )[0]
    table, q0, z0, image, near, far = call(
        bind(krylov_kernel, 0),
        [(6, plan.rows, LANE), full, padded, full, side, side],
        [everyone(sent, count)],
        scratch=[delayed, (count, SUB, LANE)],
    )
    near = lax.ppermute(near, AXES, near_route)
    far = lax.ppermute(far, AXES, far_route)
    q1, z1, image, near, far, sums = call(
        bind(krylov_kernel, 1),
        [full, padded, full, side, side, small],
        [table, image, near, far, q0],
        scratch=[delayed],
    )
    near = lax.ppermute(near, AXES, near_route)
    far = lax.ppermute(far, AXES, far_route)
    mid = everyone(sums, count)
    z2, sums = call(
        bind(krylov_kernel, 2),
        [padded, small],
        [table, image, near, far, q0, q1, mid],
        scratch=[delayed, full, full, full],
    )
    end = everyone(sums, count)
    packed = call(bind(combine_kernel), [(count * plan.outward, LANE)], [z0, z1, z2, mid, end])[0]
    shape = right_side.shape
    return tuple(
        call(
            bind(finish_kernel),
            [shape, shape],
            [everyone(packed, count), *given],
            scratch=[(2 * SUB, SUB, plan.cols), shape, shape],
            sems=(plan.groups // PAIR, 2),
            far_out=True,
        )
    )


def per_device(mesh):
    def run(right_side, diffusion, velocity):
        rows = right_side.shape[1] * mesh.shape["space"]
        steps = right_side.shape[0] * mesh.shape["tm"]
        plan = Plan(mesh, steps, rows, right_side.shape[2])
        if plan.fits():
            return strip_device(plan, right_side, diffusion, velocity)
        return generic_device(right_side, diffusion, velocity)

    return run


def solution(mesh):
    placed = (P("tm", "space", None), P("space", None), P(None, "space", None))
    return jax.shard_map(
        per_device(mesh),
        mesh=mesh,
        in_specs=placed,
        out_specs=(P("tm", "space", None), P("tm", "space", None)),
        check_vma=False,
    )
```
